256 devices in a mesh: px: 32 (over x, z_hi, core), py: 8 (over z_lo, y).
Axes of the slice: x: 4, y: 4, z: 8 (z_hi: 4, z_lo: 2; z = z_hi * 2 + z_lo), core: 2. Of those that a mesh axis runs over, the one named last changes fastest.
Arguments:
- velocity: float32 [3, 1024, 8, 1024], P(None, 'px', 'py'), may hold values from -1.5 to 2.5
- band_of: int32 [8], replicated, may hold values from 0 to 1, as said below
Outputs:
- correlation: float32 [6, 2, 1024, 1024], P(None, None, ('px', 'py'))
The draws below stay inside these ranges and needn't reach their ends.
Inputs may be any that keep to these rules, and one draw needn't show every extreme that they name: `band_of`: every band 0 to 1 holds at least one plane.
All inputs are finite; a program needn't handle non-finite values.
Results may differ from the reference program's by a relative error of at most 0.00013.
Values sent between devices are 32-bit elements; how exact they have to be, the bound alone decides.
No kernel may reach another device: no remote copies, remote signals or barrier semaphores. Data moves between devices by JAX's collectives and lax.ppermute only.
A program may use at most 64 MiB of HBM per device.

```python
import math
import jax
import jax.numpy as jnp
from jax import lax

NX = 1024
NZ = 1024
NY = 8
NB = 2


def draw_band_of(key, part):
    first_key = jax.random.fold_in(key, 11)
    second_key = jax.random.fold_in(key, 23)
    random_band = jax.random.randint(first_key, (NY,), 0, NB, dtype=jnp.int32)
    shuffled = jax.random.permutation(second_key, jnp.arange(NY, dtype=jnp.int32))
    return jnp.where(shuffled < NB, shuffled, random_band).astype(jnp.int32)


def level_of(key, dims, cuts, low, high):
    level, own = 1.0, jax.random.fold_in(key, 6)
    for axis_at, blocks in cuts:
        draws = jnp.exp(jax.random.uniform(jax.random.fold_in(own, axis_at), (blocks,), jnp.float32, low / len(cuts), high / len(cuts)))
        level = level * jnp.repeat(draws, dims[axis_at] // blocks).reshape([-1 if axis == axis_at else 1 for axis in range(len(dims))])
    return level


def setup_inputs(seed: int = 0) -> dict:
    splits = jax.random.split(jax.random.key(seed), 3)
    velocity = jnp.clip(-1.5 + 4.0 * jax.random.uniform(splits[0], (3, NX, NY, NZ), jnp.float32) ** level_of(splits[0], (3, NX, NY, NZ), ((1, 32), (2, 8)), -0.2, 0.2), -1.5, 2.5)
    band_of = draw_band_of(jax.random.fold_in(splits[2], 71), 0)
    return dict(velocity=velocity, band_of=band_of)


PAIR_LIST = ((0, 0), (0, 1), (0, 2), (1, 1), (1, 2), (2, 2))

def reference(velocity, band_of):
    half = NZ // 2
    cells = NX * NZ
    span_spec = jnp.fft.rfft(velocity, axis=3)[..., :half]
    spectrum = jnp.fft.fft(span_spec, axis=1)
    spectrum = spectrum.at[:, 0, :, 0].set(0.0)
    band_ids = jnp.arange(NB, dtype=jnp.int32)
    onehot = (band_of[:, None] == band_ids[None, :]).astype(jnp.float32)
    counts = lax.optimization_barrier(jnp.sum(onehot, 0))
    band_weight = onehot / (counts[None, :] * (cells * math.sqrt(cells)))
    results = []
    for left_comp, right_comp in PAIR_LIST:
        product = jnp.conj(spectrum[left_comp]) * spectrum[right_comp]
        banded_real = jnp.einsum('xyk,yb->bxk', jnp.real(product), band_weight, precision=lax.Precision.HIGHEST)
        banded_imag = jnp.einsum('xyk,yb->bxk', jnp.imag(product), band_weight, precision=lax.Precision.HIGHEST)
        stream_back = jnp.fft.ifft(lax.complex(banded_real, banded_imag), axis=1) * NX
        padded = jnp.concatenate((stream_back, jnp.zeros((NB, NX, 1), stream_back.dtype)), 2)
        results.append(jnp.fft.irfft(padded, n=NZ, axis=2) * NZ)
    return jnp.stack(results, 0)
```

```python
import math

import jax
import jax.numpy as jnp
import numpy as np
from jax import lax
from jax.experimental import pallas as pl
from jax.experimental.pallas import tpu as pltpu
from jax.sharding import PartitionSpec as P

NX = 1024
NZ = 1024
NY = 8
NB = 2
PAIR_LIST = ((0, 0), (0, 1), (0, 2), (1, 1), (1, 2), (2, 2))
ROOT_HALF = math.sqrt(0.5)
F32 = jnp.float32
BF16 = jnp.bfloat16


def wave(rows, cols, length):
    angle = 2.0 * np.pi * (np.multiply.outer(rows, cols) % length) / length
    return np.cos(angle), np.sin(angle)


def stacked_split(table):
    high = table.astype(np.float32).astype(jnp.bfloat16)
    low = (table - high.astype(np.float64)).astype(np.float32).astype(jnp.bfloat16)
    return np.concatenate((high, low), 0)


def span_forward_tables():
    cos_tw, sin_tw = wave(np.arange(8), np.arange(128), 1024)
    twiddle = np.concatenate((cos_tw, sin_tw), 0).astype(np.float32)
    cos_t, sin_t = wave(np.arange(64), np.arange(128), 128)
    return twiddle, stacked_split(np.concatenate((cos_t, sin_t), 1))


def middle_tables():
    base = np.arange(32)
    cos32, sin32 = wave(base, base, 32)
    eye8 = np.eye(8)
    over_px = stacked_split(np.concatenate((np.kron(cos32, eye8), np.kron(-sin32, eye8)), 0))
    cos_tw, sin_tw = wave(base, base, 1024)
    spread = lambda t: np.repeat(np.tile(t, (1, 4)), 8, 0)
    front_twiddle = np.concatenate((spread(cos_tw), spread(sin_tw)), 0).astype(np.float32)
    eye2 = np.eye(2)
    block = lambda t: np.kron(eye2, t)
    within = stacked_split(np.block([[block(cos32), block(sin32)], [block(-sin32), block(cos32)]]))
    back = np.zeros((8, 2, 2, 4, 2, 2, 32))
    for py in range(8):
        for i in range(4):
            c, s = cos32[4 * py + i], sin32[4 * py + i]
            for s2 in range(2):
                back[py, 0, s2, i, s2, 0] = c
                back[py, 0, s2, i, s2, 1] = -s
                back[py, 1, s2, i, s2, 0] = s
                back[py, 1, s2, i, s2, 1] = c
    back = stacked_split(back.reshape(128, 128))
    first = np.zeros((8, 2, 4, 2, 2, 32))
    second = np.zeros((8, 2, 4, 2, 2, 32))
    for py in range(8):
        for i in range(4):
            c, s = cos_tw[4 * py + i], sin_tw[4 * py + i]
            first[py, :, i, 0] = c
            first[py, :, i, 1] = -s
            second[py, :, i, 0] = s
            second[py, :, i, 1] = c
    back_twiddle = np.concatenate((first.reshape(64, 128), second.reshape(64, 128)), 0).astype(np.float32)
    final = stacked_split(np.concatenate((np.kron(eye2, cos32), np.kron(eye2, sin32)), 1))
    return over_px, front_twiddle, within, back, back_twiddle, final


def span_inverse_tables():
    cos_t, sin_t = wave(np.arange(64), np.arange(128), 128)
    one = 2.0 * np.concatenate((cos_t, sin_t), 1)
    table = stacked_split(np.kron(np.eye(2), one))
    cos_tw, sin_tw = wave(np.arange(8), np.arange(128), 1024)
    return table, np.concatenate((cos_tw, sin_tw), 0).astype(np.float32)


def split(x):
    high = x.astype(BF16)
    return high, (x - high.astype(F32)).astype(BF16)


def dot_nn(a, b):
    return lax.dot_general(a, b, (((1,), (0,)), ((), ())), preferred_element_type=F32)


def dot_nt(a, b):
    return lax.dot_general(a, b, (((1,), (1,)), ((), ())), preferred_element_type=F32)


def table_times(dot, table, high, low):
    rows = table.shape[0] // 2
    both = dot(table, high)
    return both[:rows] + both[rows:] + dot(table[:rows], low)


def span_forward_kernel(v_ref, twiddle_ref, table_ref, out_ref):
    x = [v_ref[pl.ds(s, 96, stride=8), :] for s in range(8)]
    e = [x[s] + x[s + 4] for s in range(4)]
    o = [x[s] - x[s + 4] for s in range(4)]
    e02, e13 = e[0] + e[2], e[1] + e[3]
    om, op = ROOT_HALF * (o[1] - o[3]), ROOT_HALF * (o[1] + o[3])
    e02m, e13m = e[0] - e[2], e[1] - e[3]
    one = (o[0] + om, -(o[2] + op))
    three = (o[0] - om, o[2] - op)
    spec = [
        (e02 + e13, None),
        one,
        (e02m, -e13m),
        three,
        (e02 - e13, None),
        (three[0], -three[1]),
        (e02m, e13m),
        (one[0], -one[1]),
    ]
    parts = []
    for k1 in range(8):
        re, im = spec[k1]
        c = twiddle_ref[pl.ds(k1, 1), :]
        s = twiddle_ref[pl.ds(8 + k1, 1), :]
        if k1 == 0:
            new_re, new_im = re, jnp.zeros_like(re)
        elif im is None:
            new_re, new_im = re * c, -(re * s)
        else:
            new_re, new_im = re * c + im * s, im * c - re * s
        parts.append((split(new_re), split(new_im)))
    table = table_ref[...]
    for j in range(4):
        columns = []
        for level in range(2):
            rows = []
            for c in range(3):
                cut = slice(32 * c, 32 * c + 32)
                for turn in range(2):
                    for k1 in (2 * j, 2 * j + 1):
                        re, im = parts[k1][0][level][cut], parts[k1][1][level][cut]
                        rows.append(jnp.concatenate((re, im) if turn == 0 else (im, -re), 1))
            columns.append(jnp.concatenate(rows, 0))
        result = table_times(dot_nt, table, columns[0], columns[1])
        for c in range(3):
            out_ref[pl.ds(192 * j + c, 64, stride=3), :] = result[:, 128 * c : 128 * c + 128]


def middle_kernel(anchor, band_ref, r_ref, over_px_ref, front_tw_ref, within_ref, back_ref, back_tw_ref, final_ref, out_ref):
    data = jnp.concatenate([r_ref[pl.ds(c, 256, stride=3), :] for c in range(3)], 1)
    high, low = split(data)
    turned = table_times(dot_nn, over_px_ref[...], high, low)
    cos_tw, sin_tw = front_tw_ref[:256, :], front_tw_ref[256:, :]
    lane = lax.broadcasted_iota(jnp.int32, (1, 128), 1)
    sign = jnp.where(lane < 64, -1.0, 1.0).astype(F32)
    spectrum = []
    for c in range(3):
        p, q = turned[:256, 128 * c : 128 * c + 128], turned[256:, 128 * c : 128 * c + 128]
        a = p * cos_tw + q * sin_tw
        b = q * cos_tw - p * sin_tw
        u_high, u_low = split(a + pltpu.roll(b, 64, axis=1) * sign)
        out = table_times(dot_nt, within_ref[...], u_high, u_low)
        spectrum.append((out[:64], out[64:]))
    sub = lax.broadcasted_iota(jnp.int32, (8, 128), 0)
    lanes = lax.broadcasted_iota(jnp.int32, (8, 128), 1)
    band = jnp.zeros((8, 128), jnp.int32)
    count_one = jnp.int32(0)
    for y in range(8):
        band = jnp.where(sub == y, band_ref[y], band)
        count_one = count_one + band_ref[y]
    lane_band = (lanes // 32) % 2
    in_band = band == lane_band
    select = jnp.concatenate(
        [jnp.where(jnp.logical_and(in_band, lanes % 32 == k1), 1.0, 0.0).astype(F32) for k1 in range(32)], 0
    ).astype(BF16)
    one_f = jnp.full((8, 128), count_one, jnp.int32).astype(F32)
    count = jnp.where(lane_band == 1, one_f, 8.0 - one_f)
    weight = 1.0 / (count * float(NX * NZ * 1024))
    row64 = lax.broadcasted_iota(jnp.int32, (64, 128), 0)
    lane64 = lax.broadcasted_iota(jnp.int32, (64, 128), 1)
    scale = jnp.concatenate([weight] * 8, 0)
    scale = jnp.where(jnp.logical_and(anchor, row64 < 32), 0.5 * scale, scale)
    mean = jnp.logical_and(anchor, jnp.logical_and(row64 == 0, lane64 % 32 == 0))
    scale = jnp.where(mean, 0.0, scale)
    banded = []
    for left, right in PAIR_LIST:
        lr, li = spectrum[left]
        rr, ri = spectrum[right]
        values = [lr * rr + li * ri]
        if left != right:
            values.append(lr * ri - li * rr)
        sums = []
        for value in values:
            value_high, value_low = split(value)
            sums.append((dot_nn(value_high, select) + dot_nn(value_low, select)) * scale)
        if left == right:
            sums.append(jnp.zeros((64, 128), F32))
        banded.append(sums)
    columns = []
    for k in range(2):
        for sp in range(3):
            cut = slice(32 * k, 32 * k + 32)
            columns.append(jnp.concatenate([banded[2 * sp + s2][part][cut] for s2 in range(2) for part in range(2)], 0))
    x_high, x_low = split(jnp.concatenate(columns, 1))
    v = table_times(dot_nn, back_ref[...], x_high, x_low)
    pad = jnp.zeros((32, 128), F32)
    for py in range(8):
        t1 = back_tw_ref[pl.ds(8 * py, 8), :]
        t2 = back_tw_ref[pl.ds(64 + 8 * py, 8), :]
        re_rows, im_rows = [], []
        for column in range(6):
            cut = slice(128 * column, 128 * column + 128)
            vr, vi = v[16 * py : 16 * py + 8, cut], v[16 * py + 8 : 16 * py + 16, cut]
            re_rows.append(vr * t1 - vi * t2)
            im_rows.append(vr * t2 + vi * t1)
        rows_high, rows_low = split(jnp.concatenate(re_rows + im_rows + [pad], 0))
        out = table_times(dot_nt, final_ref[...], rows_high, rows_low)
        for b in range(2):
            out_ref[pl.ds(2 * py + b, 32, stride=16), :] = out[32 * b : 32 * b + 32]


def span_inverse_kernel(r_ref, table_ref, twiddle_ref, out_ref):
    table = table_ref[...]
    lhs = []
    for b in range(2):
        rows = r_ref[pl.ds(b, 256, stride=2), :].T
        for jp in range(2):
            lhs.append(rows[:96, 128 * jp : 128 * jp + 128])
    high, low = split(jnp.concatenate(lhs, 0))
    sums = dot_nn(high, table[:128]) + dot_nn(high, table[128:]) + dot_nn(low, table[:128])
    sub = lax.broadcasted_iota(jnp.int32, (8, 128), 0)
    for b in range(2):
        for sp in range(3):
            y = []
            for k1 in range(8):
                j, k = k1 // 2, k1 % 2
                row = (b * 2 + j // 2) * 96 + k * 24 + sp * 8
                col = (j % 2) * 256
                rc, rs = sums[row : row + 8, col : col + 128], sums[row : row + 8, col + 128 : col + 256]
                ic, is_ = sums[row + 48 : row + 56, col : col + 128], sums[row + 48 : row + 56, col + 128 : col + 256]
                zr, zi = rc - is_, rs + ic
                c, s = twiddle_ref[pl.ds(k1, 1), :], twiddle_ref[pl.ds(8 + k1, 1), :]
                if k1 == 0:
                    y.append((zr, None))
                elif k1 == 4:
                    y.append((zr * c - zi * s, None))
                else:
                    y.append((zr * c - zi * s, zr * s + zi * c))
            a = [None] + [y[k][0] + y[8 - k][0] for k in (1, 2, 3)]
            d = [None] + [y[k][1] - y[8 - k][1] for k in (1, 2, 3)]
            up, um = y[0][0] + y[4][0], y[0][0] - y[4][0]
            ap, am = a[1] + a[3], ROOT_HALF * (a[1] - a[3])
            dm, dp = d[1] - d[3], ROOT_HALF * (d[1] + d[3])
            upp, upm = up + a[2], up - a[2]
            ump, umm = um + d[2], um - d[2]
            outs = [
                upp + ap,
                umm + am - dp,
                upm - dm,
                ump - am - dp,
                upp - ap,
                umm - am + dp,
                upm + dm,
                ump + am + dp,
            ]
            for half in range(4):
                v0, v1 = outs[2 * half], outs[2 * half + 1]
                base = (sp * 2 * 2 + b) * 32 + half * 8
                out_ref[pl.ds(base, 8), :] = jnp.where(sub < 4, v0, pltpu.roll(v1, 4, axis=0))
                out_ref[pl.ds(base + 64, 8), :] = jnp.where(sub < 4, pltpu.roll(v0, 4, axis=0), v1)


def vmem(count):
    return [pl.BlockSpec(memory_space=pltpu.VMEM)] * count


def call(kernel, out_shape, in_specs, name):
    return pl.pallas_call(
        kernel,
        out_shape=jax.ShapeDtypeStruct(out_shape, F32),
        in_specs=in_specs,
        out_specs=pl.BlockSpec(memory_space=pltpu.VMEM),
        name=name,
    )


def run_span_forward(velocity):
    twiddle, table = span_forward_tables()
    return call(span_forward_kernel, (768, 128), vmem(3), "span_forward")(velocity, twiddle, table)


def run_middle(received, band_of, anchor=None):
    def kernel(band_ref, *refs):
        if anchor is None:
            at_anchor = jnp.logical_and(lax.axis_index("px") == 0, lax.axis_index("py") == 0)
        else:
            at_anchor = anchor
        middle_kernel(at_anchor, band_ref, *refs)

    specs = [pl.BlockSpec(memory_space=pltpu.SMEM)] + vmem(7)
    return call(kernel, (512, 128), specs, "middle")(band_of, received, *middle_tables())


def run_span_inverse(received):
    return call(span_inverse_kernel, (384, 128), vmem(3), "span_inverse")(received, *span_inverse_tables())


def per_device(velocity, band_of):
    sent = run_span_forward(velocity.reshape(768, 128))
    received = lax.all_to_all(sent.reshape(256, 1, 384), ("px", "py"), 0, 0, tiled=True)
    back = run_middle(received.reshape(768, 128), band_of)
    gathered = lax.all_to_all(back.reshape(256, 1, 256), ("px", "py"), 0, 0, tiled=True)
    out = run_span_inverse(gathered.reshape(512, 128))
    return out.reshape(6, 2, 8, 4, 128).transpose(0, 1, 3, 2, 4).reshape(6, 2, 4, 1024)


def solution(mesh):
    in_specs = (P(None, "px", "py", None), P())
    out_specs = P(None, None, ("px", "py"), None)
    return jax.shard_map(per_device, mesh=mesh, in_specs=in_specs, out_specs=out_specs, check_vma=False)
```

```python
import math

import jax
import jax.numpy as jnp
import numpy as np
from jax import lax
from jax.experimental import pallas as pl
from jax.experimental.pallas import tpu as pltpu
from jax.sharding import PartitionSpec as P

NX = 1024
NZ = 1024
NY = 8
NB = 2
PAIR_LIST = ((0, 0), (0, 1), (0, 2), (1, 1), (1, 2), (2, 2))
ROOT_HALF = math.sqrt(0.5)
F32 = jnp.float32
BF16 = jnp.bfloat16


def wave(rows, cols, length):
    angle = 2.0 * np.pi * (np.multiply.outer(rows, cols) % length) / length
    return np.cos(angle), np.sin(angle)


def stacked_split(table):
    high = table.astype(np.float32).astype(jnp.bfloat16)
    low = (table - high.astype(np.float64)).astype(np.float32).astype(jnp.bfloat16)
    return np.concatenate((high, low), 0)


def span_forward_tables():
    cos_tw, sin_tw = wave(np.arange(8), np.arange(128), 1024)
    twiddle = np.concatenate((cos_tw, sin_tw), 0).astype(np.float32)
    cos_t, sin_t = wave(np.arange(64), np.arange(128), 128)
    return twiddle, stacked_split(np.concatenate((cos_t, sin_t), 1))


def middle_tables():
    base = np.arange(32)
    cos32, sin32 = wave(base, base, 32)
    eye8 = np.eye(8)
    over_px = stacked_split(np.concatenate((np.kron(cos32, eye8), np.kron(-sin32, eye8)), 0))
    cos_tw, sin_tw = wave(base, base, 1024)
    spread = lambda t: np.repeat(np.tile(t, (1, 4)), 8, 0)
    front_twiddle = np.concatenate((spread(cos_tw), spread(sin_tw)), 0).astype(np.float32)
    eye2 = np.eye(2)
    block = lambda t: np.kron(eye2, t)
    within = stacked_split(np.block([[block(cos32), block(sin32)], [block(-sin32), block(cos32)]]))
    back = np.zeros((8, 2, 2, 4, 2, 2, 32))
    for py in range(8):
        for i in range(4):
            c, s = cos32[4 * py + i], sin32[4 * py + i]
            for s2 in range(2):
                back[py, 0, s2, i, s2, 0] = c
                back[py, 0, s2, i, s2, 1] = -s
                back[py, 1, s2, i, s2, 0] = s
                back[py, 1, s2, i, s2, 1] = c
    back = stacked_split(back.reshape(128, 128))
    first = np.zeros((8, 2, 4, 2, 2, 32))
    second = np.zeros((8, 2, 4, 2, 2, 32))
    for py in range(8):
        for i in range(4):
            c, s = cos_tw[4 * py + i], sin_tw[4 * py + i]
            first[py, :, i, 0] = c
            first[py, :, i, 1] = -s
            second[py, :, i, 0] = s
            second[py, :, i, 1] = c
    back_twiddle = np.concatenate((first.reshape(64, 128), second.reshape(64, 128)), 0).astype(np.float32)
    final = stacked_split(np.concatenate((np.kron(eye2, cos32), np.kron(eye2, sin32)), 1))
    return over_px, front_twiddle, within, back, back_twiddle, final


def span_inverse_tables():
    cos_t, sin_t = wave(np.arange(64), np.arange(128), 128)
    one = 2.0 * np.concatenate((cos_t, sin_t), 1)
    table = stacked_split(np.kron(np.eye(2), one))
    cos_tw, sin_tw = wave(np.arange(8), np.arange(128), 1024)
    return table, np.concatenate((cos_tw, sin_tw), 0).astype(np.float32)


def split(x):
    high = x.astype(BF16)
    return high, (x - high.astype(F32)).astype(BF16)


def dot_nn(a, b):
    return lax.dot_general(a, b, (((1,), (0,)), ((), ())), preferred_element_type=F32)


def dot_nt(a, b):
    return lax.dot_general(a, b, (((1,), (1,)), ((), ())), preferred_element_type=F32)


def table_times(dot, table, high, low):
    rows = table.shape[0] // 2
    both = dot(table, high)
    return both[:rows] + both[rows:] + dot(table[:rows], low)


def span_forward_kernel(v_ref, twiddle_ref, table_ref, out_ref):
    x = [v_ref[pl.ds(s, 96, stride=8), :] for s in range(8)]
    e = [x[s] + x[s + 4] for s in range(4)]
    o = [x[s] - x[s + 4] for s in range(4)]
    e02, e13 = e[0] + e[2], e[1] + e[3]
    om, op = ROOT_HALF * (o[1] - o[3]), ROOT_HALF * (o[1] + o[3])
    e02m, e13m = e[0] - e[2], e[1] - e[3]
    one = (o[0] + om, -(o[2] + op))
    three = (o[0] - om, o[2] - op)
    spec = [
        (e02 + e13, None),
        one,
        (e02m, -e13m),
        three,
        (e02 - e13, None),
        (three[0], -three[1]),
        (e02m, e13m),
        (one[0], -one[1]),
    ]
    parts = []
    for k1 in range(8):
        re, im = spec[k1]
        c = twiddle_ref[pl.ds(k1, 1), :]
        s = twiddle_ref[pl.ds(8 + k1, 1), :]
        if k1 == 0:
            new_re, new_im = re, jnp.zeros_like(re)
        elif im is None:
            new_re, new_im = re * c, -(re * s)
        else:
            new_re, new_im = re * c + im * s, im * c - re * s
        parts.append((split(new_re), split(new_im)))
    table = table_ref[...]
    for j in range(4):
        columns = []
        for level in range(2):
            rows = []
            for c in range(3):
                cut = slice(32 * c, 32 * c + 32)
                for turn in range(2):
                    for k1 in (2 * j, 2 * j + 1):
                        re, im = parts[k1][0][level][cut], parts[k1][1][level][cut]
                        rows.append(jnp.concatenate((re, im) if turn == 0 else (im, -re), 1))
            columns.append(jnp.concatenate(rows, 0))
        result = table_times(dot_nt, table, columns[0], columns[1])
        for c in range(3):
            out_ref[pl.ds(192 * j + c, 64, stride=3), :] = result[:, 128 * c : 128 * c + 128]


def middle_kernel(anchor, band_ref, r_ref, over_px_ref, front_tw_ref, within_ref, back_ref, back_tw_ref, final_ref, out_ref):
    data = jnp.concatenate([r_ref[pl.ds(c, 256, stride=3), :] for c in range(3)], 1)
    high, low = split(data)
    turned = table_times(dot_nn, over_px_ref[...], high, low)
    cos_tw, sin_tw = front_tw_ref[:256, :], front_tw_ref[256:, :]
    lane = lax.broadcasted_iota(jnp.int32, (1, 128), 1)
    sign = jnp.where(lane < 64, -1.0, 1.0).astype(F32)
    spectrum = []
    for c in range(3):
        p, q = turned[:256, 128 * c : 128 * c + 128], turned[256:, 128 * c : 128 * c + 128]
        a = p * cos_tw + q * sin_tw
        b = q * cos_tw - p * sin_tw
        u_high, u_low = split(a + pltpu.roll(b, 64, axis=1) * sign)
        out = table_times(dot_nt, within_ref[...], u_high, u_low)
        spectrum.append((out[:64], out[64:]))
    sub = lax.broadcasted_iota(jnp.int32, (8, 128), 0)
    lanes = lax.broadcasted_iota(jnp.int32, (8, 128), 1)
    band = jnp.zeros((8, 128), jnp.int32)
    count_one = jnp.int32(0)
    for y in range(8):
        band = jnp.where(sub == y, band_ref[y], band)
        count_one = count_one + band_ref[y]
    lane_band = (lanes // 32) % 2
    in_band = band == lane_band
    select = jnp.concatenate(
        [jnp.where(jnp.logical_and(in_band, lanes % 32 == k1), 1.0, 0.0).astype(F32) for k1 in range(32)], 0
    ).astype(BF16)
    one_f = jnp.full((8, 128), count_one, jnp.int32).astype(F32)
    count = jnp.where(lane_band == 1, one_f, 8.0 - one_f)
    weight = 1.0 / (count * float(NX * NZ * 1024))
    row64 = lax.broadcasted_iota(jnp.int32, (64, 128), 0)
    lane64 = lax.broadcasted_iota(jnp.int32, (64, 128), 1)
    scale = jnp.concatenate([weight] * 8, 0)
    scale = jnp.where(jnp.logical_and(anchor, row64 < 32), 0.5 * scale, scale)
    mean = jnp.logical_and(anchor, jnp.logical_and(row64 == 0, lane64 % 32 == 0))
    scale = jnp.where(mean, 0.0, scale)
    banded = []
    for left, right in PAIR_LIST:
        lr, li = spectrum[left]
        rr, ri = spectrum[right]
        values = [lr * rr + li * ri]
        if left != right:
            values.append(lr * ri - li * rr)
        sums = []
        for value in values:
            value_high, value_low = split(value)
            sums.append((dot_nn(value_high, select) + dot_nn(value_low, select)) * scale)
        if left == right:
            sums.append(jnp.zeros((64, 128), F32))
        banded.append(sums)
    columns = []
    for k in range(2):
        for sp in range(3):
            cut = slice(32 * k, 32 * k + 32)
            columns.append(jnp.concatenate([banded[2 * sp + s2][part][cut] for s2 in range(2) for part in range(2)], 0))
    x_high, x_low = split(jnp.concatenate(columns, 1))
    v = table_times(dot_nn, back_ref[...], x_high, x_low)
    pad = jnp.zeros((32, 128), F32)
    for py in range(8):
        t1 = back_tw_ref[pl.ds(8 * py, 8), :]
        t2 = back_tw_ref[pl.ds(64 + 8 * py, 8), :]
        re_rows, im_rows = [], []
        for column in range(6):
            cut = slice(128 * column, 128 * column + 128)
            vr, vi = v[16 * py : 16 * py + 8, cut], v[16 * py + 8 : 16 * py + 16, cut]
            re_rows.append(vr * t1 - vi * t2)
            im_rows.append(vr * t2 + vi * t1)
        rows_high, rows_low = split(jnp.concatenate(re_rows + im_rows + [pad], 0))
        out = table_times(dot_nt, final_ref[...], rows_high, rows_low)
        for b in range(2):
            out_ref[pl.ds(2 * py + b, 32, stride=16), :] = out[32 * b : 32 * b + 32]


def span_inverse_kernel(r_ref, table_ref, twiddle_ref, out_ref):
    table = table_ref[...]
    lhs = []
    for b in range(2):
        rows = r_ref[pl.ds(b, 256, stride=2), :].T
        for jp in range(2):
            lhs.append(rows[:96, 128 * jp : 128 * jp + 128])
    high, low = split(jnp.concatenate(lhs, 0))
    sums = dot_nn(high, table[:128]) + dot_nn(high, table[128:]) + dot_nn(low, table[:128])
    sub = lax.broadcasted_iota(jnp.int32, (8, 128), 0)
    for b in range(2):
        for sp in range(3):
            y = []
            for k1 in range(8):
                j, k = k1 // 2, k1 % 2
                row = (b * 2 + j // 2) * 96 + k * 24 + sp * 8
                col = (j % 2) * 256
                rc, rs = sums[row : row + 8, col : col + 128], sums[row : row + 8, col + 128 : col + 256]
                ic, is_ = sums[row + 48 : row + 56, col : col + 128], sums[row + 48 : row + 56, col + 128 : col + 256]
                zr, zi = rc - is_, rs + ic
                c, s = twiddle_ref[pl.ds(k1, 1), :], twiddle_ref[pl.ds(8 + k1, 1), :]
                if k1 == 0:
                    y.append((zr, None))
                elif k1 == 4:
                    y.append((zr * c - zi * s, None))
                else:
                    y.append((zr * c - zi * s, zr * s + zi * c))
            a = [None] + [y[k][0] + y[8 - k][0] for k in (1, 2, 3)]
            d = [None] + [y[k][1] - y[8 - k][1] for k in (1, 2, 3)]
            up, um = y[0][0] + y[4][0], y[0][0] - y[4][0]
            ap, am = a[1] + a[3], ROOT_HALF * (a[1] - a[3])
            dm, dp = d[1] - d[3], ROOT_HALF * (d[1] + d[3])
            upp, upm = up + a[2], up - a[2]
            ump, umm = um + d[2], um - d[2]
            outs = [
                upp + ap,
                umm + am - dp,
                upm - dm,
                ump - am - dp,
                upp - ap,
                umm - am + dp,
                upm + dm,
                ump + am + dp,
            ]
            for half in range(4):
                v0, v1 = outs[2 * half], outs[2 * half + 1]
                base = (sp * 2 * 2 + b) * 32 + half * 8
                out_ref[pl.ds(base, 8), :] = jnp.where(sub < 4, v0, pltpu.roll(v1, 4, axis=0))
                out_ref[pl.ds(base + 64, 8), :] = jnp.where(sub < 4, pltpu.roll(v0, 4, axis=0), v1)


def vmem(count):
    return [pl.BlockSpec(memory_space=pltpu.VMEM)] * count


def call(kernel, out_shape, in_specs, name):
    return pl.pallas_call(
        kernel,
        out_shape=jax.ShapeDtypeStruct(out_shape, F32),
        in_specs=in_specs,
        out_specs=pl.BlockSpec(memory_space=pltpu.VMEM),
        name=name,
        compiler_params=pltpu.CompilerParams(vmem_limit_bytes=16 * 1024 * 1024),
    )


def run_span_forward(velocity):
    twiddle, table = span_forward_tables()
    return call(span_forward_kernel, (768, 128), vmem(3), "span_forward")(velocity, twiddle, table)


def run_middle(received, band_of, anchor=None):
    def kernel(band_ref, *refs):
        if anchor is None:
            at_anchor = jnp.logical_and(lax.axis_index("px") == 0, lax.axis_index("py") == 0)
        else:
            at_anchor = anchor
        middle_kernel(at_anchor, band_ref, *refs)

    specs = [pl.BlockSpec(memory_space=pltpu.SMEM)] + vmem(7)
    return call(kernel, (512, 128), specs, "middle")(band_of, received, *middle_tables())


def run_span_inverse(received):
    return call(span_inverse_kernel, (384, 128), vmem(3), "span_inverse")(received, *span_inverse_tables())


def per_device(velocity, band_of):
    sent = run_span_forward(velocity.reshape(768, 128))
    received = lax.all_to_all(sent.reshape(256, 1, 384), ("px", "py"), 0, 0, tiled=True)
    back = run_middle(received.reshape(768, 128), band_of)
    gathered = lax.all_to_all(back.reshape(256, 1, 256), ("px", "py"), 0, 0, tiled=True)
    out = run_span_inverse(gathered.reshape(512, 128))
    return out.reshape(6, 2, 8, 4, 128).transpose(0, 1, 3, 2, 4).reshape(6, 2, 4, 1024)


def solution(mesh):
    in_specs = (P(None, "px", "py", None), P())
    out_specs = P(None, None, ("px", "py"), None)
    return jax.shard_map(per_device, mesh=mesh, in_specs=in_specs, out_specs=out_specs, check_vma=False)
```

```python
import math

import jax
import jax.numpy as jnp
import numpy as np
from jax import lax
from jax.experimental import pallas as pl
from jax.experimental.pallas import tpu as pltpu
from jax.sharding import PartitionSpec as P

NX = 1024
NZ = 1024
NY = 8
NB = 2
PAIR_LIST = ((0, 0), (0, 1), (0, 2), (1, 1), (1, 2), (2, 2))
ROOT_HALF = math.sqrt(0.5)
F32 = jnp.float32
BF16 = jnp.bfloat16


def wave(rows, cols, length):
    angle = 2.0 * np.pi * (np.multiply.outer(rows, cols) % length) / length
    return np.cos(angle), np.sin(angle)


def stacked_split(table):
    high = table.astype(np.float32).astype(jnp.bfloat16)
    low = (table - high.astype(np.float64)).astype(np.float32).astype(jnp.bfloat16)
    return np.concatenate((high, low), 0)


def span_forward_tables():
    cos_tw, sin_tw = wave(np.arange(8), np.arange(128), 1024)
    twiddle = np.concatenate((cos_tw, sin_tw), 0).astype(np.float32)
    cos_t, sin_t = wave(np.arange(64), np.arange(128), 128)
    return twiddle, stacked_split(np.concatenate((cos_t, sin_t), 1))


def middle_tables():
    base = np.arange(32)
    cos32, sin32 = wave(base, base, 32)
    eye8 = np.eye(8)
    over_px = stacked_split(np.concatenate((np.kron(cos32, eye8), np.kron(-sin32, eye8)), 0))
    cos_tw, sin_tw = wave(base, base, 1024)
    spread = lambda t: np.repeat(np.tile(t, (1, 4)), 8, 0)
    front_twiddle = np.concatenate((spread(cos_tw), spread(sin_tw)), 0).astype(np.float32)
    eye2 = np.eye(2)
    block = lambda t: np.kron(eye2, t)
    within = stacked_split(np.block([[block(cos32), block(sin32)], [block(-sin32), block(cos32)]]))
    back = np.zeros((8, 2, 2, 4, 2, 2, 32))
    for py in range(8):
        for i in range(4):
            c, s = cos32[4 * py + i], sin32[4 * py + i]
            for s2 in range(2):
                back[py, 0, s2, i, s2, 0] = c
                back[py, 0, s2, i, s2, 1] = -s
                back[py, 1, s2, i, s2, 0] = s
                back[py, 1, s2, i, s2, 1] = c
    back = stacked_split(back.reshape(128, 128))
    first = np.zeros((8, 2, 4, 2, 2, 32))
    second = np.zeros((8, 2, 4, 2, 2, 32))
    for py in range(8):
        for i in range(4):
            c, s = cos_tw[4 * py + i], sin_tw[4 * py + i]
            first[py, :, i, 0] = c
            first[py, :, i, 1] = -s
            second[py, :, i, 0] = s
            second[py, :, i, 1] = c
    back_twiddle = np.concatenate((first.reshape(64, 128), second.reshape(64, 128)), 0).astype(np.float32)
    final = stacked_split(np.concatenate((np.kron(eye2, cos32), np.kron(eye2, sin32)), 1))
    return over_px, front_twiddle, within, back, back_twiddle, final


def span_inverse_tables():
    cos_t, sin_t = wave(np.arange(64), np.arange(128), 128)
    one = 2.0 * np.concatenate((cos_t, sin_t), 1)
    table = stacked_split(np.kron(np.eye(2), one))
    cos_tw, sin_tw = wave(np.arange(8), np.arange(128), 1024)
    return table, np.concatenate((cos_tw, sin_tw), 0).astype(np.float32)


def split(x):
    high = x.astype(BF16)
    return high, (x - high.astype(F32)).astype(BF16)


def dot_nn(a, b):
    return lax.dot_general(a, b, (((1,), (0,)), ((), ())), preferred_element_type=F32)


def dot_nt(a, b):
    return lax.dot_general(a, b, (((1,), (1,)), ((), ())), preferred_element_type=F32)


def table_times(dot, table, high, low):
    rows = table.shape[0] // 2
    both = dot(table, high)
    return both[:rows] + both[rows:] + dot(table[:rows], low)


def span_forward_kernel(v_hbm, twiddle_hbm, table_hbm, out_ref, v_ref, twiddle_ref, table_ref, sems):
    copies = [
        pltpu.make_async_copy(v_hbm.at[pl.ds(256 * c, 256)], v_ref.at[pl.ds(256 * c, 256)], sems.at[c]) for c in range(3)
    ]
    copies.append(pltpu.make_async_copy(twiddle_hbm, twiddle_ref, sems.at[3]))
    copies.append(pltpu.make_async_copy(table_hbm, table_ref, sems.at[4]))
    for c in (3, 0, 4, 1, 2):
        copies[c].start()
    copies[3].wait()
    for c in range(3):
        copies[c].wait()
        x = [v_ref[pl.ds(256 * c + s, 32, stride=8), :] for s in range(8)]
        e = [x[s] + x[s + 4] for s in range(4)]
        o = [x[s] - x[s + 4] for s in range(4)]
        e02, e13 = e[0] + e[2], e[1] + e[3]
        om, op = ROOT_HALF * (o[1] - o[3]), ROOT_HALF * (o[1] + o[3])
        e02m, e13m = e[0] - e[2], e[1] - e[3]
        one = (o[0] + om, -(o[2] + op))
        three = (o[0] - om, o[2] - op)
        spec = [
            (e02 + e13, None),
            one,
            (e02m, -e13m),
            three,
            (e02 - e13, None),
            (three[0], -three[1]),
            (e02m, e13m),
            (one[0], -one[1]),
        ]
        parts = []
        for k1 in range(8):
            re, im = spec[k1]
            cos_tw = twiddle_ref[pl.ds(k1, 1), :]
            sin_tw = twiddle_ref[pl.ds(8 + k1, 1), :]
            if k1 == 0:
                new_re, new_im = re, jnp.zeros_like(re)
            elif im is None:
                new_re, new_im = re * cos_tw, -(re * sin_tw)
            else:
                new_re, new_im = re * cos_tw + im * sin_tw, im * cos_tw - re * sin_tw
            parts.append((split(new_re), split(new_im)))
        columns = []
        for level in range(2):
            rows = []
            for j in range(4):
                for turn in range(2):
                    for k1 in (2 * j, 2 * j + 1):
                        re, im = parts[k1][0][level], parts[k1][1][level]
                        rows.append(jnp.concatenate((re, im) if turn == 0 else (im, -re), 1))
            columns.append(jnp.concatenate(rows, 0))
        if c == 0:
            copies[4].wait()
        result = table_times(dot_nt, table_ref[...], columns[0], columns[1])
        for j in range(4):
            out_ref[pl.ds(192 * j + c, 64, stride=3), :] = result[:, 128 * j : 128 * j + 128]


def middle_kernel(
    anchor, band_hbm, r_ref, over_px_ref, front_tw_ref, within_ref, back_ref, back_tw_ref, final_ref, out_ref, band_ref, sem
):
    band_copy = pltpu.make_async_copy(band_hbm, band_ref, sem)
    band_copy.start()
    data = jnp.concatenate([r_ref[pl.ds(c, 256, stride=3), :] for c in range(3)], 1)
    high, low = split(data)
    turned = table_times(dot_nn, over_px_ref[...], high, low)
    cos_tw, sin_tw = front_tw_ref[:256, :], front_tw_ref[256:, :]
    lane = lax.broadcasted_iota(jnp.int32, (1, 128), 1)
    sign = jnp.where(lane < 64, -1.0, 1.0).astype(F32)
    spectrum = []
    for c in range(3):
        p, q = turned[:256, 128 * c : 128 * c + 128], turned[256:, 128 * c : 128 * c + 128]
        a = p * cos_tw + q * sin_tw
        b = q * cos_tw - p * sin_tw
        u_high, u_low = split(a + pltpu.roll(b, 64, axis=1) * sign)
        out = table_times(dot_nt, within_ref[...], u_high, u_low)
        spectrum.append((out[:64], out[64:]))
    sub = lax.broadcasted_iota(jnp.int32, (8, 128), 0)
    lanes = lax.broadcasted_iota(jnp.int32, (8, 128), 1)
    band_copy.wait()
    band = jnp.zeros((8, 128), jnp.int32)
    count_one = jnp.int32(0)
    for y in range(8):
        band = jnp.where(sub == y, band_ref[y], band)
        count_one = count_one + band_ref[y]
    lane_band = (lanes // 32) % 2
    in_band = band == lane_band
    select = jnp.concatenate(
        [jnp.where(jnp.logical_and(in_band, lanes % 32 == k1), 1.0, 0.0).astype(F32) for k1 in range(32)], 0
    ).astype(BF16)
    one_f = jnp.full((8, 128), count_one, jnp.int32).astype(F32)
    count = jnp.where(lane_band == 1, one_f, 8.0 - one_f)
    weight = 1.0 / (count * float(NX * NZ * 1024))
    row64 = lax.broadcasted_iota(jnp.int32, (64, 128), 0)
    lane64 = lax.broadcasted_iota(jnp.int32, (64, 128), 1)
    scale = jnp.concatenate([weight] * 8, 0)
    scale = jnp.where(jnp.logical_and(anchor, row64 < 32), 0.5 * scale, scale)
    mean = jnp.logical_and(anchor, jnp.logical_and(row64 == 0, lane64 % 32 == 0))
    scale = jnp.where(mean, 0.0, scale)
    banded = []
    for left, right in PAIR_LIST:
        lr, li = spectrum[left]
        rr, ri = spectrum[right]
        values = [lr * rr + li * ri]
        if left != right:
            values.append(lr * ri - li * rr)
        sums = []
        for value in values:
            value_high, value_low = split(value)
            sums.append((dot_nn(value_high, select) + dot_nn(value_low, select)) * scale)
        if left == right:
            sums.append(jnp.zeros((64, 128), F32))
        banded.append(sums)
    columns = []
    for k in range(2):
        for sp in range(3):
            cut = slice(32 * k, 32 * k + 32)
            columns.append(jnp.concatenate([banded[2 * sp + s2][part][cut] for s2 in range(2) for part in range(2)], 0))
    x_high, x_low = split(jnp.concatenate(columns, 1))
    v = table_times(dot_nn, back_ref[...], x_high, x_low)
    pad = jnp.zeros((32, 128), F32)
    for py in range(8):
        t1 = back_tw_ref[pl.ds(8 * py, 8), :]
        t2 = back_tw_ref[pl.ds(64 + 8 * py, 8), :]
        re_rows, im_rows = [], []
        for column in range(6):
            cut = slice(128 * column, 128 * column + 128)
            vr, vi = v[16 * py : 16 * py + 8, cut], v[16 * py + 8 : 16 * py + 16, cut]
            re_rows.append(vr * t1 - vi * t2)
            im_rows.append(vr * t2 + vi * t1)
        rows_high, rows_low = split(jnp.concatenate(re_rows + im_rows + [pad], 0))
        out = table_times(dot_nt, final_ref[...], rows_high, rows_low)
        for b in range(2):
            out_ref[pl.ds(2 * py + b, 32, stride=16), :] = out[32 * b : 32 * b + 32]


def span_inverse_kernel(r_ref, table_ref, twiddle_ref, out_hbm, out_ref, sems):
    copies = []
    table = table_ref[...]
    lhs = []
    for b in range(2):
        rows = r_ref[pl.ds(b, 256, stride=2), :].T
        for jp in range(2):
            lhs.append(rows[:96, 128 * jp : 128 * jp + 128])
    high, low = split(jnp.concatenate(lhs, 0))
    sums = dot_nn(high, table[:128]) + dot_nn(high, table[128:]) + dot_nn(low, table[:128])
    sub = lax.broadcasted_iota(jnp.int32, (8, 128), 0)
    for sp in range(3):
        for b in range(2):
            y = []
            for k1 in range(8):
                j, k = k1 // 2, k1 % 2
                row = (b * 2 + j // 2) * 96 + k * 24 + sp * 8
                col = (j % 2) * 256
                rc, rs = sums[row : row + 8, col : col + 128], sums[row : row + 8, col + 128 : col + 256]
                ic, is_ = sums[row + 48 : row + 56, col : col + 128], sums[row + 48 : row + 56, col + 128 : col + 256]
                zr, zi = rc - is_, rs + ic
                c, s = twiddle_ref[pl.ds(k1, 1), :], twiddle_ref[pl.ds(8 + k1, 1), :]
                if k1 == 0:
                    y.append((zr, None))
                elif k1 == 4:
                    y.append((zr * c - zi * s, None))
                else:
                    y.append((zr * c - zi * s, zr * s + zi * c))
            a = [None] + [y[k][0] + y[8 - k][0] for k in (1, 2, 3)]
            d = [None] + [y[k][1] - y[8 - k][1] for k in (1, 2, 3)]
            up, um = y[0][0] + y[4][0], y[0][0] - y[4][0]
            ap, am = a[1] + a[3], ROOT_HALF * (a[1] - a[3])
            dm, dp = d[1] - d[3], ROOT_HALF * (d[1] + d[3])
            upp, upm = up + a[2], up - a[2]
            ump, umm = um + d[2], um - d[2]
            outs = [
                upp + ap,
                umm + am - dp,
                upm - dm,
                ump - am - dp,
                upp - ap,
                umm - am + dp,
                upm + dm,
                ump + am + dp,
            ]
            for half in range(4):
                v0, v1 = outs[2 * half], outs[2 * half + 1]
                base = (sp * 2 * 2 + b) * 32 + half * 8
                out_ref[pl.ds(base, 8), :] = jnp.where(sub < 4, v0, pltpu.roll(v1, 4, axis=0))
                out_ref[pl.ds(base + 64, 8), :] = jnp.where(sub < 4, pltpu.roll(v0, 4, axis=0), v1)
        block = pl.ds(128 * sp, 128)
        copies.append(pltpu.make_async_copy(out_ref.at[block], out_hbm.at[block], sems.at[sp]))
        copies[-1].start()
    for copy in copies:
        copy.wait()


def spaces(*kinds):
    return [pl.BlockSpec(memory_space=kind) for kind in kinds]


VMEM, HBM = pltpu.VMEM, pltpu.HBM


def call(kernel, out_shape, in_specs, name, out_space=VMEM, scratch=()):
    return pl.pallas_call(
        kernel,
        out_shape=jax.ShapeDtypeStruct(out_shape, F32),
        in_specs=in_specs,
        out_specs=pl.BlockSpec(memory_space=out_space),
        scratch_shapes=list(scratch),
        name=name,
        compiler_params=pltpu.CompilerParams(vmem_limit_bytes=16 * 1024 * 1024),
    )


def in_hbm(x):
    return pltpu.with_memory_space_constraint(jnp.asarray(x), HBM)


def run_span_forward(velocity):
    twiddle, table = span_forward_tables()
    scratch = (VMEM((768, 128), F32), VMEM(twiddle.shape, F32), VMEM(table.shape, BF16), pltpu.SemaphoreType.DMA((5,)))
    run = call(span_forward_kernel, (768, 128), spaces(HBM, HBM, HBM), "span_forward", scratch=scratch)
    return run(in_hbm(velocity), in_hbm(twiddle), in_hbm(table))


def run_middle(received, band_of, anchor=None):
    def kernel(*refs):
        if anchor is None:
            at_anchor = jnp.logical_and(lax.axis_index("px") == 0, lax.axis_index("py") == 0)
        else:
            at_anchor = anchor
        middle_kernel(at_anchor, *refs)

    scratch = (pltpu.SMEM((8,), jnp.int32), pltpu.SemaphoreType.DMA)
    run = call(kernel, (512, 128), spaces(HBM, *[VMEM] * 7), "middle", scratch=scratch)
    return run(in_hbm(band_of), received, *middle_tables())


def run_span_inverse(received):
    scratch = (VMEM((384, 128), F32), pltpu.SemaphoreType.DMA((3,)))
    run = call(span_inverse_kernel, (384, 128), spaces(VMEM, VMEM, VMEM), "span_inverse", HBM, scratch)
    return run(received, *span_inverse_tables())


def per_device(velocity, band_of):
    sent = run_span_forward(velocity.reshape(768, 128))
    received = lax.all_to_all(sent.reshape(256, 1, 384), ("px", "py"), 0, 0, tiled=True)
    back = run_middle(received.reshape(768, 128), band_of)
    gathered = lax.all_to_all(back.reshape(256, 1, 256), ("px", "py"), 0, 0, tiled=True)
    out = run_span_inverse(gathered.reshape(512, 128))
    return out.reshape(6, 2, 8, 4, 128).transpose(0, 1, 3, 2, 4).reshape(6, 2, 4, 1024)


def solution(mesh):
    in_specs = (P(None, "px", "py", None), P())
    out_specs = P(None, None, ("px", "py"), None)
    return jax.shard_map(per_device, mesh=mesh, in_specs=in_specs, out_specs=out_specs, check_vma=False)
```

```python
import math

import jax
import jax.numpy as jnp
import numpy as np
from jax import lax
from jax.experimental import pallas as pl
from jax.experimental.pallas import tpu as pltpu
from jax.sharding import PartitionSpec as P

NX = 1024
NZ = 1024
NY = 8
NB = 2
PAIR_LIST = ((0, 0), (0, 1), (0, 2), (1, 1), (1, 2), (2, 2))
ROOT_HALF = math.sqrt(0.5)
F32 = jnp.float32
BF16 = jnp.bfloat16


def wave(rows, cols, length):
    angle = 2.0 * np.pi * (np.multiply.outer(rows, cols) % length) / length
    return np.cos(angle), np.sin(angle)


def three_part(table, axis=1):
    high = table.astype(np.float32).astype(jnp.bfloat16)
    low = (table - high.astype(np.float64)).astype(np.float32).astype(jnp.bfloat16)
    return np.concatenate((high, high, low), axis)


def paired(table):
    parts = three_part(table)
    width = table.shape[1]
    return np.concatenate((parts[:, : 2 * width], np.concatenate((parts[:, 2 * width :], 0 * parts[:, :width]), 1)), 0)


def span_forward_tables():
    cos_tw, sin_tw = wave(np.arange(8), np.arange(128), 1024)
    twiddle = np.concatenate((cos_tw, sin_tw), 0).astype(np.float32)
    cos_t, sin_t = wave(np.arange(64), np.arange(128), 128)
    parts = three_part(np.concatenate((cos_t, sin_t), 1))
    return twiddle, np.concatenate((parts[:, :256], parts[:, 512:]), 0)


def middle_tables():
    base = np.arange(32)
    cos32, sin32 = wave(base, base, 32)
    eye8 = np.eye(8)
    over_px = three_part(np.concatenate((np.kron(cos32[:17], eye8), np.kron(-sin32[1:16], eye8)), 0))
    cos_tw, sin_tw = wave(base, base, 1024)
    spread = lambda t: np.repeat(np.tile(t, (1, 4)), 8, 0)
    turn_sign = np.where(base < 16, 1.0, -1.0)[:, None]
    lane_sign = np.where(np.arange(128) < 64, 1.0, -1.0)
    front_twiddle = np.concatenate(
        (
            spread(cos_tw),
            spread(turn_sign * sin_tw),
            spread(turn_sign * cos_tw) * lane_sign,
            -spread(sin_tw) * lane_sign,
        ),
        0,
    ).astype(np.float32)
    eye2 = np.eye(2)
    block = lambda t: np.kron(eye2, t)
    within = paired(np.block([[block(cos32), block(sin32)], [block(-sin32), block(cos32)]]))
    back = np.zeros((8, 2, 2, 4, 2, 2, 32))
    for py in range(8):
        for i in range(4):
            c, s = cos32[4 * py + i], sin32[4 * py + i]
            for s2 in range(2):
                back[py, 0, s2, i, s2, 0] = c
                back[py, 0, s2, i, s2, 1] = -s
                back[py, 1, s2, i, s2, 0] = s
                back[py, 1, s2, i, s2, 1] = c
    back = paired(back.reshape(128, 128))
    first = np.zeros((8, 2, 4, 2, 2, 32))
    second = np.zeros((8, 2, 4, 2, 2, 32))
    for py in range(8):
        for i in range(4):
            c, s = cos_tw[4 * py + i], sin_tw[4 * py + i]
            first[py, :, i, 0] = c
            first[py, :, i, 1] = -s
            second[py, :, i, 0] = s
            second[py, :, i, 1] = c
    back_twiddle = np.concatenate((first.reshape(64, 128), second.reshape(64, 128)), 0).astype(np.float32)
    final = paired(np.concatenate((np.kron(eye2, cos32), np.kron(eye2, sin32)), 1))
    return over_px, front_twiddle, within, back, back_twiddle, final


def span_inverse_tables():
    cos_t, sin_t = wave(np.arange(64), np.arange(128), 128)
    one = 2.0 * np.concatenate((cos_t, sin_t), 1)
    table = three_part(np.kron(np.eye(2), one), 0)
    cos_tw, sin_tw = wave(np.arange(8), np.arange(128), 1024)
    return table, np.concatenate((cos_tw, sin_tw), 0).astype(np.float32)


def split(x):
    high = x.astype(BF16)
    return high, (x - high.astype(F32)).astype(BF16)


def joined(x, axis):
    high, low = split(x)
    return jnp.concatenate((high, low, high), axis)


def halves_added(x):
    rows = x.shape[0] // 2
    return x[:rows] + x[rows:]


def dot_nn(a, b):
    return lax.dot_general(a, b, (((1,), (0,)), ((), ())), preferred_element_type=F32)


def dot_nt(a, b):
    return lax.dot_general(a, b, (((1,), (1,)), ((), ())), preferred_element_type=F32)


def span_forward_kernel(v_hbm, twiddle_hbm, table_hbm, out_ref, v_ref, twiddle_ref, table_ref, sems):
    copies = [
        pltpu.make_async_copy(v_hbm, v_ref, sems.at[0]),
        pltpu.make_async_copy(twiddle_hbm, twiddle_ref, sems.at[1]),
        pltpu.make_async_copy(table_hbm, table_ref, sems.at[2]),
    ]
    for copy in copies:
        copy.start()
    for copy in copies:
        copy.wait()
    x = [v_ref[pl.ds(s, 96, stride=8), :] for s in range(8)]
    e = [x[s] + x[s + 4] for s in range(4)]
    o = [x[s] - x[s + 4] for s in range(4)]
    e02, e13 = e[0] + e[2], e[1] + e[3]
    om, op = ROOT_HALF * (o[1] - o[3]), ROOT_HALF * (o[1] + o[3])
    e02m, e13m = e[0] - e[2], e[1] - e[3]
    one = (o[0] + om, -(o[2] + op))
    three = (o[0] - om, o[2] - op)
    spec = [
        (e02 + e13, None),
        one,
        (e02m, -e13m),
        three,
        (e02 - e13, None),
        (three[0], -three[1]),
        (e02m, e13m),
        (one[0], -one[1]),
    ]
    parts = []
    for k1 in range(8):
        re, im = spec[k1]
        cos_tw = twiddle_ref[pl.ds(k1, 1), :]
        sin_tw = twiddle_ref[pl.ds(8 + k1, 1), :]
        if k1 == 0:
            new_re, new_im = re, jnp.zeros_like(re)
        elif im is None:
            new_re, new_im = re * cos_tw, -(re * sin_tw)
        else:
            new_re, new_im = re * cos_tw + im * sin_tw, im * cos_tw - re * sin_tw
        parts.append((split(new_re), split(new_im)))
    table = table_ref[...]
    for j in range(4):
        columns = []
        for level in range(2):
            rows = []
            for c in range(3):
                cut = slice(32 * c, 32 * c + 32)
                for turn in range(2):
                    for k1 in (2 * j, 2 * j + 1):
                        re, im = parts[k1][0][level][cut], parts[k1][1][level][cut]
                        rows.append(jnp.concatenate((re, im) if turn == 0 else (im, -re), 1))
            columns.append(jnp.concatenate(rows, 0))
        result = halves_added(dot_nt(table, columns[0])) + dot_nt(table[:64], columns[1])
        for c in range(3):
            out_ref[pl.ds(192 * j + c, 64, stride=3), :] = result[:, 128 * c : 128 * c + 128]


def middle_kernel(
    anchor, band_hbm, r_ref, over_px_ref, front_tw_ref, within_ref, back_ref, back_tw_ref, final_ref, out_ref, band_ref, sem
):
    band_copy = pltpu.make_async_copy(band_hbm, band_ref, sem)
    band_copy.start()
    data = jnp.concatenate([r_ref[pl.ds(c, 256, stride=3), :] for c in range(3)], 1)
    turned = dot_nn(over_px_ref[...], joined(data, 0))
    spectrum = []
    for c in range(3):
        cut = slice(128 * c, 128 * c + 128)
        rows = []
        for k1 in range(32):
            t1, t2, t3, t4 = [front_tw_ref[pl.ds(256 * t + 8 * k1, 8), :] for t in range(4)]
            m = min(k1, 32 - k1)
            p = turned[8 * m : 8 * m + 8, cut]
            if m % 16 == 0:
                rows.append(p * t1 + pltpu.roll(p * t4, 64, axis=1))
            else:
                q = turned[128 + 8 * m : 136 + 8 * m, cut]
                rows.append((p * t1 + q * t2) + pltpu.roll(q * t3 + p * t4, 64, axis=1))
        u = jnp.concatenate(split(jnp.concatenate(rows, 0)), 1)
        out = halves_added(dot_nt(within_ref[...], u))
        spectrum.append((out[:64], out[64:]))
    sub = lax.broadcasted_iota(jnp.int32, (8, 128), 0)
    lanes = lax.broadcasted_iota(jnp.int32, (8, 128), 1)
    band_copy.wait()
    band = jnp.zeros((8, 128), jnp.int32)
    count_one = jnp.int32(0)
    for y in range(8):
        band = jnp.where(sub == y, band_ref[y], band)
        count_one = count_one + band_ref[y]
    lane_band = (lanes // 32) % 2
    in_band = band == lane_band
    select = jnp.concatenate(
        [jnp.where(jnp.logical_and(in_band, lanes % 32 == k1), 1.0, 0.0).astype(F32) for k1 in range(32)], 0
    ).astype(BF16)
    select = jnp.concatenate((select, select), 0)
    one_f = jnp.full((8, 128), count_one, jnp.int32).astype(F32)
    count = jnp.where(lane_band == 1, one_f, 8.0 - one_f)
    weight = 1.0 / (count * float(NX * NZ * 1024))
    row64 = lax.broadcasted_iota(jnp.int32, (64, 128), 0)
    lane64 = lax.broadcasted_iota(jnp.int32, (64, 128), 1)
    scale = jnp.concatenate([weight] * 8, 0)
    scale = jnp.where(jnp.logical_and(anchor, row64 < 32), 0.5 * scale, scale)
    mean = jnp.logical_and(anchor, jnp.logical_and(row64 == 0, lane64 % 32 == 0))
    scale = jnp.where(mean, 0.0, scale)
    banded = []
    for left, right in PAIR_LIST:
        lr, li = spectrum[left]
        rr, ri = spectrum[right]
        values = [lr * rr + li * ri]
        if left != right:
            values.append(lr * ri - li * rr)
        sums = []
        for value in values:
            sums.append(dot_nn(jnp.concatenate(split(value), 1), select) * scale)
        if left == right:
            sums.append(jnp.zeros((64, 128), F32))
        banded.append(sums)
    columns = []
    for k in range(2):
        for sp in range(3):
            cut = slice(32 * k, 32 * k + 32)
            columns.append(jnp.concatenate([banded[2 * sp + s2][part][cut] for s2 in range(2) for part in range(2)], 0))
    v = halves_added(dot_nn(back_ref[...], jnp.concatenate(split(jnp.concatenate(columns, 1)), 0)))
    middle_tail(v, back_tw_ref, final_ref, out_ref)


def middle_tail(v, back_tw_ref, final_ref, out_ref):
    pad = jnp.zeros((32, 128), F32)
    for py in range(8):
        t1 = back_tw_ref[pl.ds(8 * py, 8), :]
        t2 = back_tw_ref[pl.ds(64 + 8 * py, 8), :]
        re_rows, im_rows = [], []
        for column in range(6):
            cut = slice(128 * column, 128 * column + 128)
            vr, vi = v[16 * py : 16 * py + 8, cut], v[16 * py + 8 : 16 * py + 16, cut]
            re_rows.append(vr * t1 - vi * t2)
            im_rows.append(vr * t2 + vi * t1)
        out = halves_added(dot_nt(final_ref[...], jnp.concatenate(split(jnp.concatenate(re_rows + im_rows + [pad], 0)), 1)))
        for b in range(2):
            out_ref[pl.ds(2 * py + b, 32, stride=16), :] = out[32 * b : 32 * b + 32]


def span_inverse_kernel(r_ref, table_ref, twiddle_ref, out_hbm, out_ref, sems):
    copies = []
    table = table_ref[...]
    lhs = []
    for b in range(2):
        rows = r_ref[pl.ds(b, 256, stride=2), :].T
        for jp in range(2):
            lhs.append(rows[:96, 128 * jp : 128 * jp + 128])
    sums = dot_nn(joined(jnp.concatenate(lhs, 0), 1), table)
    sub = lax.broadcasted_iota(jnp.int32, (8, 128), 0)
    for sp in range(3):
        for b in range(2):
            y = []
            for k1 in range(8):
                j, k = k1 // 2, k1 % 2
                row = (b * 2 + j // 2) * 96 + k * 24 + sp * 8
                col = (j % 2) * 256
                rc, rs = sums[row : row + 8, col : col + 128], sums[row : row + 8, col + 128 : col + 256]
                ic, is_ = sums[row + 48 : row + 56, col : col + 128], sums[row + 48 : row + 56, col + 128 : col + 256]
                zr, zi = rc - is_, rs + ic
                c, s = twiddle_ref[pl.ds(k1, 1), :], twiddle_ref[pl.ds(8 + k1, 1), :]
                if k1 == 0:
                    y.append((zr, None))
                elif k1 == 4:
                    y.append((zr * c - zi * s, None))
                else:
                    y.append((zr * c - zi * s, zr * s + zi * c))
            a = [None] + [y[k][0] + y[8 - k][0] for k in (1, 2, 3)]
            d = [None] + [y[k][1] - y[8 - k][1] for k in (1, 2, 3)]
            up, um = y[0][0] + y[4][0], y[0][0] - y[4][0]
            ap, am = a[1] + a[3], ROOT_HALF * (a[1] - a[3])
            dm, dp = d[1] - d[3], ROOT_HALF * (d[1] + d[3])
            upp, upm = up + a[2], up - a[2]
            ump, umm = um + d[2], um - d[2]
            outs = [
                upp + ap,
                umm + am - dp,
                upm - dm,
                ump - am - dp,
                upp - ap,
                umm - am + dp,
                upm + dm,
                ump + am + dp,
            ]
            for half in range(4):
                v0, v1 = outs[2 * half], outs[2 * half + 1]
                base = (sp * 2 * 2 + b) * 32 + half * 8
                out_ref[pl.ds(base, 8), :] = jnp.where(sub < 4, v0, pltpu.roll(v1, 4, axis=0))
                out_ref[pl.ds(base + 64, 8), :] = jnp.where(sub < 4, pltpu.roll(v0, 4, axis=0), v1)
        block = pl.ds(128 * sp, 128)
        copies.append(pltpu.make_async_copy(out_ref.at[block], out_hbm.at[block], sems.at[sp]))
        copies[-1].start()
    for copy in copies:
        copy.wait()


def spaces(*kinds):
    return [pl.BlockSpec(memory_space=kind) for kind in kinds]


VMEM, HBM = pltpu.VMEM, pltpu.HBM


def call(kernel, out_shape, in_specs, name, out_space=VMEM, scratch=()):
    return pl.pallas_call(
        kernel,
        out_shape=jax.ShapeDtypeStruct(out_shape, F32),
        in_specs=in_specs,
        out_specs=pl.BlockSpec(memory_space=out_space),
        scratch_shapes=list(scratch),
        name=name,
        compiler_params=pltpu.CompilerParams(vmem_limit_bytes=16 * 1024 * 1024),
    )


def in_hbm(x):
    return pltpu.with_memory_space_constraint(jnp.asarray(x), HBM)


def run_span_forward(velocity):
    twiddle, table = span_forward_tables()
    scratch = (VMEM((768, 128), F32), VMEM(twiddle.shape, F32), VMEM(table.shape, BF16), pltpu.SemaphoreType.DMA((3,)))
    run = call(span_forward_kernel, (768, 128), spaces(HBM, HBM, HBM), "span_forward", scratch=scratch)
    return run(in_hbm(velocity), in_hbm(twiddle), in_hbm(table))


def run_middle(received, band_of, anchor=None):
    def kernel(*refs):
        if anchor is None:
            at_anchor = jnp.logical_and(lax.axis_index("px") == 0, lax.axis_index("py") == 0)
        else:
            at_anchor = anchor
        middle_kernel(at_anchor, *refs)

    scratch = (pltpu.SMEM((8,), jnp.int32), pltpu.SemaphoreType.DMA)
    run = call(kernel, (512, 128), spaces(HBM, *[VMEM] * 7), "middle", scratch=scratch)
    return run(in_hbm(band_of), received, *middle_tables())


def run_span_inverse(received):
    scratch = (VMEM((384, 128), F32), pltpu.SemaphoreType.DMA((3,)))
    run = call(span_inverse_kernel, (384, 128), spaces(VMEM, VMEM, VMEM), "span_inverse", HBM, scratch)
    return run(received, *span_inverse_tables())


def per_device(velocity, band_of):
    sent = run_span_forward(velocity.reshape(768, 128))
    received = lax.all_to_all(sent.reshape(256, 1, 384), ("px", "py"), 0, 0, tiled=True)
    back = run_middle(received.reshape(768, 128), band_of)
    gathered = lax.all_to_all(back.reshape(256, 1, 256), ("px", "py"), 0, 0, tiled=True)
    out = run_span_inverse(gathered.reshape(512, 128))
    return out.reshape(6, 2, 8, 4, 128).transpose(0, 1, 3, 2, 4).reshape(6, 2, 4, 1024)


def solution(mesh):
    in_specs = (P(None, "px", "py", None), P())
    out_specs = P(None, None, ("px", "py"), None)
    return jax.shard_map(per_device, mesh=mesh, in_specs=in_specs, out_specs=out_specs, check_vma=False)
```

```python
import math

import jax
import jax.numpy as jnp
import numpy as np
from jax import lax
from jax.experimental import pallas as pl
from jax.experimental.pallas import tpu as pltpu
from jax.sharding import PartitionSpec as P

NX = 1024
NZ = 1024
NY = 8
NB = 2
PAIR_LIST = ((0, 0), (0, 1), (0, 2), (1, 1), (1, 2), (2, 2))
ROOT_HALF = math.sqrt(0.5)
F32 = jnp.float32
BF16 = jnp.bfloat16


def wave(rows, cols, length):
    angle = 2.0 * np.pi * (np.multiply.outer(rows, cols) % length) / length
    return np.cos(angle), np.sin(angle)


def three_part(table, axis=1):
    high = table.astype(np.float32).astype(jnp.bfloat16)
    low = (table - high.astype(np.float64)).astype(np.float32).astype(jnp.bfloat16)
    return np.concatenate((high, high, low), axis)


def paired(table):
    parts = three_part(table)
    width = table.shape[1]
    return np.concatenate((parts[:, : 2 * width], np.concatenate((parts[:, 2 * width :], 0 * parts[:, :width]), 1)), 0)


def span_forward_tables():
    cos_tw, sin_tw = wave(np.arange(8), np.arange(128), 1024)
    twiddle = np.concatenate((cos_tw, sin_tw), 0).astype(np.float32)
    cos_t, sin_t = wave(np.arange(64), np.arange(128), 128)
    parts = three_part(np.concatenate((cos_t, sin_t), 1))
    return twiddle, np.concatenate((parts[:, :256], parts[:, 512:]), 0)


def middle_tables():
    base = np.arange(32)
    cos32, sin32 = wave(base, base, 32)
    eye8 = np.eye(8)
    over_px = three_part(np.concatenate((np.kron(cos32[:17], eye8), np.kron(-sin32[1:16], eye8)), 0))
    cos_tw, sin_tw = wave(base, base, 1024)
    spread = lambda t: np.repeat(np.tile(t, (1, 4)), 8, 0)
    turn_sign = np.where(base < 16, 1.0, -1.0)[:, None]
    lane_sign = np.where(np.arange(128) < 64, 1.0, -1.0)
    front_twiddle = np.concatenate(
        (
            spread(cos_tw),
            spread(turn_sign * sin_tw),
            spread(turn_sign * cos_tw) * lane_sign,
            -spread(sin_tw) * lane_sign,
        ),
        0,
    ).astype(np.float32)
    eye2 = np.eye(2)
    block = lambda t: np.kron(eye2, t)
    within = paired(np.block([[block(cos32), block(sin32)], [block(-sin32), block(cos32)]]))
    back = np.zeros((8, 2, 2, 4, 2, 2, 32))
    for py in range(8):
        for i in range(4):
            c, s = cos32[4 * py + i], sin32[4 * py + i]
            for s2 in range(2):
                back[py, 0, s2, i, s2, 0] = c
                back[py, 0, s2, i, s2, 1] = -s
                back[py, 1, s2, i, s2, 0] = s
                back[py, 1, s2, i, s2, 1] = c
    back = paired(back.reshape(128, 128))
    back_twiddle = np.zeros((2, 2, 8, 2, 4, 2, 2, 32))
    for core in range(2):
        c, s = wave(32 * core + base, base, 1024)
        c, s = (t.reshape(8, 1, 4, 1, 32) for t in (c, s))
        back_twiddle[core, 0, :, :, :, 0] = c
        back_twiddle[core, 0, :, :, :, 1] = -s
        back_twiddle[core, 1, :, :, :, 0] = s
        back_twiddle[core, 1, :, :, :, 1] = c
    back_twiddle = back_twiddle.reshape(256, 128).astype(np.float32)
    cos16, sin16 = wave(np.arange(16), base, 16)
    final = paired(np.concatenate((np.kron(eye2, cos16), np.kron(eye2, sin16)), 1))
    return (over_px, front_twiddle, within), (back, back_twiddle, final)


def span_inverse_tables():
    cos_t, sin_t = wave(np.arange(64), np.arange(128), 128)
    one = 2.0 * np.concatenate((cos_t, sin_t), 1)
    table = three_part(np.kron(np.eye(2), one), 0)
    cos_tw, sin_tw = wave(np.arange(8), np.arange(128), 1024)
    return table, np.concatenate((cos_tw, sin_tw), 0).astype(np.float32)


def split(x):
    high = x.astype(BF16)
    return high, (x - high.astype(F32)).astype(BF16)


def joined(x, axis):
    high, low = split(x)
    return jnp.concatenate((high, low, high), axis)


def halves_added(x):
    rows = x.shape[0] // 2
    return x[:rows] + x[rows:]


def dot_nn(a, b):
    return lax.dot_general(a, b, (((1,), (0,)), ((), ())), preferred_element_type=F32)


def dot_nt(a, b):
    return lax.dot_general(a, b, (((1,), (1,)), ((), ())), preferred_element_type=F32)


def span_forward_kernel(v_hbm, twiddle_hbm, table_hbm, out_ref, v_ref, twiddle_ref, table_ref, sems):
    copies = [
        pltpu.make_async_copy(v_hbm, v_ref, sems.at[0]),
        pltpu.make_async_copy(twiddle_hbm, twiddle_ref, sems.at[1]),
        pltpu.make_async_copy(table_hbm, table_ref, sems.at[2]),
    ]
    for copy in copies:
        copy.start()
    for copy in copies:
        copy.wait()
    x = [v_ref[pl.ds(s, 96, stride=8), :] for s in range(8)]
    e = [x[s] + x[s + 4] for s in range(4)]
    o = [x[s] - x[s + 4] for s in range(4)]
    e02, e13 = e[0] + e[2], e[1] + e[3]
    om, op = ROOT_HALF * (o[1] - o[3]), ROOT_HALF * (o[1] + o[3])
    e02m, e13m = e[0] - e[2], e[1] - e[3]
    one = (o[0] + om, -(o[2] + op))
    three = (o[0] - om, o[2] - op)
    spec = [
        (e02 + e13, None),
        one,
        (e02m, -e13m),
        three,
        (e02 - e13, None),
        (three[0], -three[1]),
        (e02m, e13m),
        (one[0], -one[1]),
    ]
    parts = []
    for k1 in range(8):
        re, im = spec[k1]
        cos_tw = twiddle_ref[pl.ds(k1, 1), :]
        sin_tw = twiddle_ref[pl.ds(8 + k1, 1), :]
        if k1 == 0:
            new_re, new_im = re, jnp.zeros_like(re)
        elif im is None:
            new_re, new_im = re * cos_tw, -(re * sin_tw)
        else:
            new_re, new_im = re * cos_tw + im * sin_tw, im * cos_tw - re * sin_tw
        parts.append((split(new_re), split(new_im)))
    table = table_ref[...]
    for j in range(4):
        columns = []
        for level in range(2):
            rows = []
            for c in range(3):
                cut = slice(32 * c, 32 * c + 32)
                for turn in range(2):
                    for k1 in (2 * j, 2 * j + 1):
                        re, im = parts[k1][0][level][cut], parts[k1][1][level][cut]
                        rows.append(jnp.concatenate((re, im) if turn == 0 else (im, -re), 1))
            columns.append(jnp.concatenate(rows, 0))
        result = halves_added(dot_nt(table, columns[0])) + dot_nt(table[:64], columns[1])
        for c in range(3):
            for t in range(8):
                first = 384 * (j // 2) + 24 * (j % 2) + 48 * t + c
                out_ref[pl.ds(first, 8, stride=3), :] = result[8 * t : 8 * t + 8, 128 * c : 128 * c + 128]


def middle_front_kernel(anchor, band_hbm, r_ref, over_px_ref, front_tw_ref, within_ref, out_ref, band_ref, sem):
    band_copy = pltpu.make_async_copy(band_hbm, band_ref, sem)
    band_copy.start()
    data = jnp.concatenate([r_ref[pl.ds(c, 256, stride=3), :] for c in range(3)], 1)
    turned = dot_nn(over_px_ref[...], joined(data, 0))
    spectrum = []
    for c in range(3):
        cut = slice(128 * c, 128 * c + 128)
        rows = []
        for k1 in range(32):
            t1, t2, t3, t4 = [front_tw_ref[pl.ds(256 * t + 8 * k1, 8), :] for t in range(4)]
            m = min(k1, 32 - k1)
            p = turned[8 * m : 8 * m + 8, cut]
            if m % 16 == 0:
                rows.append(p * t1 + pltpu.roll(p * t4, 64, axis=1))
            else:
                q = turned[128 + 8 * m : 136 + 8 * m, cut]
                rows.append((p * t1 + q * t2) + pltpu.roll(q * t3 + p * t4, 64, axis=1))
        u = jnp.concatenate(split(jnp.concatenate(rows, 0)), 1)
        out = halves_added(dot_nt(within_ref[...], u))
        spectrum.append((out[:64], out[64:]))
    sub = lax.broadcasted_iota(jnp.int32, (8, 128), 0)
    lanes = lax.broadcasted_iota(jnp.int32, (8, 128), 1)
    band_copy.wait()
    band = jnp.zeros((8, 128), jnp.int32)
    count_one = jnp.int32(0)
    for y in range(8):
        band = jnp.where(sub == y, band_ref[y], band)
        count_one = count_one + band_ref[y]
    lane_band = (lanes // 32) % 2
    in_band = band == lane_band
    select = jnp.concatenate(
        [jnp.where(jnp.logical_and(in_band, lanes % 32 == k1), 1.0, 0.0).astype(F32) for k1 in range(32)], 0
    ).astype(BF16)
    select = jnp.concatenate((select, select), 0)
    one_f = jnp.full((8, 128), count_one, jnp.int32).astype(F32)
    count = jnp.where(lane_band == 1, one_f, 8.0 - one_f)
    weight = 1.0 / (count * float(NX * NZ * 1024))
    row64 = lax.broadcasted_iota(jnp.int32, (64, 128), 0)
    lane64 = lax.broadcasted_iota(jnp.int32, (64, 128), 1)
    scale = jnp.concatenate([weight] * 8, 0)
    scale = jnp.where(jnp.logical_and(anchor, row64 < 32), 0.5 * scale, scale)
    mean = jnp.logical_and(anchor, jnp.logical_and(row64 == 0, lane64 % 32 == 0))
    scale = jnp.where(mean, 0.0, scale)
    place = 0
    for left, right in PAIR_LIST:
        lr, li = spectrum[left]
        rr, ri = spectrum[right]
        values = [lr * rr + li * ri]
        if left != right:
            values.append(lr * ri - li * rr)
        for value in values:
            out_ref[64 * place : 64 * place + 64, :] = dot_nn(jnp.concatenate(split(value), 1), select) * scale
            place += 1


def middle_back_kernel(core, own_ref, got_ref, back_ref, back_tw_ref, final_ref, out_ref):
    first_core = core == 0
    zeros = jnp.zeros((32, 128), F32)
    columns = []
    for g in range(2):
        for k in range(2):
            place, pieces = 0, []
            for left, right in PAIR_LIST:
                for part in range(2):
                    if part == 1 and left == right:
                        pieces.append(zeros)
                        continue
                    rows = slice(64 * place + 32 * k, 64 * place + 32 * k + 32)
                    own, got = own_ref[rows, :], got_ref[rows, :]
                    pieces.append(jnp.where(first_core, own, got) if g == 0 else jnp.where(first_core, got, own))
                    place += 1
            for sp in range(3):
                columns.append(jnp.concatenate(pieces[4 * sp : 4 * sp + 4], 0))
    v = halves_added(dot_nn(back_ref[...], jnp.concatenate(split(jnp.concatenate(columns, 1)), 0)))
    lane = lax.broadcasted_iota(jnp.int32, (16, 128), 1)
    twiddle_row = pl.multiple_of(core * 128, 128)
    for py in range(8):
        t1 = back_tw_ref[pl.ds(twiddle_row + 8 * py, 8), :]
        t2 = back_tw_ref[pl.ds(twiddle_row + 64 + 8 * py, 8), :]
        re_rows, im_rows = [], []
        for column in range(12):
            cut = slice(128 * column, 128 * column + 128)
            vr, vi = v[16 * py : 16 * py + 8, cut], v[16 * py + 8 : 16 * py + 16, cut]
            re_rows.append(vr * t1 - vi * t2)
            im_rows.append(vr * t2 + vi * t1)
        rows = jnp.concatenate(split(jnp.concatenate(re_rows + im_rows, 0)), 1)
        out = halves_added(dot_nt(final_ref[...], jnp.concatenate((rows, rows[128:]), 0)))
        out_ref[pl.ds(3 * py, 16, stride=24), :] = out[:16, :128]
        out_ref[pl.ds(3 * py + 1, 16, stride=24), :] = jnp.where(lane < 64, out[:16, 128:], out[16:, 128:])
        out_ref[pl.ds(3 * py + 2, 16, stride=24), :] = out[16:, :128]


def span_inverse_kernel(r_ref, table_ref, twiddle_ref, out_hbm, out_ref, sems):
    copies = []
    table = table_ref[...]
    lhs = [r_ref[pl.ds(part, 128, stride=3), :].T for part in range(3)]
    sums = dot_nn(joined(jnp.concatenate(lhs, 0), 1), table)
    sub = lax.broadcasted_iota(jnp.int32, (8, 128), 0)
    for sp in range(3):
        for b in range(2):
            y = []
            for k1 in range(8):
                col = (k1 // 4) * 256
                at = (k1 % 4) * 24 + sp * 8
                row_re, row_im = [n if b == 0 else (n + 256 if n < 128 else n + 64) for n in (at, at + 96)]
                rc, rs = sums[row_re : row_re + 8, col : col + 128], sums[row_re : row_re + 8, col + 128 : col + 256]
                ic, is_ = sums[row_im : row_im + 8, col : col + 128], sums[row_im : row_im + 8, col + 128 : col + 256]
                zr, zi = rc - is_, rs + ic
                c, s = twiddle_ref[pl.ds(k1, 1), :], twiddle_ref[pl.ds(8 + k1, 1), :]
                if k1 == 0:
                    y.append((zr, None))
                elif k1 == 4:
                    y.append((zr * c - zi * s, None))
                else:
                    y.append((zr * c - zi * s, zr * s + zi * c))
            a = [None] + [y[k][0] + y[8 - k][0] for k in (1, 2, 3)]
            d = [None] + [y[k][1] - y[8 - k][1] for k in (1, 2, 3)]
            up, um = y[0][0] + y[4][0], y[0][0] - y[4][0]
            ap, am = a[1] + a[3], ROOT_HALF * (a[1] - a[3])
            dm, dp = d[1] - d[3], ROOT_HALF * (d[1] + d[3])
            upp, upm = up + a[2], up - a[2]
            ump, umm = um + d[2], um - d[2]
            outs = [
                upp + ap,
                umm + am - dp,
                upm - dm,
                ump - am - dp,
                upp - ap,
                umm - am + dp,
                upm + dm,
                ump + am + dp,
            ]
            for half in range(4):
                v0, v1 = outs[2 * half], outs[2 * half + 1]
                base = (sp * 2 * 2 + b) * 32 + half * 8
                out_ref[pl.ds(base, 8), :] = jnp.where(sub < 4, v0, pltpu.roll(v1, 4, axis=0))
                out_ref[pl.ds(base + 64, 8), :] = jnp.where(sub < 4, pltpu.roll(v0, 4, axis=0), v1)
        block = pl.ds(128 * sp, 128)
        copies.append(pltpu.make_async_copy(out_ref.at[block], out_hbm.at[block], sems.at[sp]))
        copies[-1].start()
    for copy in copies:
        copy.wait()


def spaces(*kinds):
    return [pl.BlockSpec(memory_space=kind) for kind in kinds]


VMEM, HBM = pltpu.VMEM, pltpu.HBM


def call(kernel, out_shape, in_specs, name, out_space=VMEM, scratch=()):
    return pl.pallas_call(
        kernel,
        out_shape=jax.ShapeDtypeStruct(out_shape, F32),
        in_specs=in_specs,
        out_specs=pl.BlockSpec(memory_space=out_space),
        scratch_shapes=list(scratch),
        name=name,
        compiler_params=pltpu.CompilerParams(vmem_limit_bytes=16 * 1024 * 1024),
    )


def in_hbm(x):
    return pltpu.with_memory_space_constraint(jnp.asarray(x), HBM)


def run_span_forward(velocity):
    twiddle, table = span_forward_tables()
    scratch = (VMEM((768, 128), F32), VMEM(twiddle.shape, F32), VMEM(table.shape, BF16), pltpu.SemaphoreType.DMA((3,)))
    run = call(span_forward_kernel, (768, 128), spaces(HBM, HBM, HBM), "span_forward", scratch=scratch)
    return run(in_hbm(velocity), in_hbm(twiddle), in_hbm(table))


def run_middle_front(received, band_of, anchor=None):
    def kernel(*refs):
        at_anchor = anchor
        if anchor is None:
            at_anchor = lax.axis_index("q") + lax.axis_index("core") + lax.axis_index("py") == 0
        middle_front_kernel(at_anchor, *refs)

    scratch = (pltpu.SMEM((8,), jnp.int32), pltpu.SemaphoreType.DMA)
    run = call(kernel, (576, 128), spaces(HBM, *[VMEM] * 4), "middle_front", scratch=scratch)
    return run(in_hbm(band_of), received, *middle_tables()[0])


def run_middle_back(own, got, core=None):
    def kernel(*refs):
        middle_back_kernel(lax.axis_index("core") if core is None else core, *refs)

    return call(kernel, (384, 128), spaces(*[VMEM] * 5), "middle_back")(own, got, *middle_tables()[1])


def run_span_inverse(received):
    scratch = (VMEM((384, 128), F32), pltpu.SemaphoreType.DMA((3,)))
    run = call(span_inverse_kernel, (384, 128), spaces(VMEM, VMEM, VMEM), "span_inverse", HBM, scratch)
    return run(received, *span_inverse_tables())


def per_device(velocity, band_of):
    sent = run_span_forward(velocity.reshape(768, 128))
    received = lax.all_to_all(sent.reshape(256, 1, 384), ("q", "core", "py"), 0, 0, tiled=True)
    own = run_middle_front(received.reshape(768, 128), band_of)
    got = lax.ppermute(own, "core", ((0, 1), (1, 0)))
    back = run_middle_back(own, got)
    gathered = lax.all_to_all(back.reshape(128, 1, 384), ("q", "py"), 0, 0, tiled=True)
    out = run_span_inverse(gathered.reshape(384, 128))
    return out.reshape(6, 2, 8, 4, 128).transpose(0, 1, 3, 2, 4).reshape(6, 2, 4, 1024)


def solution(mesh):
    split_mesh = jax.sharding.Mesh(mesh.devices.reshape(16, 2, 8), ("q", "core", "py"))
    in_specs = (P(None, ("q", "core"), "py", None), P())
    out_specs = P(None, None, ("q", "core", "py"), None)
    return jax.shard_map(per_device, mesh=split_mesh, in_specs=in_specs, out_specs=out_specs, check_vma=False)
```

```python
import math

import jax
import jax.numpy as jnp
import numpy as np
from jax import lax
from jax.experimental import pallas as pl
from jax.experimental.pallas import tpu as pltpu
from jax.sharding import PartitionSpec as P

NX = 1024
NZ = 1024
NY = 8
NB = 2
PAIR_LIST = ((0, 0), (0, 1), (0, 2), (1, 1), (1, 2), (2, 2))
ROOT_HALF = math.sqrt(0.5)
F32 = jnp.float32
BF16 = jnp.bfloat16


def wave(rows, cols, length):
    angle = 2.0 * np.pi * (np.multiply.outer(rows, cols) % length) / length
    return np.cos(angle), np.sin(angle)


def three_part(table, axis=1):
    high = table.astype(np.float32).astype(jnp.bfloat16)
    low = (table - high.astype(np.float64)).astype(np.float32).astype(jnp.bfloat16)
    return np.concatenate((high, high, low), axis)


def paired(table):
    parts = three_part(table)
    width = table.shape[1]
    return np.concatenate((parts[:, : 2 * width], np.concatenate((parts[:, 2 * width :], 0 * parts[:, :width]), 1)), 0)


def span_forward_tables():
    cos_tw, sin_tw = wave(np.arange(8), np.arange(128), 1024)
    twiddle = np.concatenate((cos_tw, sin_tw), 0).astype(np.float32)
    cos_t, sin_t = wave(np.arange(64), np.arange(128), 128)
    return twiddle, paired(np.concatenate((cos_t, sin_t), 0))


def middle_tables():
    base = np.arange(32)
    cos32, sin32 = wave(base, base, 32)
    eye8 = np.eye(8)
    over_px = three_part(np.concatenate((np.kron(cos32[:17], eye8), np.kron(-sin32[1:16], eye8)), 0))
    cos_tw, sin_tw = wave(base, base, 1024)
    spread = lambda t: np.repeat(np.tile(t, (1, 4)), 8, 0)
    turn_sign = np.where(base < 16, 1.0, -1.0)[:, None]
    lane_sign = np.where(np.arange(128) < 64, 1.0, -1.0)
    front_twiddle = np.concatenate(
        (
            spread(cos_tw),
            spread(turn_sign * sin_tw),
            spread(turn_sign * cos_tw) * lane_sign,
            -spread(sin_tw) * lane_sign,
        ),
        0,
    ).astype(np.float32)
    eye2 = np.eye(2)
    block = lambda t: np.kron(eye2, t)
    within = paired(np.block([[block(cos32), block(sin32)], [block(-sin32), block(cos32)]]))
    back = np.zeros((8, 2, 2, 4, 2, 2, 32))
    for py in range(8):
        for i in range(4):
            c, s = cos32[4 * py + i], sin32[4 * py + i]
            for s2 in range(2):
                back[py, 0, s2, i, s2, 0] = c
                back[py, 0, s2, i, s2, 1] = -s
                back[py, 1, s2, i, s2, 0] = s
                back[py, 1, s2, i, s2, 1] = c
    back = paired(back.reshape(128, 128))
    back_twiddle = np.zeros((2, 2, 8, 2, 4, 2, 2, 32))
    for core in range(2):
        c, s = wave(32 * core + base, base, 1024)
        c, s = (t.reshape(8, 1, 4, 1, 32) for t in (c, s))
        back_twiddle[core, 0, :, :, :, 0] = c
        back_twiddle[core, 0, :, :, :, 1] = -s
        back_twiddle[core, 1, :, :, :, 0] = s
        back_twiddle[core, 1, :, :, :, 1] = c
    back_twiddle = back_twiddle.reshape(256, 128).astype(np.float32)
    cos16, sin16 = wave(np.arange(16), base, 16)
    final = paired(np.concatenate((np.kron(eye2, cos16), np.kron(eye2, sin16)), 1))
    return (over_px, front_twiddle, within), (back, back_twiddle, final)


def span_inverse_tables():
    cos_t, sin_t = wave(np.arange(64), np.arange(128), 128)
    one = 2.0 * np.concatenate((cos_t, sin_t), 1)
    table = three_part(np.kron(np.eye(2), one), 0)
    cos_tw, sin_tw = wave(np.arange(8), np.arange(128), 1024)
    return table, np.concatenate((cos_tw, sin_tw), 0).astype(np.float32)


def split(x):
    high = x.astype(BF16)
    return high, (x - high.astype(F32)).astype(BF16)


def joined(x, axis):
    high, low = split(x)
    return jnp.concatenate((high, low, high), axis)


def halves_added(x):
    rows = x.shape[0] // 2
    return x[:rows] + x[rows:]


def dot_nn(a, b):
    return lax.dot_general(a, b, (((1,), (0,)), ((), ())), preferred_element_type=F32)


def dot_nt(a, b):
    return lax.dot_general(a, b, (((1,), (1,)), ((), ())), preferred_element_type=F32)


def span_forward_kernel(v_hbm, twiddle_hbm, table_hbm, out_ref, v_ref, twiddle_ref, table_ref, sems):
    copies = [
        pltpu.make_async_copy(v_hbm, v_ref, sems.at[0]),
        pltpu.make_async_copy(twiddle_hbm, twiddle_ref, sems.at[1]),
        pltpu.make_async_copy(table_hbm, table_ref, sems.at[2]),
    ]
    for copy in copies:
        copy.start()
    for copy in copies:
        copy.wait()
    x = [v_ref[pl.ds(s, 96, stride=8), :] for s in range(8)]
    e = [x[s] + x[s + 4] for s in range(4)]
    o = [x[s] - x[s + 4] for s in range(4)]
    e02, e13 = e[0] + e[2], e[1] + e[3]
    om, op = ROOT_HALF * (o[1] - o[3]), ROOT_HALF * (o[1] + o[3])
    e02m, e13m = e[0] - e[2], e[1] - e[3]
    one = (o[0] + om, -(o[2] + op))
    three = (o[0] - om, o[2] - op)
    spec = [
        (e02 + e13, None),
        one,
        (e02m, -e13m),
        three,
        (e02 - e13, None),
        (three[0], -three[1]),
        (e02m, e13m),
        (one[0], -one[1]),
    ]
    parts = []
    for k1 in range(8):
        re, im = spec[k1]
        cos_tw = twiddle_ref[pl.ds(k1, 1), :]
        sin_tw = twiddle_ref[pl.ds(8 + k1, 1), :]
        if k1 == 0:
            new_re, new_im = re, jnp.zeros_like(re)
        elif im is None:
            new_re, new_im = re * cos_tw, -(re * sin_tw)
        else:
            new_re, new_im = re * cos_tw + im * sin_tw, im * cos_tw - re * sin_tw
        parts.append((split(new_re), split(new_im)))
    table = table_ref[...]
    lane = lax.broadcasted_iota(jnp.int32, (1, 384), 1) % 128
    sign = jnp.where(lane < 64, 1.0, -1.0).astype(F32)
    for j in range(4):
        rows = []
        for c in range(3):
            cut = slice(32 * c, 32 * c + 32)
            for part in range(2):
                for k1 in (2 * j, 2 * j + 1):
                    high, low = parts[k1][part]
                    rows.append(jnp.concatenate((high[cut], low[cut]), 1))
        sums = halves_added(dot_nt(table, jnp.concatenate(rows, 0)))
        turned = [pltpu.roll(sums[64:, 128 * c : 128 * c + 128], 64, axis=1) for c in range(3)]
        result = sums[:64] + jnp.concatenate(turned, 1) * sign
        for c in range(3):
            for t in range(8):
                first = 384 * (j // 2) + 24 * (j % 2) + 48 * t + c
                out_ref[pl.ds(first, 8, stride=3), :] = result[8 * t : 8 * t + 8, 128 * c : 128 * c + 128]


def middle_front_kernel(anchor, band_hbm, r_ref, over_px_ref, front_tw_ref, within_ref, out_ref, packed_ref, band_ref, sem):
    band_copy = pltpu.make_async_copy(band_hbm, band_ref, sem)
    band_copy.start()
    data = jnp.concatenate([r_ref[pl.ds(c, 256, stride=3), :] for c in range(3)], 1)
    turned = dot_nn(over_px_ref[...], joined(data, 0))
    spectrum = []
    for c in range(3):
        cut = slice(128 * c, 128 * c + 128)
        rows = []
        for k1 in range(32):
            t1, t2, t3, t4 = [front_tw_ref[pl.ds(256 * t + 8 * k1, 8), :] for t in range(4)]
            m = min(k1, 32 - k1)
            p = turned[8 * m : 8 * m + 8, cut]
            if m % 16 == 0:
                rows.append(p * t1 + pltpu.roll(p * t4, 64, axis=1))
            else:
                q = turned[128 + 8 * m : 136 + 8 * m, cut]
                rows.append((p * t1 + q * t2) + pltpu.roll(q * t3 + p * t4, 64, axis=1))
        u = jnp.concatenate(split(jnp.concatenate(rows, 0)), 1)
        out = halves_added(dot_nt(within_ref[...], u))
        spectrum.append((out[:64], out[64:]))
    sub = lax.broadcasted_iota(jnp.int32, (8, 128), 0)
    lanes = lax.broadcasted_iota(jnp.int32, (8, 128), 1)
    band_copy.wait()
    band = jnp.zeros((8, 128), jnp.int32)
    count_one = jnp.int32(0)
    for y in range(8):
        band = jnp.where(sub == y, band_ref[y], band)
        count_one = count_one + band_ref[y]
    lane_band = (lanes // 32) % 2
    in_band = band == lane_band
    select = jnp.concatenate(
        [jnp.where(jnp.logical_and(in_band, lanes % 32 == k1), 1.0, 0.0).astype(F32) for k1 in range(32)], 0
    ).astype(BF16)
    select = jnp.concatenate((select, select), 0)
    one_f = jnp.full((8, 128), count_one, jnp.int32).astype(F32)
    count = jnp.where(lane_band == 1, one_f, 8.0 - one_f)
    weight = 1.0 / (count * float(NX * NZ * 1024))
    row64 = lax.broadcasted_iota(jnp.int32, (64, 128), 0)
    lane64 = lax.broadcasted_iota(jnp.int32, (64, 128), 1)
    scale = jnp.concatenate([weight] * 8, 0)
    scale = jnp.where(jnp.logical_and(anchor, row64 < 32), 0.5 * scale, scale)
    mean = jnp.logical_and(anchor, jnp.logical_and(row64 == 0, lane64 % 32 == 0))
    scale = jnp.where(mean, 0.0, scale)
    place = 0
    for left, right in PAIR_LIST:
        lr, li = spectrum[left]
        rr, ri = spectrum[right]
        values = [lr * rr + li * ri]
        if left != right:
            values.append(lr * ri - li * rr)
        for value in values:
            sums = dot_nn(jnp.concatenate(split(value), 1), select) * scale
            out_ref[64 * place : 64 * place + 64, :] = sums
            packed_ref[32 * place : 32 * place + 32, :] = jnp.where(lane64[:32] < 64, sums[:32], sums[32:])
            place += 1


def middle_back_kernel(core, own_ref, got_ref, back_ref, back_tw_ref, final_ref, out_ref):
    first_core = core == 0
    zeros = jnp.zeros((32, 128), F32)
    first_half = lax.broadcasted_iota(jnp.int32, (32, 128), 1) < 64
    own, got = [], []
    for place in range(9):
        packed = got_ref[32 * place : 32 * place + 32, :]
        turned = pltpu.roll(packed, 64, axis=1)
        got.append((jnp.where(first_half, packed, turned), jnp.where(first_half, turned, packed)))
        own.append([own_ref[64 * place + 32 * k : 64 * place + 32 * k + 32, :] for k in range(2)])
    columns = []
    for g in range(2):
        for k in range(2):
            place, pieces = 0, []
            for left, right in PAIR_LIST:
                for part in range(2):
                    if part == 1 and left == right:
                        pieces.append(zeros)
                        continue
                    two = (own[place][k], got[place][k])
                    pieces.append(jnp.where(first_core, two[g], two[1 - g]))
                    place += 1
            for sp in range(3):
                columns.append(jnp.concatenate(pieces[4 * sp : 4 * sp + 4], 0))
    v = halves_added(dot_nn(back_ref[...], jnp.concatenate(split(jnp.concatenate(columns, 1)), 0)))
    lane = lax.broadcasted_iota(jnp.int32, (16, 128), 1)
    twiddle_row = pl.multiple_of(core * 128, 128)
    for py in range(8):
        t1 = back_tw_ref[pl.ds(twiddle_row + 8 * py, 8), :]
        t2 = back_tw_ref[pl.ds(twiddle_row + 64 + 8 * py, 8), :]
        re_rows, im_rows = [], []
        for column in range(12):
            cut = slice(128 * column, 128 * column + 128)
            vr, vi = v[16 * py : 16 * py + 8, cut], v[16 * py + 8 : 16 * py + 16, cut]
            re_rows.append(vr * t1 - vi * t2)
            im_rows.append(vr * t2 + vi * t1)
        rows = jnp.concatenate(split(jnp.concatenate(re_rows + im_rows, 0)), 1)
        out = halves_added(dot_nt(final_ref[...], jnp.concatenate((rows, rows[128:]), 0)))
        out_ref[pl.ds(3 * py, 16, stride=24), :] = out[:16, :128]
        out_ref[pl.ds(3 * py + 1, 16, stride=24), :] = jnp.where(lane < 64, out[:16, 128:], out[16:, 128:])
        out_ref[pl.ds(3 * py + 2, 16, stride=24), :] = out[16:, :128]


def span_inverse_kernel(r_ref, table_ref, twiddle_ref, out_hbm, out_ref, sems):
    copies = []
    table = table_ref[...]
    lhs = [r_ref[pl.ds(part, 128, stride=3), :].T for part in range(3)]
    sums = dot_nn(joined(jnp.concatenate(lhs, 0), 1), table)
    sub = lax.broadcasted_iota(jnp.int32, (8, 128), 0)
    for sp in range(3):
        for b in range(2):
            y = []
            for k1 in range(8):
                col = (k1 // 4) * 256
                at = (k1 % 4) * 24 + sp * 8
                row_re, row_im = [n if b == 0 else (n + 256 if n < 128 else n + 64) for n in (at, at + 96)]
                rc, rs = sums[row_re : row_re + 8, col : col + 128], sums[row_re : row_re + 8, col + 128 : col + 256]
                ic, is_ = sums[row_im : row_im + 8, col : col + 128], sums[row_im : row_im + 8, col + 128 : col + 256]
                zr, zi = rc - is_, rs + ic
                c, s = twiddle_ref[pl.ds(k1, 1), :], twiddle_ref[pl.ds(8 + k1, 1), :]
                if k1 == 0:
                    y.append((zr, None))
                elif k1 == 4:
                    y.append((zr * c - zi * s, None))
                else:
                    y.append((zr * c - zi * s, zr * s + zi * c))
            a = [None] + [y[k][0] + y[8 - k][0] for k in (1, 2, 3)]
            d = [None] + [y[k][1] - y[8 - k][1] for k in (1, 2, 3)]
            up, um = y[0][0] + y[4][0], y[0][0] - y[4][0]
            ap, am = a[1] + a[3], ROOT_HALF * (a[1] - a[3])
            dm, dp = d[1] - d[3], ROOT_HALF * (d[1] + d[3])
            upp, upm = up + a[2], up - a[2]
            ump, umm = um + d[2], um - d[2]
            outs = [
                upp + ap,
                umm + am - dp,
                upm - dm,
                ump - am - dp,
                upp - ap,
                umm - am + dp,
                upm + dm,
                ump + am + dp,
            ]
            for half in range(4):
                v0, v1 = outs[2 * half], outs[2 * half + 1]
                base = (sp * 2 * 2 + b) * 32 + half * 8
                out_ref[pl.ds(base, 8), :] = jnp.where(sub < 4, v0, pltpu.roll(v1, 4, axis=0))
                out_ref[pl.ds(base + 64, 8), :] = jnp.where(sub < 4, pltpu.roll(v0, 4, axis=0), v1)
        block = pl.ds(128 * sp, 128)
        copies.append(pltpu.make_async_copy(out_ref.at[block], out_hbm.at[block], sems.at[sp]))
        copies[-1].start()
    for copy in copies:
        copy.wait()


def spaces(*kinds):
    return [pl.BlockSpec(memory_space=kind) for kind in kinds]


VMEM, HBM = pltpu.VMEM, pltpu.HBM


def call(kernel, out_rows, in_specs, name, out_space=VMEM, scratch=()):
    return pl.pallas_call(
        kernel,
        out_shape=jax.tree.map(lambda rows: jax.ShapeDtypeStruct((rows, 128), F32), out_rows),
        in_specs=in_specs,
        out_specs=jax.tree.map(lambda rows: pl.BlockSpec(memory_space=out_space), out_rows),
        scratch_shapes=list(scratch),
        name=name,
        compiler_params=pltpu.CompilerParams(vmem_limit_bytes=16 * 1024 * 1024),
    )


def in_hbm(x):
    return pltpu.with_memory_space_constraint(jnp.asarray(x), HBM)


def run_span_forward(velocity):
    twiddle, table = span_forward_tables()
    scratch = (VMEM((768, 128), F32), VMEM(twiddle.shape, F32), VMEM(table.shape, BF16), pltpu.SemaphoreType.DMA((3,)))
    run = call(span_forward_kernel, 768, spaces(HBM, HBM, HBM), "span_forward", scratch=scratch)
    return run(in_hbm(velocity), in_hbm(twiddle), in_hbm(table))


def run_middle_front(received, band_of, anchor=None):
    def kernel(*refs):
        at_anchor = anchor
        if anchor is None:
            at_anchor = lax.axis_index("q") + lax.axis_index("core") + lax.axis_index("py") == 0
        middle_front_kernel(at_anchor, *refs)

    scratch = (pltpu.SMEM((8,), jnp.int32), pltpu.SemaphoreType.DMA)
    run = call(kernel, (576, 288), spaces(HBM, *[VMEM] * 4), "middle_front", scratch=scratch)
    return run(in_hbm(band_of), received, *middle_tables()[0])


def run_middle_back(own, got, core=None):
    def kernel(*refs):
        middle_back_kernel(lax.axis_index("core") if core is None else core, *refs)

    return call(kernel, 384, spaces(*[VMEM] * 5), "middle_back")(own, got, *middle_tables()[1])


def run_span_inverse(received):
    scratch = (VMEM((384, 128), F32), pltpu.SemaphoreType.DMA((3,)))
    run = call(span_inverse_kernel, 384, spaces(VMEM, VMEM, VMEM), "span_inverse", HBM, scratch)
    return run(received, *span_inverse_tables())


def per_device(velocity, band_of):
    sent = run_span_forward(velocity.reshape(768, 128))
    received = lax.all_to_all(sent.reshape(256, 1, 384), ("q", "core", "py"), 0, 0, tiled=True)
    own, packed = run_middle_front(received.reshape(768, 128), band_of)
    got = lax.ppermute(packed, "core", ((0, 1), (1, 0)))
    back = run_middle_back(own, got)
    gathered = lax.all_to_all(back.reshape(128, 1, 384), ("q", "py"), 0, 0, tiled=True)
    out = run_span_inverse(gathered.reshape(384, 128))
    return out.reshape(6, 2, 8, 4, 128).transpose(0, 1, 3, 2, 4).reshape(6, 2, 4, 1024)


def solution(mesh):
    split_mesh = jax.sharding.Mesh(mesh.devices.reshape(16, 2, 8), ("q", "core", "py"))
    in_specs = (P(None, ("q", "core"), "py", None), P())
    out_specs = P(None, None, ("q", "core", "py"), None)
    return jax.shard_map(per_device, mesh=split_mesh, in_specs=in_specs, out_specs=out_specs, check_vma=False)
```

```python
import math

import jax
import jax.numpy as jnp
import numpy as np
from jax import lax
from jax.experimental import pallas as pl
from jax.experimental.pallas import tpu as pltpu
from jax.sharding import PartitionSpec as P

NX = 1024
NZ = 1024
NY = 8
NB = 2
PAIR_LIST = ((0, 0), (0, 1), (0, 2), (1, 1), (1, 2), (2, 2))
ROOT_HALF = math.sqrt(0.5)
F32 = jnp.float32
BF16 = jnp.bfloat16


def wave(rows, cols, length):
    angle = 2.0 * np.pi * (np.multiply.outer(rows, cols) % length) / length
    return np.cos(angle), np.sin(angle)


def three_part(table, axis=1):
    high = table.astype(np.float32).astype(jnp.bfloat16)
    low = (table - high.astype(np.float64)).astype(np.float32).astype(jnp.bfloat16)
    return np.concatenate((high, high, low), axis)


def paired(table):
    parts = three_part(table)
    width = table.shape[1]
    return np.concatenate((parts[:, : 2 * width], np.concatenate((parts[:, 2 * width :], 0 * parts[:, :width]), 1)), 0)


def order_of(axes):
    sizes = dict(x=4, zh=4, core=2, zl=2, y=4)
    places = np.indices([sizes[axis] for axis in axes]).reshape(len(axes), -1)
    at = dict(zip(axes, places))
    px = (at["x"] * 4 + at["zh"]) * 2 + at.get("core", 0)
    return px, at["zl"] * 4 + at["y"], ((at["zh"] * 2 + at["zl"]) * 4 + at["y"]) * 4 + at["x"]


FRONT_AXES = ("zh", "zl", "y", "x", "core")
BACK_AXES = ("zl", "y", "zh", "x")


def span_forward_tables():
    cos_tw, sin_tw = wave(np.arange(8), np.arange(128), 1024)
    twiddle = np.concatenate((cos_tw, sin_tw), 0).astype(np.float32)
    cos_t, sin_t = wave(np.arange(64), np.arange(128), 128)
    parts = three_part(np.concatenate((cos_t, sin_t), 1))
    return twiddle, np.concatenate((parts[:, :256], parts[:, 512:]), 0)


def middle_tables():
    base = np.arange(32)
    cos32, sin32 = wave(base, base, 32)
    eye8 = np.eye(8)
    over_px = np.concatenate((np.kron(cos32[:17], eye8), np.kron(-sin32[1:16], eye8)), 0)
    px, py, _ = order_of(FRONT_AXES)
    over_px = three_part(over_px[:, px * 8 + py])
    cos_tw, sin_tw = wave(base, base, 1024)
    spread = lambda t: np.repeat(np.tile(t, (1, 4)), 8, 0)
    turn_sign = np.where(base < 16, 1.0, -1.0)[:, None]
    lane_sign = np.where(np.arange(128) < 64, 1.0, -1.0)
    front_twiddle = np.concatenate(
        (
            spread(cos_tw),
            spread(turn_sign * sin_tw),
            spread(turn_sign * cos_tw) * lane_sign,
            -spread(sin_tw) * lane_sign,
        ),
        0,
    ).astype(np.float32)
    eye2 = np.eye(2)
    block = lambda t: np.kron(eye2, t)
    within = paired(np.block([[block(cos32), block(sin32)], [block(-sin32), block(cos32)]]))
    back = np.zeros((8, 2, 2, 4, 2, 2, 32))
    for py in range(8):
        for i in range(4):
            c, s = cos32[4 * py + i], sin32[4 * py + i]
            for s2 in range(2):
                back[py, 0, s2, i, s2, 0] = c
                back[py, 0, s2, i, s2, 1] = -s
                back[py, 1, s2, i, s2, 0] = s
                back[py, 1, s2, i, s2, 1] = c
    back = paired(back.reshape(128, 128))
    back_twiddle = np.zeros((2, 2, 8, 2, 4, 2, 2, 32))
    for core in range(2):
        c, s = wave(32 * core + base, base, 1024)
        c, s = (t.reshape(8, 1, 4, 1, 32) for t in (c, s))
        back_twiddle[core, 0, :, :, :, 0] = c
        back_twiddle[core, 0, :, :, :, 1] = -s
        back_twiddle[core, 1, :, :, :, 0] = s
        back_twiddle[core, 1, :, :, :, 1] = c
    back_twiddle = back_twiddle.reshape(256, 128).astype(np.float32)
    cos16, sin16 = wave(order_of(BACK_AXES)[0][:16] // 2, base, 16)
    final = paired(np.concatenate((np.kron(eye2, cos16), np.kron(eye2, sin16)), 1))
    return (over_px, front_twiddle, within), (back, back_twiddle, final)


def span_inverse_tables():
    cos_t, sin_t = wave(np.arange(64), np.arange(128), 128)
    one = 2.0 * np.concatenate((cos_t, sin_t), 1)
    table = three_part(np.kron(np.eye(2), one)[order_of(BACK_AXES)[2]], 0)
    cos_tw, sin_tw = wave(np.arange(8), np.arange(128), 1024)
    return table, np.concatenate((cos_tw, sin_tw), 0).astype(np.float32)


def split(x):
    high = x.astype(BF16)
    return high, (x - high.astype(F32)).astype(BF16)


def joined(x, axis):
    high, low = split(x)
    return jnp.concatenate((high, low, high), axis)


def halves_added(x):
    rows = x.shape[0] // 2
    return x[:rows] + x[rows:]


def dot_nn(a, b):
    return lax.dot_general(a, b, (((1,), (0,)), ((), ())), preferred_element_type=F32)


def dot_nt(a, b):
    return lax.dot_general(a, b, (((1,), (1,)), ((), ())), preferred_element_type=F32)


def span_forward_kernel(v_hbm, twiddle_hbm, table_hbm, out_ref, v_ref, twiddle_ref, table_ref, sems):
    copies = [
        pltpu.make_async_copy(v_hbm, v_ref, sems.at[0]),
        pltpu.make_async_copy(twiddle_hbm, twiddle_ref, sems.at[1]),
        pltpu.make_async_copy(table_hbm, table_ref, sems.at[2]),
    ]
    for copy in copies:
        copy.start()
    for copy in copies:
        copy.wait()
    x = [v_ref[pl.ds(s, 96, stride=8), :] for s in range(8)]
    e = [x[s] + x[s + 4] for s in range(4)]
    o = [x[s] - x[s + 4] for s in range(4)]
    e02, e13 = e[0] + e[2], e[1] + e[3]
    om, op = ROOT_HALF * (o[1] - o[3]), ROOT_HALF * (o[1] + o[3])
    e02m, e13m = e[0] - e[2], e[1] - e[3]
    one = (o[0] + om, -(o[2] + op))
    three = (o[0] - om, o[2] - op)
    spec = [
        (e02 + e13, None),
        one,
        (e02m, -e13m),
        three,
        (e02 - e13, None),
        (three[0], -three[1]),
        (e02m, e13m),
        (one[0], -one[1]),
    ]
    parts = []
    for k1 in range(8):
        re, im = spec[k1]
        cos_tw = twiddle_ref[pl.ds(k1, 1), :]
        sin_tw = twiddle_ref[pl.ds(8 + k1, 1), :]
        if k1 == 0:
            new_re, new_im = re, jnp.zeros_like(re)
        elif im is None:
            new_re, new_im = re * cos_tw, -(re * sin_tw)
        else:
            new_re, new_im = re * cos_tw + im * sin_tw, im * cos_tw - re * sin_tw
        parts.append((split(new_re), split(new_im)))
    table = table_ref[...]
    for j in range(4):
        columns = []
        for level in range(2):
            rows = []
            for c in range(3):
                cut = slice(32 * c, 32 * c + 32)
                for turn in range(2):
                    for k1 in (2 * j, 2 * j + 1):
                        re, im = parts[k1][0][level][cut], parts[k1][1][level][cut]
                        rows.append(jnp.concatenate((re, im) if turn == 0 else (im, -re), 1))
            columns.append(jnp.concatenate(rows, 0))
        result = halves_added(dot_nt(table, columns[0])) + dot_nt(table[:64], columns[1])
        for c in range(3):
            first = 384 * (j // 2) + 3 * (j % 2) + c
            out_ref[pl.ds(first, 64, stride=6), :] = result[:, 128 * c : 128 * c + 128]


def middle_front_kernel(anchor, band_hbm, r_ref, over_px_ref, front_tw_ref, within_ref, out_ref, band_ref, sem):
    band_copy = pltpu.make_async_copy(band_hbm, band_ref, sem)
    band_copy.start()
    data = jnp.concatenate([r_ref[pl.ds(c, 256, stride=3), :] for c in range(3)], 1)
    turned = dot_nn(over_px_ref[...], joined(data, 0))
    spectrum = []
    for c in range(3):
        cut = slice(128 * c, 128 * c + 128)
        rows = []
        for k1 in range(32):
            t1, t2, t3, t4 = [front_tw_ref[pl.ds(256 * t + 8 * k1, 8), :] for t in range(4)]
            m = min(k1, 32 - k1)
            p = turned[8 * m : 8 * m + 8, cut]
            if m % 16 == 0:
                rows.append(p * t1 + pltpu.roll(p * t4, 64, axis=1))
            else:
                q = turned[128 + 8 * m : 136 + 8 * m, cut]
                rows.append((p * t1 + q * t2) + pltpu.roll(q * t3 + p * t4, 64, axis=1))
        u = jnp.concatenate(split(jnp.concatenate(rows, 0)), 1)
        out = halves_added(dot_nt(within_ref[...], u))
        spectrum.append((out[:64], out[64:]))
    sub = lax.broadcasted_iota(jnp.int32, (8, 128), 0)
    lanes = lax.broadcasted_iota(jnp.int32, (8, 128), 1)
    band_copy.wait()
    band = jnp.zeros((8, 128), jnp.int32)
    count_one = jnp.int32(0)
    for y in range(8):
        band = jnp.where(sub == y, band_ref[y], band)
        count_one = count_one + band_ref[y]
    lane_band = (lanes // 32) % 2
    in_band = band == lane_band
    select = jnp.concatenate(
        [jnp.where(jnp.logical_and(in_band, lanes % 32 == k1), 1.0, 0.0).astype(F32) for k1 in range(32)], 0
    ).astype(BF16)
    select = jnp.concatenate((select, select), 0)
    one_f = jnp.full((8, 128), count_one, jnp.int32).astype(F32)
    count = jnp.where(lane_band == 1, one_f, 8.0 - one_f)
    weight = 1.0 / (count * float(NX * NZ * 1024))
    row64 = lax.broadcasted_iota(jnp.int32, (64, 128), 0)
    lane64 = lax.broadcasted_iota(jnp.int32, (64, 128), 1)
    scale = jnp.concatenate([weight] * 8, 0)
    scale = jnp.where(jnp.logical_and(anchor, row64 < 32), 0.5 * scale, scale)
    mean = jnp.logical_and(anchor, jnp.logical_and(row64 == 0, lane64 % 32 == 0))
    scale = jnp.where(mean, 0.0, scale)
    place = 0
    for left, right in PAIR_LIST:
        lr, li = spectrum[left]
        rr, ri = spectrum[right]
        values = [lr * rr + li * ri]
        if left != right:
            values.append(lr * ri - li * rr)
        for value in values:
            out_ref[64 * place : 64 * place + 64, :] = dot_nn(jnp.concatenate(split(value), 1), select) * scale
            place += 1


def middle_back_kernel(core, own_ref, got_ref, back_ref, back_tw_ref, final_ref, out_ref):
    first_core = core == 0
    zeros = jnp.zeros((32, 128), F32)
    columns = []
    for g in range(2):
        for k in range(2):
            place, pieces = 0, []
            for left, right in PAIR_LIST:
                for part in range(2):
                    if part == 1 and left == right:
                        pieces.append(zeros)
                        continue
                    rows = slice(64 * place + 32 * k, 64 * place + 32 * k + 32)
                    own, got = own_ref[rows, :], got_ref[rows, :]
                    pieces.append(jnp.where(first_core, own, got) if g == 0 else jnp.where(first_core, got, own))
                    place += 1
            for sp in range(3):
                columns.append(jnp.concatenate(pieces[4 * sp : 4 * sp + 4], 0))
    v = halves_added(dot_nn(back_ref[...], jnp.concatenate(split(jnp.concatenate(columns, 1)), 0)))
    lane = lax.broadcasted_iota(jnp.int32, (16, 128), 1)
    twiddle_row = pl.multiple_of(core * 128, 128)
    for py in range(8):
        t1 = back_tw_ref[pl.ds(twiddle_row + 8 * py, 8), :]
        t2 = back_tw_ref[pl.ds(twiddle_row + 64 + 8 * py, 8), :]
        re_rows, im_rows = [], []
        for column in range(12):
            cut = slice(128 * column, 128 * column + 128)
            vr, vi = v[16 * py : 16 * py + 8, cut], v[16 * py + 8 : 16 * py + 16, cut]
            re_rows.append(vr * t1 - vi * t2)
            im_rows.append(vr * t2 + vi * t1)
        rows = jnp.concatenate(split(jnp.concatenate(re_rows + im_rows, 0)), 1)
        out = halves_added(dot_nt(final_ref[...], jnp.concatenate((rows, rows[128:]), 0)))
        out_ref[pl.ds(48 * py, 16, stride=3), :] = out[:16, :128]
        out_ref[pl.ds(48 * py + 1, 16, stride=3), :] = jnp.where(lane < 64, out[:16, 128:], out[16:, 128:])
        out_ref[pl.ds(48 * py + 2, 16, stride=3), :] = out[16:, :128]


def span_inverse_kernel(r_ref, table_ref, twiddle_ref, out_hbm, out_ref, sems):
    copies = []
    table = table_ref[...]
    lhs = [r_ref[pl.ds(part, 128, stride=3), :].T for part in range(3)]
    sums = dot_nn(joined(jnp.concatenate(lhs, 0), 1), table)
    sub = lax.broadcasted_iota(jnp.int32, (8, 128), 0)
    for sp in range(3):
        for b in range(2):
            y = []
            for k1 in range(8):
                col = (k1 // 4) * 256
                at = (k1 % 4) * 24 + sp * 8
                row_re, row_im = [n if b == 0 else (n + 256 if n < 128 else n + 64) for n in (at, at + 96)]
                rc, rs = sums[row_re : row_re + 8, col : col + 128], sums[row_re : row_re + 8, col + 128 : col + 256]
                ic, is_ = sums[row_im : row_im + 8, col : col + 128], sums[row_im : row_im + 8, col + 128 : col + 256]
                zr, zi = rc - is_, rs + ic
                c, s = twiddle_ref[pl.ds(k1, 1), :], twiddle_ref[pl.ds(8 + k1, 1), :]
                if k1 == 0:
                    y.append((zr, None))
                elif k1 == 4:
                    y.append((zr * c - zi * s, None))
                else:
                    y.append((zr * c - zi * s, zr * s + zi * c))
            a = [None] + [y[k][0] + y[8 - k][0] for k in (1, 2, 3)]
            d = [None] + [y[k][1] - y[8 - k][1] for k in (1, 2, 3)]
            up, um = y[0][0] + y[4][0], y[0][0] - y[4][0]
            ap, am = a[1] + a[3], ROOT_HALF * (a[1] - a[3])
            dm, dp = d[1] - d[3], ROOT_HALF * (d[1] + d[3])
            upp, upm = up + a[2], up - a[2]
            ump, umm = um + d[2], um - d[2]
            outs = [
                upp + ap,
                umm + am - dp,
                upm - dm,
                ump - am - dp,
                upp - ap,
                umm - am + dp,
                upm + dm,
                ump + am + dp,
            ]
            for half in range(4):
                v0, v1 = outs[2 * half], outs[2 * half + 1]
                base = (sp * 2 * 2 + b) * 32 + half * 8
                out_ref[pl.ds(base, 8), :] = jnp.where(sub < 4, v0, pltpu.roll(v1, 4, axis=0))
                out_ref[pl.ds(base + 64, 8), :] = jnp.where(sub < 4, pltpu.roll(v0, 4, axis=0), v1)
        block = pl.ds(128 * sp, 128)
        copies.append(pltpu.make_async_copy(out_ref.at[block], out_hbm.at[block], sems.at[sp]))
        copies[-1].start()
    for copy in copies:
        copy.wait()


def spaces(*kinds):
    return [pl.BlockSpec(memory_space=kind) for kind in kinds]


VMEM, HBM = pltpu.VMEM, pltpu.HBM


def call(kernel, out_shape, in_specs, name, out_space=VMEM, scratch=()):
    return pl.pallas_call(
        kernel,
        out_shape=jax.ShapeDtypeStruct(out_shape, F32),
        in_specs=in_specs,
        out_specs=pl.BlockSpec(memory_space=out_space),
        scratch_shapes=list(scratch),
        name=name,
        compiler_params=pltpu.CompilerParams(vmem_limit_bytes=16 * 1024 * 1024),
    )


def in_hbm(x):
    return pltpu.with_memory_space_constraint(jnp.asarray(x), HBM)


def run_span_forward(velocity):
    twiddle, table = span_forward_tables()
    scratch = (VMEM((768, 128), F32), VMEM(twiddle.shape, F32), VMEM(table.shape, BF16), pltpu.SemaphoreType.DMA((3,)))
    run = call(span_forward_kernel, (768, 128), spaces(HBM, HBM, HBM), "span_forward", scratch=scratch)
    return run(in_hbm(velocity), in_hbm(twiddle), in_hbm(table))


def run_middle_front(received, band_of, anchor=None):
    def kernel(*refs):
        at_anchor = anchor
        if anchor is None:
            at_anchor = sum(lax.axis_index(axis) for axis in FRONT_AXES) == 0
        middle_front_kernel(at_anchor, *refs)

    scratch = (pltpu.SMEM((8,), jnp.int32), pltpu.SemaphoreType.DMA)
    run = call(kernel, (576, 128), spaces(HBM, *[VMEM] * 4), "middle_front", scratch=scratch)
    return run(in_hbm(band_of), received, *middle_tables()[0])


def run_middle_back(own, got, core=None):
    def kernel(*refs):
        middle_back_kernel(lax.axis_index("core") if core is None else core, *refs)

    return call(kernel, (384, 128), spaces(*[VMEM] * 5), "middle_back")(own, got, *middle_tables()[1])


def run_span_inverse(received):
    scratch = (VMEM((384, 128), F32), pltpu.SemaphoreType.DMA((3,)))
    run = call(span_inverse_kernel, (384, 128), spaces(VMEM, VMEM, VMEM), "span_inverse", HBM, scratch)
    return run(received, *span_inverse_tables())


def per_device(velocity, band_of):
    sent = run_span_forward(velocity.reshape(768, 128))
    received = lax.all_to_all(sent.reshape(256, 1, 384), FRONT_AXES, 0, 0, tiled=True)
    own = run_middle_front(received.reshape(768, 128), band_of)
    got = lax.ppermute(own, "core", ((0, 1), (1, 0)))
    back = run_middle_back(own, got)
    gathered = lax.all_to_all(back.reshape(128, 1, 384), BACK_AXES, 0, 0, tiled=True)
    out = run_span_inverse(gathered.reshape(384, 128))
    return out.reshape(6, 2, 8, 4, 128).transpose(0, 1, 3, 2, 4).reshape(6, 2, 4, 1024)


def solution(mesh):
    split_mesh = jax.sharding.Mesh(mesh.devices.reshape(4, 4, 2, 2, 4), ("x", "zh", "core", "zl", "y"))
    px, py = ("x", "zh", "core"), ("zl", "y")
    in_specs = (P(None, px, py, None), P())
    out_specs = P(None, None, px + py, None)
    return jax.shard_map(per_device, mesh=split_mesh, in_specs=in_specs, out_specs=out_specs, check_vma=False)
```

```python
import math

import jax
import jax.numpy as jnp
import numpy as np
from jax import lax
from jax.experimental import pallas as pl
from jax.experimental.pallas import tpu as pltpu
from jax.sharding import PartitionSpec as P

NX = 1024
NZ = 1024
NY = 8
NB = 2
PAIR_LIST = ((0, 0), (0, 1), (0, 2), (1, 1), (1, 2), (2, 2))
ROOT_HALF = math.sqrt(0.5)
F32 = jnp.float32
BF16 = jnp.bfloat16


def wave(rows, cols, length):
    angle = 2.0 * np.pi * (np.multiply.outer(rows, cols) % length) / length
    return np.cos(angle), np.sin(angle)


def three_part(table, axis=1):
    high = table.astype(np.float32).astype(jnp.bfloat16)
    low = (table - high.astype(np.float64)).astype(np.float32).astype(jnp.bfloat16)
    return np.concatenate((high, high, low), axis)


def paired(table):
    parts = three_part(table)
    width = table.shape[1]
    return np.concatenate((parts[:, : 2 * width], np.concatenate((parts[:, 2 * width :], 0 * parts[:, :width]), 1)), 0)


def order_of(axes):
    sizes = dict(x=4, zh=4, core=2, zl=2, y=4)
    places = np.indices([sizes[axis] for axis in axes]).reshape(len(axes), -1)
    at = dict(zip(axes, places))
    px = (at["x"] * 4 + at["zh"]) * 2 + at.get("core", 0)
    return px, at["zl"] * 4 + at["y"], ((at["x"] * 4 + at["zh"]) * 2 + at["zl"]) * 4 + at["y"]


FRONT_AXES = ("zh", "zl", "y", "core", "x")
BACK_AXES = ("zl", "y", "zh", "x")


def span_forward_tables():
    cos_tw, sin_tw = wave(np.arange(8), np.arange(128), 1024)
    twiddle = np.concatenate((cos_tw, sin_tw), 0).astype(np.float32)
    cos_t, sin_t = wave(np.arange(64), np.arange(128), 128)
    parts = three_part(np.concatenate((cos_t, sin_t), 1))
    return twiddle, np.concatenate((parts[:, :256], parts[:, 512:]), 0)


def middle_tables():
    base = np.arange(32)
    cos32, sin32 = wave(base, base, 32)
    eye8 = np.eye(8)
    over_px = np.concatenate((np.kron(cos32[:17], eye8), np.kron(-sin32[1:16], eye8)), 0)
    px, py, _ = order_of(FRONT_AXES)
    over_px = three_part(over_px[:, px * 8 + py])
    cos_tw, sin_tw = wave(base, base, 1024)
    spread = lambda t: np.repeat(np.tile(t, (1, 4)), 8, 0)
    turn_sign = np.where(base < 16, 1.0, -1.0)[:, None]
    lane_sign = np.where(np.arange(128) < 64, 1.0, -1.0)
    front_twiddle = np.concatenate(
        (
            spread(cos_tw),
            spread(turn_sign * sin_tw),
            spread(turn_sign * cos_tw) * lane_sign,
            -spread(sin_tw) * lane_sign,
        ),
        0,
    ).astype(np.float32)
    eye2 = np.eye(2)
    block = lambda t: np.kron(eye2, t)
    within = paired(np.block([[block(cos32), block(sin32)], [block(-sin32), block(cos32)]]))
    back = np.zeros((8, 2, 2, 4, 2, 2, 32))
    for py in range(8):
        for i in range(4):
            c, s = cos32[4 * py + i], sin32[4 * py + i]
            for s2 in range(2):
                back[py, 0, s2, i, s2, 0] = c
                back[py, 0, s2, i, s2, 1] = -s
                back[py, 1, s2, i, s2, 0] = s
                back[py, 1, s2, i, s2, 1] = c
    back = paired(back.reshape(128, 128))
    back_twiddle = np.zeros((2, 2, 8, 2, 4, 2, 2, 32))
    for core in range(2):
        c, s = wave(32 * core + base, base, 1024)
        c, s = (t.reshape(8, 1, 4, 1, 32) for t in (c, s))
        back_twiddle[core, 0, :, :, :, 0] = c
        back_twiddle[core, 0, :, :, :, 1] = -s
        back_twiddle[core, 1, :, :, :, 0] = s
        back_twiddle[core, 1, :, :, :, 1] = c
    back_twiddle = back_twiddle.reshape(256, 128).astype(np.float32)
    cos16, sin16 = wave(order_of(BACK_AXES)[0][:16] // 2, base, 16)
    final = paired(np.concatenate((np.kron(eye2, cos16), np.kron(eye2, sin16)), 1))
    return (over_px, front_twiddle, within), (back, back_twiddle, final)


def span_inverse_tables():
    cos_t, sin_t = wave(np.arange(64), np.arange(128), 128)
    one = 2.0 * np.concatenate((cos_t, sin_t), 1)
    table = three_part(np.kron(np.eye(2), one)[order_of(BACK_AXES)[2]], 0)
    cos_tw, sin_tw = wave(np.arange(8), np.arange(128), 1024)
    return table, np.concatenate((cos_tw, sin_tw), 0).astype(np.float32)


def split(x):
    high = x.astype(BF16)
    return high, (x - high.astype(F32)).astype(BF16)


def joined(x, axis):
    high, low = split(x)
    return jnp.concatenate((high, low, high), axis)


def halves_added(x):
    rows = x.shape[0] // 2
    return x[:rows] + x[rows:]


def dot_nn(a, b):
    return lax.dot_general(a, b, (((1,), (0,)), ((), ())), preferred_element_type=F32)


def dot_nt(a, b):
    return lax.dot_general(a, b, (((1,), (1,)), ((), ())), preferred_element_type=F32)


def span_forward_kernel(v_hbm, twiddle_hbm, table_hbm, out_ref, v_ref, twiddle_ref, table_ref, sems):
    copies = [
        pltpu.make_async_copy(v_hbm, v_ref, sems.at[0]),
        pltpu.make_async_copy(twiddle_hbm, twiddle_ref, sems.at[1]),
        pltpu.make_async_copy(table_hbm, table_ref, sems.at[2]),
    ]
    for copy in copies:
        copy.start()
    for copy in copies:
        copy.wait()
    x = [v_ref[pl.ds(s, 96, stride=8), :] for s in range(8)]
    e = [x[s] + x[s + 4] for s in range(4)]
    o = [x[s] - x[s + 4] for s in range(4)]
    e02, e13 = e[0] + e[2], e[1] + e[3]
    om, op = ROOT_HALF * (o[1] - o[3]), ROOT_HALF * (o[1] + o[3])
    e02m, e13m = e[0] - e[2], e[1] - e[3]
    one = (o[0] + om, -(o[2] + op))
    three = (o[0] - om, o[2] - op)
    spec = [
        (e02 + e13, None),
        one,
        (e02m, -e13m),
        three,
        (e02 - e13, None),
        (three[0], -three[1]),
        (e02m, e13m),
        (one[0], -one[1]),
    ]
    parts = []
    for k1 in range(8):
        re, im = spec[k1]
        cos_tw = twiddle_ref[pl.ds(k1, 1), :]
        sin_tw = twiddle_ref[pl.ds(8 + k1, 1), :]
        if k1 == 0:
            new_re, new_im = re, jnp.zeros_like(re)
        elif im is None:
            new_re, new_im = re * cos_tw, -(re * sin_tw)
        else:
            new_re, new_im = re * cos_tw + im * sin_tw, im * cos_tw - re * sin_tw
        parts.append((split(new_re), split(new_im)))
    table = table_ref[...]
    for j in range(4):
        columns = []
        for level in range(2):
            rows = []
            for c in range(3):
                cut = slice(32 * c, 32 * c + 32)
                for turn in range(2):
                    for k1 in (2 * j, 2 * j + 1):
                        re, im = parts[k1][0][level][cut], parts[k1][1][level][cut]
                        rows.append(jnp.concatenate((re, im) if turn == 0 else (im, -re), 1))
            columns.append(jnp.concatenate(rows, 0))
        result = halves_added(dot_nt(table, columns[0])) + dot_nt(table[:64], columns[1])
        for c in range(3):
            for half in range(2):
                first = 3 * (4 * (j % 2) + 2 * (j // 2) + half) + c
                out_ref[pl.ds(first, 32, stride=24), :] = result[32 * half : 32 * half + 32, 128 * c : 128 * c + 128]


def middle_front_kernel(anchor, band_hbm, r_ref, over_px_ref, front_tw_ref, within_ref, out_ref, band_ref, sem):
    band_copy = pltpu.make_async_copy(band_hbm, band_ref, sem)
    band_copy.start()
    data = jnp.concatenate([r_ref[pl.ds(c, 256, stride=3), :] for c in range(3)], 1)
    turned = dot_nn(over_px_ref[...], joined(data, 0))
    spectrum = []
    for c in range(3):
        cut = slice(128 * c, 128 * c + 128)
        rows = []
        for k1 in range(32):
            t1, t2, t3, t4 = [front_tw_ref[pl.ds(256 * t + 8 * k1, 8), :] for t in range(4)]
            m = min(k1, 32 - k1)
            p = turned[8 * m : 8 * m + 8, cut]
            if m % 16 == 0:
                rows.append(p * t1 + pltpu.roll(p * t4, 64, axis=1))
            else:
                q = turned[128 + 8 * m : 136 + 8 * m, cut]
                rows.append((p * t1 + q * t2) + pltpu.roll(q * t3 + p * t4, 64, axis=1))
        u = jnp.concatenate(split(jnp.concatenate(rows, 0)), 1)
        out = halves_added(dot_nt(within_ref[...], u))
        spectrum.append((out[:64], out[64:]))
    sub = lax.broadcasted_iota(jnp.int32, (8, 128), 0)
    lanes = lax.broadcasted_iota(jnp.int32, (8, 128), 1)
    band_copy.wait()
    band = jnp.zeros((8, 128), jnp.int32)
    count_one = jnp.int32(0)
    for y in range(8):
        band = jnp.where(sub == y, band_ref[y], band)
        count_one = count_one + band_ref[y]
    lane_band = (lanes // 32) % 2
    in_band = band == lane_band
    select = jnp.concatenate(
        [jnp.where(jnp.logical_and(in_band, lanes % 32 == k1), 1.0, 0.0).astype(F32) for k1 in range(32)], 0
    ).astype(BF16)
    select = jnp.concatenate((select, select), 0)
    one_f = jnp.full((8, 128), count_one, jnp.int32).astype(F32)
    count = jnp.where(lane_band == 1, one_f, 8.0 - one_f)
    weight = 1.0 / (count * float(NX * NZ * 1024))
    row64 = lax.broadcasted_iota(jnp.int32, (64, 128), 0)
    lane64 = lax.broadcasted_iota(jnp.int32, (64, 128), 1)
    scale = jnp.concatenate([weight] * 8, 0)
    scale = jnp.where(jnp.logical_and(anchor, row64 < 32), 0.5 * scale, scale)
    mean = jnp.logical_and(anchor, jnp.logical_and(row64 == 0, lane64 % 32 == 0))
    scale = jnp.where(mean, 0.0, scale)
    place = 0
    for left, right in PAIR_LIST:
        lr, li = spectrum[left]
        rr, ri = spectrum[right]
        values = [lr * rr + li * ri]
        if left != right:
            values.append(lr * ri - li * rr)
        for value in values:
            out_ref[64 * place : 64 * place + 64, :] = dot_nn(jnp.concatenate(split(value), 1), select) * scale
            place += 1


def middle_back_kernel(core, own_ref, got_ref, back_ref, back_tw_ref, final_ref, out_ref):
    first_core = core == 0
    zeros = jnp.zeros((32, 128), F32)
    columns = []
    for g in range(2):
        for k in range(2):
            place, pieces = 0, []
            for left, right in PAIR_LIST:
                for part in range(2):
                    if part == 1 and left == right:
                        pieces.append(zeros)
                        continue
                    rows = slice(64 * place + 32 * k, 64 * place + 32 * k + 32)
                    own, got = own_ref[rows, :], got_ref[rows, :]
                    pieces.append(jnp.where(first_core, own, got) if g == 0 else jnp.where(first_core, got, own))
                    place += 1
            for sp in range(3):
                columns.append(jnp.concatenate(pieces[4 * sp : 4 * sp + 4], 0))
    v = halves_added(dot_nn(back_ref[...], jnp.concatenate(split(jnp.concatenate(columns, 1)), 0)))
    lane = lax.broadcasted_iota(jnp.int32, (16, 128), 1)
    twiddle_row = pl.multiple_of(core * 128, 128)
    for py in range(8):
        t1 = back_tw_ref[pl.ds(twiddle_row + 8 * py, 8), :]
        t2 = back_tw_ref[pl.ds(twiddle_row + 64 + 8 * py, 8), :]
        re_rows, im_rows = [], []
        for column in range(12):
            cut = slice(128 * column, 128 * column + 128)
            vr, vi = v[16 * py : 16 * py + 8, cut], v[16 * py + 8 : 16 * py + 16, cut]
            re_rows.append(vr * t1 - vi * t2)
            im_rows.append(vr * t2 + vi * t1)
        rows = jnp.concatenate(split(jnp.concatenate(re_rows + im_rows, 0)), 1)
        out = halves_added(dot_nt(final_ref[...], jnp.concatenate((rows, rows[128:]), 0)))
        out_ref[pl.ds(48 * py, 16, stride=3), :] = out[:16, :128]
        out_ref[pl.ds(48 * py + 1, 16, stride=3), :] = jnp.where(lane < 64, out[:16, 128:], out[16:, 128:])
        out_ref[pl.ds(48 * py + 2, 16, stride=3), :] = out[16:, :128]


def span_inverse_kernel(r_ref, table_ref, twiddle_ref, out_hbm, out_ref, sems):
    copies = []
    table = table_ref[...]
    lhs = [r_ref[pl.ds(part, 128, stride=3), :].T for part in range(3)]
    sums = dot_nn(joined(jnp.concatenate(lhs, 0), 1), table)
    sub = lax.broadcasted_iota(jnp.int32, (8, 128), 0)
    for sp in range(3):
        for b in range(2):
            y = []
            for k1 in range(8):
                col = (k1 // 4) * 256
                at = (k1 % 4) * 24 + sp * 8
                row_re, row_im = [n if b == 0 else (n + 256 if n < 128 else n + 64) for n in (at, at + 96)]
                rc, rs = sums[row_re : row_re + 8, col : col + 128], sums[row_re : row_re + 8, col + 128 : col + 256]
                ic, is_ = sums[row_im : row_im + 8, col : col + 128], sums[row_im : row_im + 8, col + 128 : col + 256]
                zr, zi = rc - is_, rs + ic
                c, s = twiddle_ref[pl.ds(k1, 1), :], twiddle_ref[pl.ds(8 + k1, 1), :]
                if k1 == 0:
                    y.append((zr, None))
                elif k1 == 4:
                    y.append((zr * c - zi * s, None))
                else:
                    y.append((zr * c - zi * s, zr * s + zi * c))
            a = [None] + [y[k][0] + y[8 - k][0] for k in (1, 2, 3)]
            d = [None] + [y[k][1] - y[8 - k][1] for k in (1, 2, 3)]
            up, um = y[0][0] + y[4][0], y[0][0] - y[4][0]
            ap, am = a[1] + a[3], ROOT_HALF * (a[1] - a[3])
            dm, dp = d[1] - d[3], ROOT_HALF * (d[1] + d[3])
            upp, upm = up + a[2], up - a[2]
            ump, umm = um + d[2], um - d[2]
            outs = [
                upp + ap,
                umm + am - dp,
                upm - dm,
                ump - am - dp,
                upp - ap,
                umm - am + dp,
                upm + dm,
                ump + am + dp,
            ]
            for half in range(4):
                v0, v1 = outs[2 * half], outs[2 * half + 1]
                base = (sp * 2 * 2 + b) * 32 + half * 8
                out_ref[pl.ds(base, 8), :] = jnp.where(sub < 4, v0, pltpu.roll(v1, 4, axis=0))
                out_ref[pl.ds(base + 64, 8), :] = jnp.where(sub < 4, pltpu.roll(v0, 4, axis=0), v1)
        block = pl.ds(128 * sp, 128)
        copies.append(pltpu.make_async_copy(out_ref.at[block], out_hbm.at[block], sems.at[sp]))
        copies[-1].start()
    for copy in copies:
        copy.wait()


def spaces(*kinds):
    return [pl.BlockSpec(memory_space=kind) for kind in kinds]


VMEM, HBM = pltpu.VMEM, pltpu.HBM


def call(kernel, out_shape, in_specs, name, out_space=VMEM, scratch=()):
    return pl.pallas_call(
        kernel,
        out_shape=jax.ShapeDtypeStruct(out_shape, F32),
        in_specs=in_specs,
        out_specs=pl.BlockSpec(memory_space=out_space),
        scratch_shapes=list(scratch),
        name=name,
        compiler_params=pltpu.CompilerParams(vmem_limit_bytes=16 * 1024 * 1024),
    )


def in_hbm(x):
    return pltpu.with_memory_space_constraint(jnp.asarray(x), HBM)


def run_span_forward(velocity):
    twiddle, table = span_forward_tables()
    scratch = (VMEM((768, 128), F32), VMEM(twiddle.shape, F32), VMEM(table.shape, BF16), pltpu.SemaphoreType.DMA((3,)))
    run = call(span_forward_kernel, (768, 128), spaces(HBM, HBM, HBM), "span_forward", scratch=scratch)
    return run(in_hbm(velocity), in_hbm(twiddle), in_hbm(table))


def run_middle_front(received, band_of, anchor=None):
    def kernel(*refs):
        at_anchor = anchor
        if anchor is None:
            at_anchor = sum(lax.axis_index(axis) for axis in FRONT_AXES) == 0
        middle_front_kernel(at_anchor, *refs)

    scratch = (pltpu.SMEM((8,), jnp.int32), pltpu.SemaphoreType.DMA)
    run = call(kernel, (576, 128), spaces(HBM, *[VMEM] * 4), "middle_front", scratch=scratch)
    return run(in_hbm(band_of), received, *middle_tables()[0])


def run_middle_back(own, got, core=None):
    def kernel(*refs):
        middle_back_kernel(lax.axis_index("core") if core is None else core, *refs)

    return call(kernel, (384, 128), spaces(*[VMEM] * 5), "middle_back")(own, got, *middle_tables()[1])


def run_span_inverse(received):
    scratch = (VMEM((384, 128), F32), pltpu.SemaphoreType.DMA((3,)))
    run = call(span_inverse_kernel, (384, 128), spaces(VMEM, VMEM, VMEM), "span_inverse", HBM, scratch)
    return run(received, *span_inverse_tables())


def per_device(velocity, band_of):
    sent = run_span_forward(velocity.reshape(768, 128))
    received = lax.all_to_all(sent.reshape(256, 1, 384), FRONT_AXES, 0, 0, tiled=True)
    own = run_middle_front(received.reshape(768, 128), band_of)
    got = lax.ppermute(own, "core", ((0, 1), (1, 0)))
    back = run_middle_back(own, got)
    gathered = lax.all_to_all(back.reshape(128, 1, 384), BACK_AXES, 0, 0, tiled=True)
    out = run_span_inverse(gathered.reshape(384, 128))
    return out.reshape(6, 2, 8, 4, 128).transpose(0, 1, 3, 2, 4).reshape(6, 2, 4, 1024)


def solution(mesh):
    split_mesh = jax.sharding.Mesh(mesh.devices.reshape(4, 4, 2, 2, 4), ("x", "zh", "core", "zl", "y"))
    px, py = ("x", "zh", "core"), ("zl", "y")
    in_specs = (P(None, px, py, None), P())
    out_specs = P(None, None, px + py, None)
    return jax.shard_map(per_device, mesh=split_mesh, in_specs=in_specs, out_specs=out_specs, check_vma=False)
```

```python
import math

import jax
import jax.numpy as jnp
import numpy as np
from jax import lax
from jax.experimental import pallas as pl
from jax.experimental.pallas import tpu as pltpu
from jax.sharding import PartitionSpec as P

NX = 1024
NZ = 1024
NY = 8
NB = 2
PAIR_LIST = ((0, 0), (0, 1), (0, 2), (1, 1), (1, 2), (2, 2))
ROOT_HALF = math.sqrt(0.5)
F32 = jnp.float32
BF16 = jnp.bfloat16


def wave(rows, cols, length):
    angle = 2.0 * np.pi * (np.multiply.outer(rows, cols) % length) / length
    return np.cos(angle), np.sin(angle)


def three_part(table, axis=1):
    high = table.astype(np.float32).astype(jnp.bfloat16)
    low = (table - high.astype(np.float64)).astype(np.float32).astype(jnp.bfloat16)
    return np.concatenate((high, high, low), axis)


def paired(table):
    parts = three_part(table)
    width = table.shape[1]
    return np.concatenate((parts[:, : 2 * width], np.concatenate((parts[:, 2 * width :], 0 * parts[:, :width]), 1)), 0)


def order_of(axes):
    sizes = dict(x=4, zh=4, core=2, zl=2, y=4)
    places = np.indices([sizes[axis] for axis in axes]).reshape(len(axes), -1)
    at = dict(zip(axes, places))
    px = (at["x"] * 4 + at["zh"]) * 2 + at.get("core", 0)
    return px, at["zl"] * 4 + at["y"], ((at["zh"] * 2 + at["zl"]) * 4 + at["y"]) * 4 + at["x"]


FRONT_AXES = ("zh", "zl", "y", "x", "core")
BACK_AXES = ("zl", "y", "zh", "x")


def span_forward_tables():
    cos_tw, sin_tw = wave(np.arange(8), np.arange(128), 1024)
    twiddle = np.concatenate((cos_tw, sin_tw), 0).astype(np.float32)
    cos_t, sin_t = wave(np.arange(64), np.arange(128), 128)
    parts = three_part(np.concatenate((cos_t, sin_t), 1))
    return twiddle, np.concatenate((parts[:, :256], parts[:, 512:]), 0)


def middle_tables():
    base = np.arange(32)
    cos32, sin32 = wave(base, base, 32)
    eye8 = np.eye(8)
    over_px = np.concatenate((np.kron(cos32[:17], eye8), np.kron(-sin32[1:16], eye8)), 0)
    px, py, _ = order_of(FRONT_AXES)
    over_px = three_part(over_px[:, px * 8 + py])
    cos_tw, sin_tw = wave(base, base, 1024)
    spread = lambda t: np.repeat(np.tile(t, (1, 4)), 8, 0)
    turn_sign = np.where(base < 16, 1.0, -1.0)[:, None]
    lane_sign = np.where(np.arange(128) < 64, 1.0, -1.0)
    front_twiddle = np.concatenate(
        (
            spread(cos_tw),
            spread(turn_sign * sin_tw),
            spread(turn_sign * cos_tw) * lane_sign,
            -spread(sin_tw) * lane_sign,
        ),
        0,
    ).astype(np.float32)
    eye2 = np.eye(2)
    block = lambda t: np.kron(eye2, t)
    within = paired(np.block([[block(cos32), block(sin32)], [block(-sin32), block(cos32)]]))
    back = np.zeros((8, 2, 2, 4, 2, 2, 32))
    for py in range(8):
        for i in range(4):
            c, s = cos32[4 * py + i], sin32[4 * py + i]
            for s2 in range(2):
                back[py, 0, s2, i, s2, 0] = c
                back[py, 0, s2, i, s2, 1] = -s
                back[py, 1, s2, i, s2, 0] = s
                back[py, 1, s2, i, s2, 1] = c
    back = paired(back.reshape(128, 128))
    back_twiddle = np.zeros((2, 2, 8, 2, 4, 2, 2, 32))
    for core in range(2):
        c, s = wave(32 * core + base, base, 1024)
        c, s = (t.reshape(8, 1, 4, 1, 32) for t in (c, s))
        back_twiddle[core, 0, :, :, :, 0] = c
        back_twiddle[core, 0, :, :, :, 1] = -s
        back_twiddle[core, 1, :, :, :, 0] = s
        back_twiddle[core, 1, :, :, :, 1] = c
    back_twiddle = back_twiddle.reshape(256, 128).astype(np.float32)
    cos16, sin16 = wave(order_of(BACK_AXES)[0][:16] // 2, base, 16)
    final = paired(np.concatenate((np.kron(eye2, cos16), np.kron(eye2, sin16)), 1))
    return (over_px, front_twiddle, within), (back, back_twiddle, final)


def span_inverse_tables():
    cos_t, sin_t = wave(np.arange(64), np.arange(128), 128)
    one = 2.0 * np.concatenate((cos_t, sin_t), 1)
    table = three_part(np.kron(np.eye(2), one)[order_of(BACK_AXES)[2]], 0)
    cos_tw, sin_tw = wave(np.arange(8), np.arange(128), 1024)
    return table, np.concatenate((cos_tw, sin_tw), 0).astype(np.float32)


def split(x):
    high = x.astype(BF16)
    return high, (x - high.astype(F32)).astype(BF16)


def joined(x, axis):
    high, low = split(x)
    return jnp.concatenate((high, low, high), axis)


def halves_added(x):
    rows = x.shape[0] // 2
    return x[:rows] + x[rows:]


def dot_nn(a, b):
    return lax.dot_general(a, b, (((1,), (0,)), ((), ())), preferred_element_type=F32)


def dot_nt(a, b):
    return lax.dot_general(a, b, (((1,), (1,)), ((), ())), preferred_element_type=F32)


def span_forward_kernel(v_hbm, twiddle_hbm, table_hbm, out_ref, v_ref, twiddle_ref, table_ref, sems):
    copies = [
        pltpu.make_async_copy(v_hbm, v_ref, sems.at[0]),
        pltpu.make_async_copy(twiddle_hbm, twiddle_ref, sems.at[1]),
        pltpu.make_async_copy(table_hbm, table_ref, sems.at[2]),
    ]
    for copy in copies:
        copy.start()
    for copy in copies:
        copy.wait()
    x = [v_ref[pl.ds(s, 96, stride=8), :] for s in range(8)]
    e = [x[s] + x[s + 4] for s in range(4)]
    o = [x[s] - x[s + 4] for s in range(4)]
    e02, e13 = e[0] + e[2], e[1] + e[3]
    om, op = ROOT_HALF * (o[1] - o[3]), ROOT_HALF * (o[1] + o[3])
    e02m, e13m = e[0] - e[2], e[1] - e[3]
    one = (o[0] + om, -(o[2] + op))
    three = (o[0] - om, o[2] - op)
    spec = [
        (e02 + e13, None),
        one,
        (e02m, -e13m),
        three,
        (e02 - e13, None),
        (three[0], -three[1]),
        (e02m, e13m),
        (one[0], -one[1]),
    ]
    parts = []
    for k1 in range(8):
        re, im = spec[k1]
        cos_tw = twiddle_ref[pl.ds(k1, 1), :]
        sin_tw = twiddle_ref[pl.ds(8 + k1, 1), :]
        if k1 == 0:
            new_re, new_im = re, jnp.zeros_like(re)
        elif im is None:
            new_re, new_im = re * cos_tw, -(re * sin_tw)
        else:
            new_re, new_im = re * cos_tw + im * sin_tw, im * cos_tw - re * sin_tw
        parts.append((split(new_re), split(new_im)))
    table = table_ref[...]
    for j in range(4):
        columns = []
        for level in range(2):
            rows = []
            for c in range(3):
                cut = slice(32 * c, 32 * c + 32)
                for turn in range(2):
                    for k1 in (2 * j, 2 * j + 1):
                        re, im = parts[k1][0][level][cut], parts[k1][1][level][cut]
                        rows.append(jnp.concatenate((re, im) if turn == 0 else (im, -re), 1))
            columns.append(jnp.concatenate(rows, 0))
        result = halves_added(dot_nt(table, columns[0])) + dot_nt(table[:64], columns[1])
        for c in range(3):
            first = 384 * (j // 2) + 3 * (j % 2) + c
            out_ref[pl.ds(first, 64, stride=6), :] = result[:, 128 * c : 128 * c + 128]


def middle_front_kernel(anchor, band_hbm, r_ref, over_px_ref, front_tw_ref, within_ref, out_ref, band_ref, sem):
    band_copy = pltpu.make_async_copy(band_hbm, band_ref, sem)
    band_copy.start()
    data = jnp.concatenate([r_ref[pl.ds(c, 256, stride=3), :] for c in range(3)], 1)
    turned = dot_nn(over_px_ref[...], joined(data, 0))
    spectrum = []
    for c in range(3):
        cut = slice(128 * c, 128 * c + 128)
        rows = []
        for k1 in range(32):
            t1, t2, t3, t4 = [front_tw_ref[pl.ds(256 * t + 8 * k1, 8), :] for t in range(4)]
            m = min(k1, 32 - k1)
            p = turned[8 * m : 8 * m + 8, cut]
            if m % 16 == 0:
                rows.append(p * t1 + pltpu.roll(p * t4, 64, axis=1))
            else:
                q = turned[128 + 8 * m : 136 + 8 * m, cut]
                rows.append((p * t1 + q * t2) + pltpu.roll(q * t3 + p * t4, 64, axis=1))
        u = jnp.concatenate(split(jnp.concatenate(rows, 0)), 1)
        out = halves_added(dot_nt(within_ref[...], u))
        spectrum.append((out[:64], out[64:]))
    sub = lax.broadcasted_iota(jnp.int32, (8, 128), 0)
    lanes = lax.broadcasted_iota(jnp.int32, (8, 128), 1)
    band_copy.wait()
    band = jnp.zeros((8, 128), jnp.int32)
    count_one = jnp.int32(0)
    for y in range(8):
        band = jnp.where(sub == y, band_ref[y], band)
        count_one = count_one + band_ref[y]
    lane_band = (lanes // 32) % 2
    in_band = band == lane_band
    select = jnp.concatenate(
        [jnp.where(jnp.logical_and(in_band, lanes % 32 == k1), 1.0, 0.0).astype(F32) for k1 in range(32)], 0
    ).astype(BF16)
    select = jnp.concatenate((select, select), 0)
    one_f = jnp.full((8, 128), count_one, jnp.int32).astype(F32)
    count = jnp.where(lane_band == 1, one_f, 8.0 - one_f)
    weight = 1.0 / (count * float(NX * NZ * 1024))
    row64 = lax.broadcasted_iota(jnp.int32, (64, 128), 0)
    lane64 = lax.broadcasted_iota(jnp.int32, (64, 128), 1)
    scale = jnp.concatenate([weight] * 8, 0)
    scale = jnp.where(jnp.logical_and(anchor, row64 < 32), 0.5 * scale, scale)
    mean = jnp.logical_and(anchor, jnp.logical_and(row64 == 0, lane64 % 32 == 0))
    scale = jnp.where(mean, 0.0, scale)
    place = 0
    for left, right in PAIR_LIST:
        lr, li = spectrum[left]
        rr, ri = spectrum[right]
        values = [lr * rr + li * ri]
        if left != right:
            values.append(lr * ri - li * rr)
        for value in values:
            out_ref[64 * place : 64 * place + 64, :] = dot_nn(jnp.concatenate(split(value), 1), select) * scale
            place += 1


def back_rows(core, banded_ref, back_ref, back_tw_ref):
    zeros = jnp.zeros((32, 128), F32)
    columns = []
    for k in range(2):
        place, pieces = 0, []
        for left, right in PAIR_LIST:
            for part in range(2):
                if part == 1 and left == right:
                    pieces.append(zeros)
                    continue
                pieces.append(banded_ref[64 * place + 32 * k : 64 * place + 32 * k + 32, :])
                place += 1
        for sp in range(3):
            columns.append(jnp.concatenate(pieces[4 * sp : 4 * sp + 4], 0))
    v = halves_added(dot_nn(back_ref[...], jnp.concatenate(split(jnp.concatenate(columns, 1)), 0)))
    twiddle_row = pl.multiple_of(core * 128, 128)
    blocks = []
    for py in range(8):
        t1 = back_tw_ref[pl.ds(twiddle_row + 8 * py, 8), :]
        t2 = back_tw_ref[pl.ds(twiddle_row + 64 + 8 * py, 8), :]
        re_rows, im_rows = [], []
        for column in range(6):
            cut = slice(128 * column, 128 * column + 128)
            vr, vi = v[16 * py : 16 * py + 8, cut], v[16 * py + 8 : 16 * py + 16, cut]
            re_rows.append(vr * t1 - vi * t2)
            im_rows.append(vr * t2 + vi * t1)
        blocks.append(jnp.concatenate(split(jnp.concatenate(re_rows + im_rows, 0)), 1))
    return blocks


def middle_own_kernel(core, own_ref, back_ref, back_tw_ref, out_ref):
    for py, block in enumerate(back_rows(core, own_ref, back_ref, back_tw_ref)):
        out_ref[96 * py : 96 * py + 96, :] = block


def middle_back_kernel(core, rows_ref, got_ref, back_ref, back_tw_ref, final_ref, out_ref):
    first_core = core == 0
    lane = lax.broadcasted_iota(jnp.int32, (16, 128), 1)
    for py, got in enumerate(back_rows(core, got_ref, back_ref, back_tw_ref)):
        own = rows_ref[96 * py : 96 * py + 96, :]
        first = jnp.where(first_core, own, got)
        second = jnp.where(first_core, got, own)
        rows = jnp.concatenate((first[:48], second[:48], first[48:], second[48:]), 0)
        out = halves_added(dot_nt(final_ref[...], jnp.concatenate((rows, rows[128:]), 0)))
        out_ref[pl.ds(48 * py, 16, stride=3), :] = out[:16, :128]
        out_ref[pl.ds(48 * py + 1, 16, stride=3), :] = jnp.where(lane < 64, out[:16, 128:], out[16:, 128:])
        out_ref[pl.ds(48 * py + 2, 16, stride=3), :] = out[16:, :128]


def span_inverse_kernel(r_ref, table_ref, twiddle_ref, out_hbm, out_ref, sems):
    copies = []
    table = table_ref[...]
    lhs = [r_ref[pl.ds(part, 128, stride=3), :].T for part in range(3)]
    sums = dot_nn(joined(jnp.concatenate(lhs, 0), 1), table)
    sub = lax.broadcasted_iota(jnp.int32, (8, 128), 0)
    for sp in range(3):
        for b in range(2):
            y = []
            for k1 in range(8):
                col = (k1 // 4) * 256
                at = (k1 % 4) * 24 + sp * 8
                row_re, row_im = [n if b == 0 else (n + 256 if n < 128 else n + 64) for n in (at, at + 96)]
                rc, rs = sums[row_re : row_re + 8, col : col + 128], sums[row_re : row_re + 8, col + 128 : col + 256]
                ic, is_ = sums[row_im : row_im + 8, col : col + 128], sums[row_im : row_im + 8, col + 128 : col + 256]
                zr, zi = rc - is_, rs + ic
                c, s = twiddle_ref[pl.ds(k1, 1), :], twiddle_ref[pl.ds(8 + k1, 1), :]
                if k1 == 0:
                    y.append((zr, None))
                elif k1 == 4:
                    y.append((zr * c - zi * s, None))
                else:
                    y.append((zr * c - zi * s, zr * s + zi * c))
            a = [None] + [y[k][0] + y[8 - k][0] for k in (1, 2, 3)]
            d = [None] + [y[k][1] - y[8 - k][1] for k in (1, 2, 3)]
            up, um = y[0][0] + y[4][0], y[0][0] - y[4][0]
            ap, am = a[1] + a[3], ROOT_HALF * (a[1] - a[3])
            dm, dp = d[1] - d[3], ROOT_HALF * (d[1] + d[3])
            upp, upm = up + a[2], up - a[2]
            ump, umm = um + d[2], um - d[2]
            outs = [
                upp + ap,
                umm + am - dp,
                upm - dm,
                ump - am - dp,
                upp - ap,
                umm - am + dp,
                upm + dm,
                ump + am + dp,
            ]
            for half in range(4):
                v0, v1 = outs[2 * half], outs[2 * half + 1]
                base = (sp * 2 * 2 + b) * 32 + half * 8
                out_ref[pl.ds(base, 8), :] = jnp.where(sub < 4, v0, pltpu.roll(v1, 4, axis=0))
                out_ref[pl.ds(base + 64, 8), :] = jnp.where(sub < 4, pltpu.roll(v0, 4, axis=0), v1)
        block = pl.ds(128 * sp, 128)
        copies.append(pltpu.make_async_copy(out_ref.at[block], out_hbm.at[block], sems.at[sp]))
        copies[-1].start()
    for copy in copies:
        copy.wait()


def spaces(*kinds):
    return [pl.BlockSpec(memory_space=kind) for kind in kinds]


VMEM, HBM = pltpu.VMEM, pltpu.HBM


def call(kernel, out_shape, in_specs, name, out_space=VMEM, scratch=(), dtype=F32):
    return pl.pallas_call(
        kernel,
        out_shape=jax.ShapeDtypeStruct(out_shape, dtype),
        in_specs=in_specs,
        out_specs=pl.BlockSpec(memory_space=out_space),
        scratch_shapes=list(scratch),
        name=name,
        compiler_params=pltpu.CompilerParams(vmem_limit_bytes=16 * 1024 * 1024),
    )


def in_hbm(x):
    return pltpu.with_memory_space_constraint(jnp.asarray(x), HBM)


def run_span_forward(velocity):
    twiddle, table = span_forward_tables()
    scratch = (VMEM((768, 128), F32), VMEM(twiddle.shape, F32), VMEM(table.shape, BF16), pltpu.SemaphoreType.DMA((3,)))
    run = call(span_forward_kernel, (768, 128), spaces(HBM, HBM, HBM), "span_forward", scratch=scratch)
    return run(in_hbm(velocity), in_hbm(twiddle), in_hbm(table))


def run_middle_front(received, band_of, anchor=None):
    def kernel(*refs):
        at_anchor = anchor
        if anchor is None:
            at_anchor = sum(lax.axis_index(axis) for axis in FRONT_AXES) == 0
        middle_front_kernel(at_anchor, *refs)

    scratch = (pltpu.SMEM((8,), jnp.int32), pltpu.SemaphoreType.DMA)
    run = call(kernel, (576, 128), spaces(HBM, *[VMEM] * 4), "middle_front", scratch=scratch)
    return run(in_hbm(band_of), received, *middle_tables()[0])


def run_middle_own(own, core=None):
    def kernel(*refs):
        middle_own_kernel(lax.axis_index("core") if core is None else core, *refs)

    back, twiddle, _ = middle_tables()[1]
    return call(kernel, (768, 256), spaces(*[VMEM] * 3), "middle_own", dtype=BF16)(own, back, twiddle)


def run_middle_back(rows, got, core=None):
    def kernel(*refs):
        middle_back_kernel(lax.axis_index("core") if core is None else core, *refs)

    return call(kernel, (384, 128), spaces(*[VMEM] * 5), "middle_back")(rows, got, *middle_tables()[1])


def run_span_inverse(received):
    scratch = (VMEM((384, 128), F32), pltpu.SemaphoreType.DMA((3,)))
    run = call(span_inverse_kernel, (384, 128), spaces(VMEM, VMEM, VMEM), "span_inverse", HBM, scratch)
    return run(received, *span_inverse_tables())


def per_device(velocity, band_of):
    sent = run_span_forward(velocity.reshape(768, 128))
    received = lax.all_to_all(sent.reshape(256, 1, 384), FRONT_AXES, 0, 0, tiled=True)
    own = run_middle_front(received.reshape(768, 128), band_of)
    got = lax.ppermute(own, "core", ((0, 1), (1, 0)))
    back = run_middle_back(run_middle_own(own), got)
    gathered = lax.all_to_all(back.reshape(128, 1, 384), BACK_AXES, 0, 0, tiled=True)
    out = run_span_inverse(gathered.reshape(384, 128))
    return out.reshape(6, 2, 8, 4, 128).transpose(0, 1, 3, 2, 4).reshape(6, 2, 4, 1024)


def solution(mesh):
    split_mesh = jax.sharding.Mesh(mesh.devices.reshape(4, 4, 2, 2, 4), ("x", "zh", "core", "zl", "y"))
    px, py = ("x", "zh", "core"), ("zl", "y")
    in_specs = (P(None, px, py, None), P())
    out_specs = P(None, None, px + py, None)
    return jax.shard_map(per_device, mesh=split_mesh, in_specs=in_specs, out_specs=out_specs, check_vma=False)
```

```python
import math

import jax
import jax.numpy as jnp
import numpy as np
from jax import lax
from jax.experimental import pallas as pl
from jax.experimental.pallas import tpu as pltpu
from jax.sharding import PartitionSpec as P

NX = 1024
NZ = 1024
NY = 8
NB = 2
PAIR_LIST = ((0, 0), (0, 1), (0, 2), (1, 1), (1, 2), (2, 2))
ROOT_HALF = math.sqrt(0.5)
F32 = jnp.float32
BF16 = jnp.bfloat16


def wave(rows, cols, length):
    angle = 2.0 * np.pi * (np.multiply.outer(rows, cols) % length) / length
    return np.cos(angle), np.sin(angle)


def three_part(table, axis=1):
    high = table.astype(np.float32).astype(jnp.bfloat16)
    low = (table - high.astype(np.float64)).astype(np.float32).astype(jnp.bfloat16)
    return np.concatenate((high, high, low), axis)


def paired(table):
    parts = three_part(table)
    width = table.shape[1]
    return np.concatenate((parts[:, : 2 * width], np.concatenate((parts[:, 2 * width :], 0 * parts[:, :width]), 1)), 0)


def order_of(axes):
    sizes = dict(x=4, zh=4, core=2, zl=2, y=4)
    places = np.indices([sizes[axis] for axis in axes]).reshape(len(axes), -1)
    at = dict(zip(axes, places))
    px = (at["x"] * 4 + at["zh"]) * 2 + at.get("core", 0)
    return px, at["zl"] * 4 + at["y"], ((at["zh"] * 2 + at["zl"]) * 4 + at["y"]) * 4 + at["x"]


FRONT_AXES = ("zh", "zl", "y", "x", "core")
BACK_AXES = ("zl", "y", "zh", "x")


def span_forward_tables():
    cos_tw, sin_tw = wave(np.arange(8), np.arange(128), 1024)
    twiddle = np.concatenate((cos_tw, sin_tw), 0).astype(np.float32)
    cos_t, sin_t = wave(np.arange(64), np.arange(128), 128)
    parts = three_part(np.concatenate((cos_t, sin_t), 1))
    return twiddle, np.concatenate((parts[:, :256], parts[:, 512:]), 0)


def middle_tables():
    base = np.arange(32)
    cos32, sin32 = wave(base, base, 32)
    eye8 = np.eye(8)
    over_px = np.concatenate((np.kron(cos32[:17], eye8), np.kron(-sin32[1:16], eye8)), 0)
    px, py, _ = order_of(FRONT_AXES)
    over_px = three_part(over_px[:, px * 8 + py])
    cos_tw, sin_tw = wave(base, base, 1024)
    spread = lambda t: np.repeat(np.tile(t, (1, 4)), 8, 0)
    turn_sign = np.where(base < 16, 1.0, -1.0)[:, None]
    lane_sign = np.where(np.arange(128) < 64, 1.0, -1.0)
    front_twiddle = np.concatenate(
        (
            spread(cos_tw),
            spread(turn_sign * sin_tw),
            spread(turn_sign * cos_tw) * lane_sign,
            -spread(sin_tw) * lane_sign,
        ),
        0,
    ).astype(np.float32)
    eye2 = np.eye(2)
    block = lambda t: np.kron(eye2, t)
    within = paired(np.block([[block(cos32), block(sin32)], [block(-sin32), block(cos32)]]))
    back = np.zeros((8, 2, 2, 4, 2, 2, 32))
    for py in range(8):
        for i in range(4):
            c, s = cos32[4 * py + i], sin32[4 * py + i]
            for s2 in range(2):
                back[py, 0, s2, i, s2, 0] = c
                back[py, 0, s2, i, s2, 1] = -s
                back[py, 1, s2, i, s2, 0] = s
                back[py, 1, s2, i, s2, 1] = c
    back = paired(back.reshape(128, 128))
    back_twiddle = np.zeros((2, 2, 8, 2, 4, 2, 2, 32))
    for core in range(2):
        c, s = wave(32 * core + base, base, 1024)
        c, s = (t.reshape(8, 1, 4, 1, 32) for t in (c, s))
        back_twiddle[core, 0, :, :, :, 0] = c
        back_twiddle[core, 0, :, :, :, 1] = -s
        back_twiddle[core, 1, :, :, :, 0] = s
        back_twiddle[core, 1, :, :, :, 1] = c
    back_twiddle = back_twiddle.reshape(256, 128).astype(np.float32)
    cos16, sin16 = wave(order_of(BACK_AXES)[0][:16] // 2, base, 16)
    final = paired(np.concatenate((np.kron(eye2, cos16), np.kron(eye2, sin16)), 1))
    return (over_px, front_twiddle, within), (back, back_twiddle, final)


def span_inverse_tables():
    cos_t, sin_t = wave(np.arange(64), np.arange(128), 128)
    one = 2.0 * np.concatenate((cos_t, sin_t), 1)
    table = three_part(np.kron(np.eye(2), one)[order_of(BACK_AXES)[2]], 0)
    cos_tw, sin_tw = wave(np.arange(8), np.arange(128), 1024)
    return table, np.concatenate((cos_tw, sin_tw), 0).astype(np.float32)


def split(x):
    high = x.astype(BF16)
    return high, (x - high.astype(F32)).astype(BF16)


def joined(x, axis):
    high, low = split(x)
    return jnp.concatenate((high, low, high), axis)


def halves_added(x):
    rows = x.shape[0] // 2
    return x[:rows] + x[rows:]


def dot_nn(a, b):
    return lax.dot_general(a, b, (((1,), (0,)), ((), ())), preferred_element_type=F32)


def dot_nt(a, b):
    return lax.dot_general(a, b, (((1,), (1,)), ((), ())), preferred_element_type=F32)


def span_forward_kernel(v_hbm, twiddle_hbm, table_hbm, out_ref, v_ref, twiddle_ref, table_ref, sems):
    copies = [
        pltpu.make_async_copy(v_hbm, v_ref, sems.at[0]),
        pltpu.make_async_copy(twiddle_hbm, twiddle_ref, sems.at[1]),
        pltpu.make_async_copy(table_hbm, table_ref, sems.at[2]),
    ]
    for copy in copies:
        copy.start()
    for copy in copies:
        copy.wait()
    x = [v_ref[pl.ds(s, 96, stride=8), :] for s in range(8)]
    e = [x[s] + x[s + 4] for s in range(4)]
    o = [x[s] - x[s + 4] for s in range(4)]
    e02, e13 = e[0] + e[2], e[1] + e[3]
    om, op = ROOT_HALF * (o[1] - o[3]), ROOT_HALF * (o[1] + o[3])
    e02m, e13m = e[0] - e[2], e[1] - e[3]
    one = (o[0] + om, -(o[2] + op))
    three = (o[0] - om, o[2] - op)
    spec = [
        (e02 + e13, None),
        one,
        (e02m, -e13m),
        three,
        (e02 - e13, None),
        (three[0], -three[1]),
        (e02m, e13m),
        (one[0], -one[1]),
    ]
    parts = []
    for k1 in range(8):
        re, im = spec[k1]
        cos_tw = twiddle_ref[pl.ds(k1, 1), :]
        sin_tw = twiddle_ref[pl.ds(8 + k1, 1), :]
        if k1 == 0:
            new_re, new_im = re, jnp.zeros_like(re)
        elif im is None:
            new_re, new_im = re * cos_tw, -(re * sin_tw)
        else:
            new_re, new_im = re * cos_tw + im * sin_tw, im * cos_tw - re * sin_tw
        parts.append((split(new_re), split(new_im)))
    table = table_ref[...]
    for j in range(4):
        columns = []
        for level in range(2):
            rows = []
            for c in range(3):
                cut = slice(32 * c, 32 * c + 32)
                for turn in range(2):
                    for k1 in (2 * j, 2 * j + 1):
                        re, im = parts[k1][0][level][cut], parts[k1][1][level][cut]
                        rows.append(jnp.concatenate((re, im) if turn == 0 else (im, -re), 1))
            columns.append(jnp.concatenate(rows, 0))
        result = halves_added(dot_nt(table, columns[0])) + dot_nt(table[:64], columns[1])
        for c in range(3):
            first = 384 * (j // 2) + 3 * (j % 2) + c
            out_ref[pl.ds(first, 64, stride=6), :] = result[:, 128 * c : 128 * c + 128]


def middle_front_kernel(anchor, band_hbm, r_ref, over_px_ref, front_tw_ref, within_ref, out_ref, packed_ref, band_ref, sem):
    band_copy = pltpu.make_async_copy(band_hbm, band_ref, sem)
    band_copy.start()
    data = jnp.concatenate([r_ref[pl.ds(c, 256, stride=3), :] for c in range(3)], 1)
    turned = dot_nn(over_px_ref[...], joined(data, 0))
    spectrum = []
    for c in range(3):
        cut = slice(128 * c, 128 * c + 128)
        rows = []
        for k1 in range(32):
            t1, t2, t3, t4 = [front_tw_ref[pl.ds(256 * t + 8 * k1, 8), :] for t in range(4)]
            m = min(k1, 32 - k1)
            p = turned[8 * m : 8 * m + 8, cut]
            if m % 16 == 0:
                rows.append(p * t1 + pltpu.roll(p * t4, 64, axis=1))
            else:
                q = turned[128 + 8 * m : 136 + 8 * m, cut]
                rows.append((p * t1 + q * t2) + pltpu.roll(q * t3 + p * t4, 64, axis=1))
        u = jnp.concatenate(split(jnp.concatenate(rows, 0)), 1)
        out = halves_added(dot_nt(within_ref[...], u))
        spectrum.append((out[:64], out[64:]))
    sub = lax.broadcasted_iota(jnp.int32, (8, 128), 0)
    lanes = lax.broadcasted_iota(jnp.int32, (8, 128), 1)
    band_copy.wait()
    band = jnp.zeros((8, 128), jnp.int32)
    count_one = jnp.int32(0)
    for y in range(8):
        band = jnp.where(sub == y, band_ref[y], band)
        count_one = count_one + band_ref[y]
    lane_band = (lanes // 32) % 2
    in_band = band == lane_band
    select = jnp.concatenate(
        [jnp.where(jnp.logical_and(in_band, lanes % 32 == k1), 1.0, 0.0).astype(F32) for k1 in range(32)], 0
    ).astype(BF16)
    select = jnp.concatenate((select, select), 0)
    one_f = jnp.full((8, 128), count_one, jnp.int32).astype(F32)
    count = jnp.where(lane_band == 1, one_f, 8.0 - one_f)
    weight = 1.0 / (count * float(NX * NZ * 1024))
    row64 = lax.broadcasted_iota(jnp.int32, (64, 128), 0)
    lane64 = lax.broadcasted_iota(jnp.int32, (64, 128), 1)
    scale = jnp.concatenate([weight] * 8, 0)
    scale = jnp.where(jnp.logical_and(anchor, row64 < 32), 0.5 * scale, scale)
    mean = jnp.logical_and(anchor, jnp.logical_and(row64 == 0, lane64 % 32 == 0))
    scale = jnp.where(mean, 0.0, scale)
    place = 0
    for left, right in PAIR_LIST:
        lr, li = spectrum[left]
        rr, ri = spectrum[right]
        values = [lr * rr + li * ri]
        if left != right:
            values.append(lr * ri - li * rr)
        for value in values:
            sums = dot_nn(jnp.concatenate(split(value), 1), select) * scale
            out_ref[64 * place : 64 * place + 64, :] = sums
            packed_ref[32 * place : 32 * place + 32, :] = jnp.where(lane64[:32] < 64, sums[:32], sums[32:])
            place += 1


def back_rows(core, banded, back_ref, back_tw_ref):
    zeros = jnp.zeros((32, 128), F32)
    columns = []
    for k in range(2):
        place, pieces = 0, []
        for left, right in PAIR_LIST:
            for part in range(2):
                if part == 1 and left == right:
                    pieces.append(zeros)
                    continue
                pieces.append(banded[place][k])
                place += 1
        for sp in range(3):
            columns.append(jnp.concatenate(pieces[4 * sp : 4 * sp + 4], 0))
    v = halves_added(dot_nn(back_ref[...], jnp.concatenate(split(jnp.concatenate(columns, 1)), 0)))
    twiddle_row = pl.multiple_of(core * 128, 128)
    blocks = []
    for py in range(8):
        t1 = back_tw_ref[pl.ds(twiddle_row + 8 * py, 8), :]
        t2 = back_tw_ref[pl.ds(twiddle_row + 64 + 8 * py, 8), :]
        re_rows, im_rows = [], []
        for column in range(6):
            cut = slice(128 * column, 128 * column + 128)
            vr, vi = v[16 * py : 16 * py + 8, cut], v[16 * py + 8 : 16 * py + 16, cut]
            re_rows.append(vr * t1 - vi * t2)
            im_rows.append(vr * t2 + vi * t1)
        blocks.append(jnp.concatenate(split(jnp.concatenate(re_rows + im_rows, 0)), 1))
    return blocks


def middle_own_kernel(core, own_ref, back_ref, back_tw_ref, out_ref):
    banded = [[own_ref[64 * place + 32 * k : 64 * place + 32 * k + 32, :] for k in range(2)] for place in range(9)]
    for py, block in enumerate(back_rows(core, banded, back_ref, back_tw_ref)):
        out_ref[96 * py : 96 * py + 96, :] = block


def middle_back_kernel(core, rows_ref, got_ref, back_ref, back_tw_ref, final_ref, out_ref):
    first_core = core == 0
    lane = lax.broadcasted_iota(jnp.int32, (16, 128), 1)
    first_half = lax.broadcasted_iota(jnp.int32, (32, 128), 1) < 64
    banded = []
    for place in range(9):
        packed = got_ref[32 * place : 32 * place + 32, :]
        turned = pltpu.roll(packed, 64, axis=1)
        banded.append((jnp.where(first_half, packed, turned), jnp.where(first_half, turned, packed)))
    for py, got in enumerate(back_rows(core, banded, back_ref, back_tw_ref)):
        own = rows_ref[96 * py : 96 * py + 96, :]
        first = jnp.where(first_core, own, got)
        second = jnp.where(first_core, got, own)
        rows = jnp.concatenate((first[:48], second[:48], first[48:], second[48:]), 0)
        out = halves_added(dot_nt(final_ref[...], jnp.concatenate((rows, rows[128:]), 0)))
        out_ref[pl.ds(48 * py, 16, stride=3), :] = out[:16, :128]
        out_ref[pl.ds(48 * py + 1, 16, stride=3), :] = jnp.where(lane < 64, out[:16, 128:], out[16:, 128:])
        out_ref[pl.ds(48 * py + 2, 16, stride=3), :] = out[16:, :128]


def span_inverse_kernel(r_ref, table_ref, twiddle_ref, out_hbm, out_ref, sems):
    copies = []
    table = table_ref[...]
    lhs = [r_ref[pl.ds(part, 128, stride=3), :].T for part in range(3)]
    sums = dot_nn(joined(jnp.concatenate(lhs, 0), 1), table)
    sub = lax.broadcasted_iota(jnp.int32, (8, 128), 0)
    for sp in range(3):
        for b in range(2):
            y = []
            for k1 in range(8):
                col = (k1 // 4) * 256
                at = (k1 % 4) * 24 + sp * 8
                row_re, row_im = [n if b == 0 else (n + 256 if n < 128 else n + 64) for n in (at, at + 96)]
                rc, rs = sums[row_re : row_re + 8, col : col + 128], sums[row_re : row_re + 8, col + 128 : col + 256]
                ic, is_ = sums[row_im : row_im + 8, col : col + 128], sums[row_im : row_im + 8, col + 128 : col + 256]
                zr, zi = rc - is_, rs + ic
                c, s = twiddle_ref[pl.ds(k1, 1), :], twiddle_ref[pl.ds(8 + k1, 1), :]
                if k1 == 0:
                    y.append((zr, None))
                elif k1 == 4:
                    y.append((zr * c - zi * s, None))
                else:
                    y.append((zr * c - zi * s, zr * s + zi * c))
            a = [None] + [y[k][0] + y[8 - k][0] for k in (1, 2, 3)]
            d = [None] + [y[k][1] - y[8 - k][1] for k in (1, 2, 3)]
            up, um = y[0][0] + y[4][0], y[0][0] - y[4][0]
            ap, am = a[1] + a[3], ROOT_HALF * (a[1] - a[3])
            dm, dp = d[1] - d[3], ROOT_HALF * (d[1] + d[3])
            upp, upm = up + a[2], up - a[2]
            ump, umm = um + d[2], um - d[2]
            outs = [
                upp + ap,
                umm + am - dp,
                upm - dm,
                ump - am - dp,
                upp - ap,
                umm - am + dp,
                upm + dm,
                ump + am + dp,
            ]
            for half in range(4):
                v0, v1 = outs[2 * half], outs[2 * half + 1]
                base = (sp * 2 * 2 + b) * 32 + half * 8
                out_ref[pl.ds(base, 8), :] = jnp.where(sub < 4, v0, pltpu.roll(v1, 4, axis=0))
                out_ref[pl.ds(base + 64, 8), :] = jnp.where(sub < 4, pltpu.roll(v0, 4, axis=0), v1)
        block = pl.ds(128 * sp, 128)
        copies.append(pltpu.make_async_copy(out_ref.at[block], out_hbm.at[block], sems.at[sp]))
        copies[-1].start()
    for copy in copies:
        copy.wait()


def spaces(*kinds):
    return [pl.BlockSpec(memory_space=kind) for kind in kinds]


VMEM, HBM = pltpu.VMEM, pltpu.HBM


def call(kernel, out_shapes, in_specs, name, out_space=VMEM, scratch=(), dtype=F32):
    shapes = [jax.ShapeDtypeStruct(shape, dtype) for shape in out_shapes]
    out_specs = spaces(*[out_space] * len(shapes))
    return pl.pallas_call(
        kernel,
        out_shape=shapes if len(shapes) > 1 else shapes[0],
        in_specs=in_specs,
        out_specs=out_specs if len(shapes) > 1 else out_specs[0],
        scratch_shapes=list(scratch),
        name=name,
        compiler_params=pltpu.CompilerParams(vmem_limit_bytes=16 * 1024 * 1024),
    )


def in_hbm(x):
    return pltpu.with_memory_space_constraint(jnp.asarray(x), HBM)


def run_span_forward(velocity):
    twiddle, table = span_forward_tables()
    scratch = (VMEM((768, 128), F32), VMEM(twiddle.shape, F32), VMEM(table.shape, BF16), pltpu.SemaphoreType.DMA((3,)))
    run = call(span_forward_kernel, [(768, 128)], spaces(HBM, HBM, HBM), "span_forward", scratch=scratch)
    return run(in_hbm(velocity), in_hbm(twiddle), in_hbm(table))


def run_middle_front(received, band_of, anchor=None):
    def kernel(*refs):
        at_anchor = anchor
        if anchor is None:
            at_anchor = sum(lax.axis_index(axis) for axis in FRONT_AXES) == 0
        middle_front_kernel(at_anchor, *refs)

    scratch = (pltpu.SMEM((8,), jnp.int32), pltpu.SemaphoreType.DMA)
    run = call(kernel, [(576, 128), (288, 128)], spaces(HBM, *[VMEM] * 4), "middle_front", scratch=scratch)
    return run(in_hbm(band_of), received, *middle_tables()[0])


def run_middle_own(own, core=None):
    def kernel(*refs):
        middle_own_kernel(lax.axis_index("core") if core is None else core, *refs)

    back, twiddle, _ = middle_tables()[1]
    return call(kernel, [(768, 256)], spaces(*[VMEM] * 3), "middle_own", dtype=BF16)(own, back, twiddle)


def run_middle_back(rows, got, core=None):
    def kernel(*refs):
        middle_back_kernel(lax.axis_index("core") if core is None else core, *refs)

    return call(kernel, [(384, 128)], spaces(*[VMEM] * 5), "middle_back")(rows, got, *middle_tables()[1])


def run_span_inverse(received):
    scratch = (VMEM((384, 128), F32), pltpu.SemaphoreType.DMA((3,)))
    run = call(span_inverse_kernel, [(384, 128)], spaces(VMEM, VMEM, VMEM), "span_inverse", HBM, scratch)
    return run(received, *span_inverse_tables())


def per_device(velocity, band_of):
    sent = run_span_forward(velocity.reshape(768, 128))
    received = lax.all_to_all(sent.reshape(256, 1, 384), FRONT_AXES, 0, 0, tiled=True)
    own, packed = run_middle_front(received.reshape(768, 128), band_of)
    got = lax.ppermute(packed, "core", ((0, 1), (1, 0)))
    back = run_middle_back(run_middle_own(own), got)
    gathered = lax.all_to_all(back.reshape(128, 1, 384), BACK_AXES, 0, 0, tiled=True)
    out = run_span_inverse(gathered.reshape(384, 128))
    return out.reshape(6, 2, 8, 4, 128).transpose(0, 1, 3, 2, 4).reshape(6, 2, 4, 1024)


def solution(mesh):
    split_mesh = jax.sharding.Mesh(mesh.devices.reshape(4, 4, 2, 2, 4), ("x", "zh", "core", "zl", "y"))
    px, py = ("x", "zh", "core"), ("zl", "y")
    in_specs = (P(None, px, py, None), P())
    out_specs = P(None, None, px + py, None)
    return jax.shard_map(per_device, mesh=split_mesh, in_specs=in_specs, out_specs=out_specs, check_vma=False)
```

```python
import math

import jax
import jax.numpy as jnp
import numpy as np
from jax import lax
from jax.experimental import pallas as pl
from jax.experimental.pallas import tpu as pltpu
from jax.sharding import PartitionSpec as P

NX = 1024
NZ = 1024
NY = 8
NB = 2
PAIR_LIST = ((0, 0), (0, 1), (0, 2), (1, 1), (1, 2), (2, 2))
ROOT_HALF = math.sqrt(0.5)
F32 = jnp.float32
BF16 = jnp.bfloat16


def wave(rows, cols, length):
    angle = 2.0 * np.pi * (np.multiply.outer(rows, cols) % length) / length
    return np.cos(angle), np.sin(angle)


def three_part(table, axis=1):
    high = table.astype(np.float32).astype(jnp.bfloat16)
    low = (table - high.astype(np.float64)).astype(np.float32).astype(jnp.bfloat16)
    return np.concatenate((high, high, low), axis)


def paired(table):
    parts = three_part(table)
    width = table.shape[1]
    return np.concatenate((parts[:, : 2 * width], np.concatenate((parts[:, 2 * width :], 0 * parts[:, :width]), 1)), 0)


def order_of(axes):
    sizes = dict(x=4, zh=4, core=2, zl=2, y=4)
    places = np.indices([sizes[axis] for axis in axes]).reshape(len(axes), -1)
    at = dict(zip(axes, places))
    px = (at["x"] * 4 + at["zh"]) * 2 + at.get("core", 0)
    return px, at["zl"] * 4 + at["y"], ((at["x"] * 4 + at["zh"]) * 2 + at["zl"]) * 4 + at["y"]


FRONT_AXES = ("zh", "zl", "y", "core", "x")
BACK_AXES = ("zl", "y", "zh", "x")


def span_forward_tables():
    cos_tw, sin_tw = wave(np.arange(8), np.arange(128), 1024)
    twiddle = np.concatenate((cos_tw, sin_tw), 0).astype(np.float32)
    cos_t, sin_t = wave(np.arange(64), np.arange(128), 128)
    parts = three_part(np.concatenate((cos_t, sin_t), 1))
    return twiddle, np.concatenate((parts[:, :256], parts[:, 512:]), 0)


def middle_tables():
    base = np.arange(32)
    cos32, sin32 = wave(base, base, 32)
    eye8 = np.eye(8)
    over_px = np.concatenate((np.kron(cos32[:17], eye8), np.kron(-sin32[1:16], eye8)), 0)
    px, py, _ = order_of(FRONT_AXES)
    over_px = three_part(over_px[:, px * 8 + py])
    cos_tw, sin_tw = wave(base, base, 1024)
    spread = lambda t: np.repeat(np.tile(t, (1, 4)), 8, 0)
    turn_sign = np.where(base < 16, 1.0, -1.0)[:, None]
    lane_sign = np.where(np.arange(128) < 64, 1.0, -1.0)
    front_twiddle = np.concatenate(
        (
            spread(cos_tw),
            spread(turn_sign * sin_tw),
            spread(turn_sign * cos_tw) * lane_sign,
            -spread(sin_tw) * lane_sign,
        ),
        0,
    ).astype(np.float32)
    eye2 = np.eye(2)
    block = lambda t: np.kron(eye2, t)
    within = paired(np.block([[block(cos32), block(sin32)], [block(-sin32), block(cos32)]]))
    back = np.zeros((8, 2, 2, 4, 2, 2, 32))
    for py in range(8):
        for i in range(4):
            c, s = cos32[4 * py + i], sin32[4 * py + i]
            for s2 in range(2):
                back[py, 0, s2, i, s2, 0] = c
                back[py, 0, s2, i, s2, 1] = -s
                back[py, 1, s2, i, s2, 0] = s
                back[py, 1, s2, i, s2, 1] = c
    back = paired(back.reshape(128, 128))
    back_twiddle = np.zeros((2, 2, 8, 2, 4, 2, 2, 32))
    for core in range(2):
        c, s = wave(32 * core + base, base, 1024)
        c, s = (t.reshape(8, 1, 4, 1, 32) for t in (c, s))
        back_twiddle[core, 0, :, :, :, 0] = c
        back_twiddle[core, 0, :, :, :, 1] = -s
        back_twiddle[core, 1, :, :, :, 0] = s
        back_twiddle[core, 1, :, :, :, 1] = c
    back_twiddle = back_twiddle.reshape(256, 128).astype(np.float32)
    cos16, sin16 = wave(order_of(BACK_AXES)[0][:16] // 2, base, 16)
    final = paired(np.concatenate((np.kron(eye2, cos16), np.kron(eye2, sin16)), 1))
    return (over_px, front_twiddle, within), (back, back_twiddle, final)


def span_inverse_tables():
    cos_t, sin_t = wave(np.arange(64), np.arange(128), 128)
    one = 2.0 * np.concatenate((cos_t, sin_t), 1)
    table = three_part(np.kron(np.eye(2), one)[order_of(BACK_AXES)[2]], 0)
    cos_tw, sin_tw = wave(np.arange(8), np.arange(128), 1024)
    return table, np.concatenate((cos_tw, sin_tw), 0).astype(np.float32)


def split(x):
    high = x.astype(BF16)
    return high, (x - high.astype(F32)).astype(BF16)


def joined(x, axis):
    high, low = split(x)
    return jnp.concatenate((high, low, high), axis)


def halves_added(x):
    rows = x.shape[0] // 2
    return x[:rows] + x[rows:]


def dot_nn(a, b):
    return lax.dot_general(a, b, (((1,), (0,)), ((), ())), preferred_element_type=F32)


def dot_nt(a, b):
    return lax.dot_general(a, b, (((1,), (1,)), ((), ())), preferred_element_type=F32)


def span_forward_kernel(v_hbm, twiddle_hbm, table_hbm, out_ref, v_ref, twiddle_ref, table_ref, sems):
    copies = [
        pltpu.make_async_copy(v_hbm, v_ref, sems.at[0]),
        pltpu.make_async_copy(twiddle_hbm, twiddle_ref, sems.at[1]),
        pltpu.make_async_copy(table_hbm, table_ref, sems.at[2]),
    ]
    for copy in copies:
        copy.start()
    for copy in copies:
        copy.wait()
    x = [v_ref[pl.ds(s, 96, stride=8), :] for s in range(8)]
    e = [x[s] + x[s + 4] for s in range(4)]
    o = [x[s] - x[s + 4] for s in range(4)]
    e02, e13 = e[0] + e[2], e[1] + e[3]
    om, op = ROOT_HALF * (o[1] - o[3]), ROOT_HALF * (o[1] + o[3])
    e02m, e13m = e[0] - e[2], e[1] - e[3]
    one = (o[0] + om, -(o[2] + op))
    three = (o[0] - om, o[2] - op)
    spec = [
        (e02 + e13, None),
        one,
        (e02m, -e13m),
        three,
        (e02 - e13, None),
        (three[0], -three[1]),
        (e02m, e13m),
        (one[0], -one[1]),
    ]
    parts = []
    for k1 in range(8):
        re, im = spec[k1]
        cos_tw = twiddle_ref[pl.ds(k1, 1), :]
        sin_tw = twiddle_ref[pl.ds(8 + k1, 1), :]
        if k1 == 0:
            new_re, new_im = re, jnp.zeros_like(re)
        elif im is None:
            new_re, new_im = re * cos_tw, -(re * sin_tw)
        else:
            new_re, new_im = re * cos_tw + im * sin_tw, im * cos_tw - re * sin_tw
        parts.append((split(new_re), split(new_im)))
    table = table_ref[...]
    for j in range(4):
        columns = []
        for level in range(2):
            rows = []
            for c in range(3):
                cut = slice(32 * c, 32 * c + 32)
                for turn in range(2):
                    for k1 in (2 * j, 2 * j + 1):
                        re, im = parts[k1][0][level][cut], parts[k1][1][level][cut]
                        rows.append(jnp.concatenate((re, im) if turn == 0 else (im, -re), 1))
            columns.append(jnp.concatenate(rows, 0))
        result = halves_added(dot_nt(table, columns[0])) + dot_nt(table[:64], columns[1])
        for c in range(3):
            for half in range(2):
                first = 3 * (4 * (j % 2) + 2 * (j // 2) + half) + c
                out_ref[pl.ds(first, 32, stride=24), :] = result[32 * half : 32 * half + 32, 128 * c : 128 * c + 128]


def middle_front_kernel(anchor, band_hbm, r_ref, over_px_ref, front_tw_ref, within_ref, out_ref, packed_ref, band_ref, sem):
    band_copy = pltpu.make_async_copy(band_hbm, band_ref, sem)
    band_copy.start()
    data = jnp.concatenate([r_ref[pl.ds(c, 256, stride=3), :] for c in range(3)], 1)
    turned = dot_nn(over_px_ref[...], joined(data, 0))
    spectrum = []
    for c in range(3):
        cut = slice(128 * c, 128 * c + 128)
        rows = []
        for k1 in range(32):
            t1, t2, t3, t4 = [front_tw_ref[pl.ds(256 * t + 8 * k1, 8), :] for t in range(4)]
            m = min(k1, 32 - k1)
            p = turned[8 * m : 8 * m + 8, cut]
            if m % 16 == 0:
                rows.append(p * t1 + pltpu.roll(p * t4, 64, axis=1))
            else:
                q = turned[128 + 8 * m : 136 + 8 * m, cut]
                rows.append((p * t1 + q * t2) + pltpu.roll(q * t3 + p * t4, 64, axis=1))
        u = jnp.concatenate(split(jnp.concatenate(rows, 0)), 1)
        out = halves_added(dot_nt(within_ref[...], u))
        spectrum.append((out[:64], out[64:]))
    sub = lax.broadcasted_iota(jnp.int32, (8, 128), 0)
    lanes = lax.broadcasted_iota(jnp.int32, (8, 128), 1)
    band_copy.wait()
    band = jnp.zeros((8, 128), jnp.int32)
    count_one = jnp.int32(0)
    for y in range(8):
        band = jnp.where(sub == y, band_ref[y], band)
        count_one = count_one + band_ref[y]
    lane_band = (lanes // 32) % 2
    in_band = band == lane_band
    select = jnp.concatenate(
        [jnp.where(jnp.logical_and(in_band, lanes % 32 == k1), 1.0, 0.0).astype(F32) for k1 in range(32)], 0
    ).astype(BF16)
    select = jnp.concatenate((select, select), 0)
    one_f = jnp.full((8, 128), count_one, jnp.int32).astype(F32)
    count = jnp.where(lane_band == 1, one_f, 8.0 - one_f)
    weight = 1.0 / (count * float(NX * NZ * 1024))
    row64 = lax.broadcasted_iota(jnp.int32, (64, 128), 0)
    lane64 = lax.broadcasted_iota(jnp.int32, (64, 128), 1)
    scale = jnp.concatenate([weight] * 8, 0)
    scale = jnp.where(jnp.logical_and(anchor, row64 < 32), 0.5 * scale, scale)
    mean = jnp.logical_and(anchor, jnp.logical_and(row64 == 0, lane64 % 32 == 0))
    scale = jnp.where(mean, 0.0, scale)
    place = 0
    for left, right in PAIR_LIST:
        lr, li = spectrum[left]
        rr, ri = spectrum[right]
        values = [lr * rr + li * ri]
        if left != right:
            values.append(lr * ri - li * rr)
        for value in values:
            sums = dot_nn(jnp.concatenate(split(value), 1), select) * scale
            out_ref[64 * place : 64 * place + 64, :] = sums
            packed_ref[32 * place : 32 * place + 32, :] = jnp.where(lane64[:32] < 64, sums[:32], sums[32:])
            place += 1


def back_rows(core, banded, back_ref, back_tw_ref):
    zeros = jnp.zeros((32, 128), F32)
    columns = []
    for k in range(2):
        place, pieces = 0, []
        for left, right in PAIR_LIST:
            for part in range(2):
                if part == 1 and left == right:
                    pieces.append(zeros)
                    continue
                pieces.append(banded[place][k])
                place += 1
        for sp in range(3):
            columns.append(jnp.concatenate(pieces[4 * sp : 4 * sp + 4], 0))
    v = halves_added(dot_nn(back_ref[...], jnp.concatenate(split(jnp.concatenate(columns, 1)), 0)))
    twiddle_row = pl.multiple_of(core * 128, 128)
    blocks = []
    for py in range(8):
        t1 = back_tw_ref[pl.ds(twiddle_row + 8 * py, 8), :]
        t2 = back_tw_ref[pl.ds(twiddle_row + 64 + 8 * py, 8), :]
        re_rows, im_rows = [], []
        for column in range(6):
            cut = slice(128 * column, 128 * column + 128)
            vr, vi = v[16 * py : 16 * py + 8, cut], v[16 * py + 8 : 16 * py + 16, cut]
            re_rows.append(vr * t1 - vi * t2)
            im_rows.append(vr * t2 + vi * t1)
        blocks.append(jnp.concatenate(split(jnp.concatenate(re_rows + im_rows, 0)), 1))
    return blocks


def middle_own_kernel(core, own_ref, back_ref, back_tw_ref, out_ref):
    banded = [[own_ref[64 * place + 32 * k : 64 * place + 32 * k + 32, :] for k in range(2)] for place in range(9)]
    for py, block in enumerate(back_rows(core, banded, back_ref, back_tw_ref)):
        out_ref[96 * py : 96 * py + 96, :] = block


def middle_back_kernel(core, rows_ref, got_ref, back_ref, back_tw_ref, final_ref, out_ref):
    first_core = core == 0
    lane = lax.broadcasted_iota(jnp.int32, (16, 128), 1)
    first_half = lax.broadcasted_iota(jnp.int32, (32, 128), 1) < 64
    banded = []
    for place in range(9):
        packed = got_ref[32 * place : 32 * place + 32, :]
        turned = pltpu.roll(packed, 64, axis=1)
        banded.append((jnp.where(first_half, packed, turned), jnp.where(first_half, turned, packed)))
    for py, got in enumerate(back_rows(core, banded, back_ref, back_tw_ref)):
        own = rows_ref[96 * py : 96 * py + 96, :]
        first = jnp.where(first_core, own, got)
        second = jnp.where(first_core, got, own)
        rows = jnp.concatenate((first[:48], second[:48], first[48:], second[48:]), 0)
        out = halves_added(dot_nt(final_ref[...], jnp.concatenate((rows, rows[128:]), 0)))
        out_ref[pl.ds(48 * py, 16, stride=3), :] = out[:16, :128]
        out_ref[pl.ds(48 * py + 1, 16, stride=3), :] = jnp.where(lane < 64, out[:16, 128:], out[16:, 128:])
        out_ref[pl.ds(48 * py + 2, 16, stride=3), :] = out[16:, :128]


def span_inverse_kernel(r_ref, table_ref, twiddle_ref, out_hbm, out_ref, sems):
    copies = []
    table = table_ref[...]
    lhs = [r_ref[pl.ds(part, 128, stride=3), :].T for part in range(3)]
    sums = dot_nn(joined(jnp.concatenate(lhs, 0), 1), table)
    sub = lax.broadcasted_iota(jnp.int32, (8, 128), 0)
    for sp in range(3):
        for b in range(2):
            y = []
            for k1 in range(8):
                col = (k1 // 4) * 256
                at = (k1 % 4) * 24 + sp * 8
                row_re, row_im = [n if b == 0 else (n + 256 if n < 128 else n + 64) for n in (at, at + 96)]
                rc, rs = sums[row_re : row_re + 8, col : col + 128], sums[row_re : row_re + 8, col + 128 : col + 256]
                ic, is_ = sums[row_im : row_im + 8, col : col + 128], sums[row_im : row_im + 8, col + 128 : col + 256]
                zr, zi = rc - is_, rs + ic
                c, s = twiddle_ref[pl.ds(k1, 1), :], twiddle_ref[pl.ds(8 + k1, 1), :]
                if k1 == 0:
                    y.append((zr, None))
                elif k1 == 4:
                    y.append((zr * c - zi * s, None))
                else:
                    y.append((zr * c - zi * s, zr * s + zi * c))
            a = [None] + [y[k][0] + y[8 - k][0] for k in (1, 2, 3)]
            d = [None] + [y[k][1] - y[8 - k][1] for k in (1, 2, 3)]
            up, um = y[0][0] + y[4][0], y[0][0] - y[4][0]
            ap, am = a[1] + a[3], ROOT_HALF * (a[1] - a[3])
            dm, dp = d[1] - d[3], ROOT_HALF * (d[1] + d[3])
            upp, upm = up + a[2], up - a[2]
            ump, umm = um + d[2], um - d[2]
            outs = [
                upp + ap,
                umm + am - dp,
                upm - dm,
                ump - am - dp,
                upp - ap,
                umm - am + dp,
                upm + dm,
                ump + am + dp,
            ]
            for half in range(4):
                v0, v1 = outs[2 * half], outs[2 * half + 1]
                base = (sp * 2 * 2 + b) * 32 + half * 8
                out_ref[pl.ds(base, 8), :] = jnp.where(sub < 4, v0, pltpu.roll(v1, 4, axis=0))
                out_ref[pl.ds(base + 64, 8), :] = jnp.where(sub < 4, pltpu.roll(v0, 4, axis=0), v1)
        block = pl.ds(128 * sp, 128)
        copies.append(pltpu.make_async_copy(out_ref.at[block], out_hbm.at[block], sems.at[sp]))
        copies[-1].start()
    for copy in copies:
        copy.wait()


def spaces(*kinds):
    return [pl.BlockSpec(memory_space=kind) for kind in kinds]


VMEM, HBM = pltpu.VMEM, pltpu.HBM


def call(kernel, out_shapes, in_specs, name, out_space=VMEM, scratch=(), dtype=F32):
    shapes = [jax.ShapeDtypeStruct(shape, dtype) for shape in out_shapes]
    out_specs = spaces(*[out_space] * len(shapes))
    return pl.pallas_call(
        kernel,
        out_shape=shapes if len(shapes) > 1 else shapes[0],
        in_specs=in_specs,
        out_specs=out_specs if len(shapes) > 1 else out_specs[0],
        scratch_shapes=list(scratch),
        name=name,
        compiler_params=pltpu.CompilerParams(vmem_limit_bytes=16 * 1024 * 1024),
    )


def in_hbm(x):
    return pltpu.with_memory_space_constraint(jnp.asarray(x), HBM)


def run_span_forward(velocity):
    twiddle, table = span_forward_tables()
    scratch = (VMEM((768, 128), F32), VMEM(twiddle.shape, F32), VMEM(table.shape, BF16), pltpu.SemaphoreType.DMA((3,)))
    run = call(span_forward_kernel, [(768, 128)], spaces(HBM, HBM, HBM), "span_forward", scratch=scratch)
    return run(in_hbm(velocity), in_hbm(twiddle), in_hbm(table))


def run_middle_front(received, band_of, anchor=None):
    def kernel(*refs):
        at_anchor = anchor
        if anchor is None:
            at_anchor = sum(lax.axis_index(axis) for axis in FRONT_AXES) == 0
        middle_front_kernel(at_anchor, *refs)

    scratch = (pltpu.SMEM((8,), jnp.int32), pltpu.SemaphoreType.DMA)
    run = call(kernel, [(576, 128), (288, 128)], spaces(HBM, *[VMEM] * 4), "middle_front", scratch=scratch)
    return run(in_hbm(band_of), received, *middle_tables()[0])


def run_middle_own(own, core=None):
    def kernel(*refs):
        middle_own_kernel(lax.axis_index("core") if core is None else core, *refs)

    back, twiddle, _ = middle_tables()[1]
    return call(kernel, [(768, 256)], spaces(*[VMEM] * 3), "middle_own", dtype=BF16)(own, back, twiddle)


def run_middle_back(rows, got, core=None):
    def kernel(*refs):
        middle_back_kernel(lax.axis_index("core") if core is None else core, *refs)

    return call(kernel, [(384, 128)], spaces(*[VMEM] * 5), "middle_back")(rows, got, *middle_tables()[1])


def run_span_inverse(received):
    scratch = (VMEM((384, 128), F32), pltpu.SemaphoreType.DMA((3,)))
    run = call(span_inverse_kernel, [(384, 128)], spaces(VMEM, VMEM, VMEM), "span_inverse", HBM, scratch)
    return run(received, *span_inverse_tables())


def per_device(velocity, band_of):
    sent = run_span_forward(velocity.reshape(768, 128))
    received = lax.all_to_all(sent.reshape(256, 1, 384), FRONT_AXES, 0, 0, tiled=True)
    own, packed = run_middle_front(received.reshape(768, 128), band_of)
    got = lax.ppermute(packed, "core", ((0, 1), (1, 0)))
    back = run_middle_back(run_middle_own(own), got)
    gathered = lax.all_to_all(back.reshape(128, 1, 384), BACK_AXES, 0, 0, tiled=True)
    out = run_span_inverse(gathered.reshape(384, 128))
    return out.reshape(6, 2, 8, 4, 128).transpose(0, 1, 3, 2, 4).reshape(6, 2, 4, 1024)


def solution(mesh):
    split_mesh = jax.sharding.Mesh(mesh.devices.reshape(4, 4, 2, 2, 4), ("x", "zh", "core", "zl", "y"))
    px, py = ("x", "zh", "core"), ("zl", "y")
    in_specs = (P(None, px, py, None), P())
    out_specs = P(None, None, px + py, None)
    return jax.shard_map(per_device, mesh=split_mesh, in_specs=in_specs, out_specs=out_specs, check_vma=False)
```

```python
import math

import jax
import jax.numpy as jnp
import numpy as np
from jax import lax
from jax.experimental import pallas as pl
from jax.experimental.pallas import tpu as pltpu
from jax.sharding import PartitionSpec as P

NX = 1024
NZ = 1024
NY = 8
NB = 2
PAIR_LIST = ((0, 0), (0, 1), (0, 2), (1, 1), (1, 2), (2, 2))
ROOT_HALF = math.sqrt(0.5)
F32 = jnp.float32
BF16 = jnp.bfloat16


def wave(rows, cols, length):
    angle = 2.0 * np.pi * (np.multiply.outer(rows, cols) % length) / length
    return np.cos(angle), np.sin(angle)


def three_part(table, axis=1):
    high = table.astype(np.float32).astype(jnp.bfloat16)
    low = (table - high.astype(np.float64)).astype(np.float32).astype(jnp.bfloat16)
    return np.concatenate((high, high, low), axis)


def paired(table):
    parts = three_part(table)
    width = table.shape[1]
    return np.concatenate((parts[:, : 2 * width], np.concatenate((parts[:, 2 * width :], 0 * parts[:, :width]), 1)), 0)


def order_of(axes):
    sizes = dict(x=4, zh=4, core=2, zl=2, y=4)
    places = np.indices([sizes[axis] for axis in axes]).reshape(len(axes), -1)
    at = dict(zip(axes, places))
    px = (at["x"] * 4 + at["zh"]) * 2 + at.get("core", 0)
    return px, at["zl"] * 4 + at["y"], ((at["zh"] * 2 + at["zl"]) * 4 + at["y"]) * 4 + at["x"]


FRONT_AXES = ("zh", "zl", "y", "x", "core")
BACK_AXES = ("zl", "y", "zh", "x")


def span_forward_tables():
    cos_tw, sin_tw = wave(np.arange(8), np.arange(128), 1024)
    twiddle = np.concatenate((cos_tw, sin_tw), 0).astype(np.float32)
    cos_t, sin_t = wave(np.arange(64), np.arange(128), 128)
    parts = three_part(np.concatenate((cos_t, sin_t), 1))
    return twiddle, np.concatenate((parts[:, :256], parts[:, 512:]), 0)


def middle_tables():
    base = np.arange(32)
    cos32, sin32 = wave(base, base, 32)
    eye8 = np.eye(8)
    over_px = np.concatenate((np.kron(cos32[:17], eye8), np.kron(-sin32[1:16], eye8)), 0)
    px, py, _ = order_of(FRONT_AXES)
    over_px = three_part(over_px[:, px * 8 + py])
    cos_tw, sin_tw = wave(base, base, 1024)
    spread = lambda t: np.repeat(np.tile(t, (1, 4)), 8, 0)
    turn_sign = np.where(base < 16, 1.0, -1.0)[:, None]
    lane_sign = np.where(np.arange(128) < 64, 1.0, -1.0)
    front_twiddle = np.concatenate(
        (
            spread(cos_tw),
            spread(turn_sign * sin_tw),
            spread(turn_sign * cos_tw) * lane_sign,
            -spread(sin_tw) * lane_sign,
        ),
        0,
    ).astype(np.float32)
    eye2 = np.eye(2)
    block = lambda t: np.kron(eye2, t)
    within = paired(np.block([[block(cos32), block(sin32)], [block(-sin32), block(cos32)]]))
    back = np.zeros((8, 2, 2, 4, 2, 2, 32))
    for py in range(8):
        for i in range(4):
            c, s = cos32[4 * py + i], sin32[4 * py + i]
            for s2 in range(2):
                back[py, 0, s2, i, s2, 0] = c
                back[py, 0, s2, i, s2, 1] = -s
                back[py, 1, s2, i, s2, 0] = s
                back[py, 1, s2, i, s2, 1] = c
    back = paired(back.reshape(128, 128))
    back_twiddle = np.zeros((2, 2, 8, 2, 4, 2, 2, 32))
    for core in range(2):
        c, s = wave(32 * core + base, base, 1024)
        c, s = (t.reshape(8, 1, 4, 1, 32) for t in (c, s))
        back_twiddle[core, 0, :, :, :, 0] = c
        back_twiddle[core, 0, :, :, :, 1] = -s
        back_twiddle[core, 1, :, :, :, 0] = s
        back_twiddle[core, 1, :, :, :, 1] = c
    back_twiddle = back_twiddle.reshape(256, 128).astype(np.float32)
    cos16, sin16 = wave(order_of(BACK_AXES)[0][:16] // 2, base, 16)
    final = paired(np.concatenate((np.kron(eye2, cos16), np.kron(eye2, sin16)), 1))
    return (over_px, front_twiddle, within), (back, back_twiddle, final)


def span_inverse_tables():
    cos_t, sin_t = wave(np.arange(64), np.arange(128), 128)
    one = 2.0 * np.concatenate((cos_t, sin_t), 1)
    table = three_part(np.kron(np.eye(2), one)[order_of(BACK_AXES)[2]], 0)
    cos_tw, sin_tw = wave(np.arange(8), np.arange(128), 1024)
    return table, np.concatenate((cos_tw, sin_tw), 0).astype(np.float32)


def split(x):
    high = x.astype(BF16)
    return high, (x - high.astype(F32)).astype(BF16)


def joined(x, axis):
    high, low = split(x)
    return jnp.concatenate((high, low, high), axis)


def halves_added(x):
    rows = x.shape[0] // 2
    return x[:rows] + x[rows:]


def dot_nn(a, b):
    return lax.dot_general(a, b, (((1,), (0,)), ((), ())), preferred_element_type=F32)


def dot_nt(a, b):
    return lax.dot_general(a, b, (((1,), (1,)), ((), ())), preferred_element_type=F32)


def span_forward_kernel(v_hbm, twiddle_hbm, table_hbm, out_ref, v_ref, twiddle_ref, table_ref, sems):
    copies = [
        pltpu.make_async_copy(v_hbm, v_ref, sems.at[0]),
        pltpu.make_async_copy(twiddle_hbm, twiddle_ref, sems.at[1]),
        pltpu.make_async_copy(table_hbm, table_ref, sems.at[2]),
    ]
    for copy in copies:
        copy.start()
    for copy in copies:
        copy.wait()
    x = [v_ref[pl.ds(s, 96, stride=8), :] for s in range(8)]
    e = [x[s] + x[s + 4] for s in range(4)]
    o = [x[s] - x[s + 4] for s in range(4)]
    e02, e13 = e[0] + e[2], e[1] + e[3]
    om, op = ROOT_HALF * (o[1] - o[3]), ROOT_HALF * (o[1] + o[3])
    e02m, e13m = e[0] - e[2], e[1] - e[3]
    one = (o[0] + om, -(o[2] + op))
    three = (o[0] - om, o[2] - op)
    spec = [
        (e02 + e13, None),
        one,
        (e02m, -e13m),
        three,
        (e02 - e13, None),
        (three[0], -three[1]),
        (e02m, e13m),
        (one[0], -one[1]),
    ]
    parts = []
    for k1 in range(8):
        re, im = spec[k1]
        cos_tw = twiddle_ref[pl.ds(k1, 1), :]
        sin_tw = twiddle_ref[pl.ds(8 + k1, 1), :]
        if k1 == 0:
            new_re, new_im = re, jnp.zeros_like(re)
        elif im is None:
            new_re, new_im = re * cos_tw, -(re * sin_tw)
        else:
            new_re, new_im = re * cos_tw + im * sin_tw, im * cos_tw - re * sin_tw
        parts.append((split(new_re), split(new_im)))
    table = table_ref[...]
    for j in range(4):
        columns = []
        for level in range(2):
            rows = []
            for c in range(3):
                cut = slice(32 * c, 32 * c + 32)
                for turn in range(2):
                    for k1 in (2 * j, 2 * j + 1):
                        re, im = parts[k1][0][level][cut], parts[k1][1][level][cut]
                        rows.append(jnp.concatenate((re, im) if turn == 0 else (im, -re), 1))
            columns.append(jnp.concatenate(rows, 0))
        result = halves_added(dot_nt(table, columns[0])) + dot_nt(table[:64], columns[1])
        for c in range(3):
            first = 384 * (j // 2) + 3 * (j % 2) + c
            out_ref[pl.ds(first, 64, stride=6), :] = result[:, 128 * c : 128 * c + 128]


def middle_front_kernel(anchor, band_hbm, r_ref, over_px_ref, front_tw_ref, within_ref, out_ref, packed_ref, band_ref, sem):
    band_copy = pltpu.make_async_copy(band_hbm, band_ref, sem)
    band_copy.start()
    data = jnp.concatenate([r_ref[pl.ds(c, 256, stride=3), :] for c in range(3)], 1)
    turned = dot_nn(over_px_ref[...], joined(data, 0))
    spectrum = []
    for c in range(3):
        cut = slice(128 * c, 128 * c + 128)
        rows = []
        for k1 in range(32):
            t1, t2, t3, t4 = [front_tw_ref[pl.ds(256 * t + 8 * k1, 8), :] for t in range(4)]
            m = min(k1, 32 - k1)
            p = turned[8 * m : 8 * m + 8, cut]
            if m % 16 == 0:
                rows.append(p * t1 + pltpu.roll(p * t4, 64, axis=1))
            else:
                q = turned[128 + 8 * m : 136 + 8 * m, cut]
                rows.append((p * t1 + q * t2) + pltpu.roll(q * t3 + p * t4, 64, axis=1))
        u = jnp.concatenate(split(jnp.concatenate(rows, 0)), 1)
        out = halves_added(dot_nt(within_ref[...], u))
        spectrum.append((out[:64], out[64:]))
    sub = lax.broadcasted_iota(jnp.int32, (8, 128), 0)
    lanes = lax.broadcasted_iota(jnp.int32, (8, 128), 1)
    band_copy.wait()
    band = jnp.zeros((8, 128), jnp.int32)
    count_one = jnp.int32(0)
    for y in range(8):
        band = jnp.where(sub == y, band_ref[y], band)
        count_one = count_one + band_ref[y]
    lane_band = (lanes // 32) % 2
    in_band = band == lane_band
    select = jnp.concatenate(
        [jnp.where(jnp.logical_and(in_band, lanes % 32 == k1), 1.0, 0.0).astype(F32) for k1 in range(32)], 0
    ).astype(BF16)
    select = jnp.concatenate((select, select), 0)
    one_f = jnp.full((8, 128), count_one, jnp.int32).astype(F32)
    count = jnp.where(lane_band == 1, one_f, 8.0 - one_f)
    weight = 1.0 / (count * float(NX * NZ * 1024))
    row64 = lax.broadcasted_iota(jnp.int32, (64, 128), 0)
    lane64 = lax.broadcasted_iota(jnp.int32, (64, 128), 1)
    scale = jnp.concatenate([weight] * 8, 0)
    scale = jnp.where(jnp.logical_and(anchor, row64 < 32), 0.5 * scale, scale)
    mean = jnp.logical_and(anchor, jnp.logical_and(row64 == 0, lane64 % 32 == 0))
    scale = jnp.where(mean, 0.0, scale)
    place = 0
    for left, right in PAIR_LIST:
        lr, li = spectrum[left]
        rr, ri = spectrum[right]
        values = [lr * rr + li * ri]
        if left != right:
            values.append(lr * ri - li * rr)
        for value in values:
            sums = dot_nn(jnp.concatenate(split(value), 1), select) * scale
            out_ref[64 * place : 64 * place + 64, :] = sums
            packed_ref[32 * place : 32 * place + 32, :] = jnp.where(lane64[:32] < 64, sums[:32], sums[32:])
            place += 1


def back_rows(core, banded, back_ref, back_tw_ref):
    zeros = jnp.zeros((32, 128), F32)
    columns = []
    for k in range(2):
        place, pieces = 0, []
        for left, right in PAIR_LIST:
            for part in range(2):
                if part == 1 and left == right:
                    pieces.append(zeros)
                    continue
                pieces.append(banded[place][k])
                place += 1
        for sp in range(3):
            columns.append(jnp.concatenate(pieces[4 * sp : 4 * sp + 4], 0))
    v = halves_added(dot_nn(back_ref[...], jnp.concatenate(split(jnp.concatenate(columns, 1)), 0)))
    twiddle_row = pl.multiple_of(core * 128, 128)
    blocks = []
    for py in range(8):
        t1 = back_tw_ref[pl.ds(twiddle_row + 8 * py, 8), :]
        t2 = back_tw_ref[pl.ds(twiddle_row + 64 + 8 * py, 8), :]
        re_rows, im_rows = [], []
        for column in range(6):
            cut = slice(128 * column, 128 * column + 128)
            vr, vi = v[16 * py : 16 * py + 8, cut], v[16 * py + 8 : 16 * py + 16, cut]
            re_rows.append(vr * t1 - vi * t2)
            im_rows.append(vr * t2 + vi * t1)
        blocks.append(jnp.concatenate(split(jnp.concatenate(re_rows + im_rows, 0)), 1))
    return blocks


def middle_own_kernel(core, own_ref, back_ref, back_tw_ref, out_ref):
    banded = [[own_ref[64 * place + 32 * k : 64 * place + 32 * k + 32, :] for k in range(2)] for place in range(9)]
    for py, block in enumerate(back_rows(core, banded, back_ref, back_tw_ref)):
        out_ref[96 * py : 96 * py + 96, :] = block


def middle_back_kernel(core, rows_ref, got_ref, back_ref, back_tw_ref, final_ref, out_ref):
    first_core = core == 0
    lane = lax.broadcasted_iota(jnp.int32, (16, 128), 1)
    first_half = lax.broadcasted_iota(jnp.int32, (32, 128), 1) < 64
    banded = []
    for place in range(9):
        packed = got_ref[32 * place : 32 * place + 32, :]
        turned = pltpu.roll(packed, 64, axis=1)
        banded.append((jnp.where(first_half, packed, turned), jnp.where(first_half, turned, packed)))
    for py, got in enumerate(back_rows(core, banded, back_ref, back_tw_ref)):
        own = rows_ref[96 * py : 96 * py + 96, :]
        first = jnp.where(first_core, own, got)
        second = jnp.where(first_core, got, own)
        rows = jnp.concatenate((first[:48], second[:48], first[48:], second[48:]), 0)
        out = halves_added(dot_nt(final_ref[...], jnp.concatenate((rows, rows[128:]), 0)))
        out_ref[pl.ds(48 * py, 16, stride=3), :] = out[:16, :128]
        out_ref[pl.ds(48 * py + 1, 16, stride=3), :] = jnp.where(lane < 64, out[:16, 128:], out[16:, 128:])
        out_ref[pl.ds(48 * py + 2, 16, stride=3), :] = out[16:, :128]


def span_inverse_kernel(r_ref, table_ref, twiddle_ref, out_hbm, out_ref, sems):
    copies = []
    table = table_ref[...]
    lhs = [r_ref[pl.ds(part, 128, stride=3), :].T for part in range(3)]
    sums = dot_nn(joined(jnp.concatenate(lhs, 0), 1), table)
    sub = lax.broadcasted_iota(jnp.int32, (8, 128), 0)
    for sp in range(3):
        for b in range(2):
            y = []
            for k1 in range(8):
                col = (k1 // 4) * 256
                at = (k1 % 4) * 24 + sp * 8
                row_re, row_im = [n if b == 0 else (n + 256 if n < 128 else n + 64) for n in (at, at + 96)]
                rc, rs = sums[row_re : row_re + 8, col : col + 128], sums[row_re : row_re + 8, col + 128 : col + 256]
                ic, is_ = sums[row_im : row_im + 8, col : col + 128], sums[row_im : row_im + 8, col + 128 : col + 256]
                zr, zi = rc - is_, rs + ic
                c, s = twiddle_ref[pl.ds(k1, 1), :], twiddle_ref[pl.ds(8 + k1, 1), :]
                if k1 == 0:
                    y.append((zr, None))
                elif k1 == 4:
                    y.append((zr * c - zi * s, None))
                else:
                    y.append((zr * c - zi * s, zr * s + zi * c))
            a = [None] + [y[k][0] + y[8 - k][0] for k in (1, 2, 3)]
            d = [None] + [y[k][1] - y[8 - k][1] for k in (1, 2, 3)]
            up, um = y[0][0] + y[4][0], y[0][0] - y[4][0]
            ap, am = a[1] + a[3], ROOT_HALF * (a[1] - a[3])
            dm, dp = d[1] - d[3], ROOT_HALF * (d[1] + d[3])
            upp, upm = up + a[2], up - a[2]
            ump, umm = um + d[2], um - d[2]
            outs = [
                upp + ap,
                umm + am - dp,
                upm - dm,
                ump - am - dp,
                upp - ap,
                umm - am + dp,
                upm + dm,
                ump + am + dp,
            ]
            for half in range(4):
                v0, v1 = outs[2 * half], outs[2 * half + 1]
                base = (sp * 2 * 2 + b) * 32 + half * 8
                out_ref[pl.ds(base, 8), :] = jnp.where(sub < 4, v0, pltpu.roll(v1, 4, axis=0))
                out_ref[pl.ds(base + 64, 8), :] = jnp.where(sub < 4, pltpu.roll(v0, 4, axis=0), v1)
            for second in range(2):
                block = pl.ds(32 * (4 * sp + 2 * second + b), 32)
                copies.append(pltpu.make_async_copy(out_ref.at[block], out_hbm.at[block], sems.at[len(copies)]))
                copies[-1].start()
    for copy in copies:
        copy.wait()


def spaces(*kinds):
    return [pl.BlockSpec(memory_space=kind) for kind in kinds]


VMEM, HBM = pltpu.VMEM, pltpu.HBM


def call(kernel, out_shapes, in_specs, name, out_space=VMEM, scratch=(), dtype=F32):
    shapes = [jax.ShapeDtypeStruct(shape, dtype) for shape in out_shapes]
    out_specs = spaces(*[out_space] * len(shapes))
    return pl.pallas_call(
        kernel,
        out_shape=shapes if len(shapes) > 1 else shapes[0],
        in_specs=in_specs,
        out_specs=out_specs if len(shapes) > 1 else out_specs[0],
        scratch_shapes=list(scratch),
        name=name,
        compiler_params=pltpu.CompilerParams(vmem_limit_bytes=16 * 1024 * 1024),
    )


def in_hbm(x):
    return pltpu.with_memory_space_constraint(jnp.asarray(x), HBM)


def run_span_forward(velocity):
    twiddle, table = span_forward_tables()
    scratch = (VMEM((768, 128), F32), VMEM(twiddle.shape, F32), VMEM(table.shape, BF16), pltpu.SemaphoreType.DMA((3,)))
    run = call(span_forward_kernel, [(768, 128)], spaces(HBM, HBM, HBM), "span_forward", scratch=scratch)
    return run(in_hbm(velocity), in_hbm(twiddle), in_hbm(table))


def run_middle_front(received, band_of, anchor=None):
    def kernel(*refs):
        at_anchor = anchor
        if anchor is None:
            at_anchor = sum(lax.axis_index(axis) for axis in FRONT_AXES) == 0
        middle_front_kernel(at_anchor, *refs)

    scratch = (pltpu.SMEM((8,), jnp.int32), pltpu.SemaphoreType.DMA)
    run = call(kernel, [(576, 128), (288, 128)], spaces(HBM, *[VMEM] * 4), "middle_front", scratch=scratch)
    return run(in_hbm(band_of), received, *middle_tables()[0])


def run_middle_own(own, core=None):
    def kernel(*refs):
        middle_own_kernel(lax.axis_index("core") if core is None else core, *refs)

    back, twiddle, _ = middle_tables()[1]
    return call(kernel, [(768, 256)], spaces(*[VMEM] * 3), "middle_own", dtype=BF16)(own, back, twiddle)


def run_middle_back(rows, got, core=None):
    def kernel(*refs):
        middle_back_kernel(lax.axis_index("core") if core is None else core, *refs)

    return call(kernel, [(384, 128)], spaces(*[VMEM] * 5), "middle_back")(rows, got, *middle_tables()[1])


def run_span_inverse(received):
    scratch = (VMEM((384, 128), F32), pltpu.SemaphoreType.DMA((12,)))
    run = call(span_inverse_kernel, [(384, 128)], spaces(VMEM, VMEM, VMEM), "span_inverse", HBM, scratch)
    return run(received, *span_inverse_tables())


def per_device(velocity, band_of):
    sent = run_span_forward(velocity.reshape(768, 128))
    received = lax.all_to_all(sent.reshape(256, 1, 384), FRONT_AXES, 0, 0, tiled=True)
    own, packed = run_middle_front(received.reshape(768, 128), band_of)
    got = lax.ppermute(packed, "core", ((0, 1), (1, 0)))
    back = run_middle_back(run_middle_own(own), got)
    gathered = lax.all_to_all(back.reshape(128, 1, 384), BACK_AXES, 0, 0, tiled=True)
    out = run_span_inverse(gathered.reshape(384, 128))
    return out.reshape(6, 2, 8, 4, 128).transpose(0, 1, 3, 2, 4).reshape(6, 2, 4, 1024)


def solution(mesh):
    split_mesh = jax.sharding.Mesh(mesh.devices.reshape(4, 4, 2, 2, 4), ("x", "zh", "core", "zl", "y"))
    px, py = ("x", "zh", "core"), ("zl", "y")
    in_specs = (P(None, px, py, None), P())
    out_specs = P(None, None, px + py, None)
    return jax.shard_map(per_device, mesh=split_mesh, in_specs=in_specs, out_specs=out_specs, check_vma=False)
```
